32 devices in a mesh: dp: 4 (over z), ctx: 8 (over y, x, core).
Axes of the slice: x: 2, y: 2, z: 4, core: 2. Of those that a mesh axis runs over, the one named last changes fastest.
Arguments:
- block_input: bfloat16 [4096, 2048], P(('dp', 'ctx')), may hold values from -8 to 8
- out_cotangent: float32 [4096, 2048], P(('dp', 'ctx')), may hold values from -6 to 6
- group_perm: int32 [4, 16], P('dp'), may hold values from 0 to 15, each once within a row
- attn_norm_gain: bfloat16 [2048], replicated, may hold values from 0.5 to 1.5
- attn_norm_bias: bfloat16 [2048], replicated, may hold values from -2 to 2
- qkv_weight: bfloat16 [3, 2048, 2048], P(None, 'dp', 'ctx'), may hold values from -0.198873782 to 0.198873782
- qkv_bias: bfloat16 [3, 2048], replicated, may hold values from -3 to 3
- out_weight: bfloat16 [2048, 2048], P('ctx', 'dp'), may hold values from -3 to 3
- mlp_norm_gain: bfloat16 [2048], replicated, may hold values from 0.5 to 1.5
- mlp_norm_bias: bfloat16 [2048], replicated, may hold values from -2 to 2
- gateup_weight: bfloat16 [2, 2048, 5632], P(None, 'dp', 'ctx'), may hold values from -0.125 to 0.125
- down_weight: bfloat16 [5632, 2048], P('ctx', 'dp'), may hold values from -0.078125 to 0.078125
Outputs:
- block_output: bfloat16 [4096, 2048], P(('dp', 'ctx'))
- input_grad: float32 [4096, 2048], P(('dp', 'ctx'))
- attn_norm_gain_grad: float32 [2048], replicated
- attn_norm_bias_grad: float32 [2048], replicated
- qkv_weight_grad: float32 [3, 2048, 2048], P(None, 'dp', 'ctx')
- qkv_bias_grad: float32 [3, 2048], replicated
- out_weight_grad: float32 [2048, 2048], P('ctx', 'dp')
- mlp_norm_gain_grad: float32 [2048], replicated
- mlp_norm_bias_grad: float32 [2048], replicated
- gateup_weight_grad: float32 [2, 2048, 5632], P(None, 'dp', 'ctx')
- down_weight_grad: float32 [5632, 2048], P('ctx', 'dp')
The draws below stay inside these ranges and needn't reach their ends.
Inputs may be any that keep to these rules, and one draw needn't show every extreme that they name: `group_perm`: each row names every block 0 to 15 once; device c of ctx holds the blocks of 64 tokens named at entries 2 c and 2 c + 1 of its sequence's row, in that order.
All inputs are finite; a program needn't handle non-finite values.
Results may differ from the reference program's by a relative error of at most 0.025.
Values may be sent and summed in bfloat16 or wider, within the bound.
A program may use at most 192 MiB of HBM per device.

```python
import math
import jax
import jax.numpy as jnp
from jax import lax

D = 2048
HEADS = 32
HEAD_DIM = 64
ROT = 16
FF = 5632
TOK_DEV = 128
LEN = 1024
GROUPS = 16
SEQS = 4
TOKENS = 4096


def shared_direction(key):
    return jnp.clip(jax.random.normal(jax.random.fold_in(key, 7001), (D,), jnp.float32), -4.0, 4.0)


def draw_block_input(key, part):
    direction = shared_direction(key)
    noise_key = jax.random.fold_in(key, 11)
    pick_key = jax.random.fold_in(key, 13)
    spread_key = jax.random.fold_in(key, 14)
    base_draw = jnp.clip(jax.random.normal(noise_key, (TOKENS, D), jnp.float32), -5.0, 5.0)
    special_count = max(4, LEN // 256)
    row_table = jnp.broadcast_to(jnp.arange(LEN, dtype=jnp.int32)[None, :], (SEQS, LEN))
    picked = jax.random.permutation(pick_key, row_table, axis=1, independent=True)[:, :special_count]
    marks = jnp.any(picked[:, :, None] == jnp.arange(LEN, dtype=jnp.int32)[None, None, :], axis=1).reshape(TOKENS, 1)
    spread = jnp.exp(jax.random.uniform(spread_key, (TOKENS, 1), jnp.float32, math.log(0.05), math.log(0.6)))
    special = direction[None, :] + spread * base_draw
    return jnp.where(marks, special, base_draw).astype(jnp.bfloat16)


def draw_qkv_weight(key, part):
    direction = shared_direction(key)
    base_key = jax.random.fold_in(key, 21)
    base_draw = jnp.clip(jax.random.normal(base_key, (3, D, D), jnp.float32), -6.0, 6.0)
    chosen = max(1, HEADS // 16)
    head_order = jax.random.permutation(jax.random.fold_in(key, 22), HEADS)
    rank_ids = jnp.arange(HEADS, dtype=jnp.int32)
    ladder = jnp.where(rank_ids < chosen, 1.0 - 0.25 * rank_ids.astype(jnp.float32) / max(chosen - 1, 1), 0.0)
    strength = jnp.sum(jnp.where(head_order[:, None] == rank_ids[None, :], ladder[:, None], 0.0), axis=0)
    sign_table = (2 * jax.random.randint(jax.random.fold_in(key, 23), (HEADS, HEAD_DIM), 0, 2) - 1).astype(jnp.float32)
    unrotated = (jnp.arange(HEAD_DIM, dtype=jnp.int32) >= ROT).astype(jnp.float32)
    column = (strength[:, None] * sign_table * unrotated[None, :]).reshape(D) / math.sqrt(HEAD_DIM - ROT)
    amplitude = 1.4 * math.sqrt(min(D, 1024)) / D
    aligned = amplitude * direction[:, None] * column[None, :]
    layers = jnp.stack([aligned, aligned, jnp.zeros_like(aligned)])
    return (base_draw / math.sqrt(D) + layers).astype(jnp.bfloat16)


def shard_levels(key, extent, shards, low, top_value):
    level = 1.0
    for dim, shards_of in shards:
        draws = jax.random.uniform(jax.random.fold_in(jax.random.fold_in(key, 6), dim), (shards_of,), jnp.float32, low / len(shards), top_value / len(shards))
        level = level * jnp.repeat(jnp.exp(draws), extent[dim] // shards_of).reshape((-1,) + (1,) * (len(extent) - 1 - dim))
    return level


def gaussian(rng, extent, deviation, most, cuts=(), kind=jnp.bfloat16):
    loudness = shard_levels(rng, extent, cuts, -0.22, 0.18) if cuts else 1.0
    array = jax.random.normal(rng, extent, jnp.float32) * deviation * loudness
    return jnp.minimum(jnp.maximum(array, -most), most).astype(kind)


def setup_inputs(seed: int = 0) -> dict:
    splits = jax.random.split(jax.random.key(seed), 13)
    return {
        "block_input": draw_block_input(jax.random.fold_in(splits[12], 71), 0),
        "out_cotangent": gaussian(splits[1], (TOKENS, D), 1.0, 6.0, ((0, 32),), jnp.float32),
        "group_perm": jax.vmap(lambda own: jax.random.permutation(own, GROUPS))(jax.random.split(splits[2], SEQS)).reshape((SEQS, GROUPS)).astype(jnp.int32),
        "attn_norm_gain": jnp.clip(1.0 + 0.1 * jax.random.normal(splits[3], (D,), jnp.float32), 0.5, 1.5).astype(jnp.bfloat16),
        "attn_norm_bias": gaussian(splits[4], (D,), 0.3, 2.0),
        "qkv_weight": draw_qkv_weight(jax.random.fold_in(splits[12], 71), 0),
        "qkv_bias": gaussian(splits[6], (3, D), 0.5, 3.0),
        "out_weight": gaussian(splits[7], (D, D), (max(D // 512, 1)) ** -0.5, 3.0, ((0, 8), (1, 4))),
        "mlp_norm_gain": jnp.clip(1.0 + 0.1 * jax.random.normal(splits[8], (D,), jnp.float32), 0.5, 1.5).astype(jnp.bfloat16),
        "mlp_norm_bias": gaussian(splits[9], (D,), 0.3, 2.0),
        "gateup_weight": gaussian(splits[10], (2, D, FF), D ** -0.5, 0.125, ((1, 4), (2, 8))),
        "down_weight": gaussian(splits[11], (FF, D), FF ** -0.5, 0.078125, ((0, 8), (1, 4))),
    }


eps_norm = 1e-05
rope_base = 10000.0
neg_big = -1e+30

def round_back(values):
    return lax.optimization_barrier(values.astype(jnp.bfloat16)).astype(jnp.float32)

def apply_layer_norm(values, gain_vec, bias_vec):
    mean_val = lax.optimization_barrier(jnp.mean(values, axis=-1, keepdims=True))
    centred = values - mean_val
    variance = lax.optimization_barrier(jnp.mean(centred * centred, axis=-1, keepdims=True))
    rscale = lax.rsqrt(variance + eps_norm)
    normed = centred * rscale
    return (normed * gain_vec + bias_vec, normed, rscale)

def layer_norm_backward(grad_out, normed, rscale, gain_vec):
    gain_grad = lax.optimization_barrier(jnp.sum(grad_out * normed, axis=0))
    bias_grad = lax.optimization_barrier(jnp.sum(grad_out, axis=0))
    scaled = grad_out * gain_vec
    grad_in = rscale * (scaled - lax.optimization_barrier(jnp.mean(scaled, axis=-1, keepdims=True)) - normed * lax.optimization_barrier(jnp.mean(scaled * normed, axis=-1, keepdims=True)))
    return (grad_in, gain_grad, bias_grad)

def rope_tables(positions):
    half_rot = ROT // 2
    exponent = jnp.arange(half_rot, dtype=jnp.float32) * (2.0 / ROT)
    inverse = jnp.exp(-exponent * math.log(rope_base))
    angle_val = positions.astype(jnp.float32)[:, None] * inverse[None, :]
    return (jnp.cos(angle_val)[:, None, :], jnp.sin(angle_val)[:, None, :])

def rotate(tensor, cosine, sine_val):
    half_rot = ROT // 2
    first_half = tensor[..., :half_rot]
    second = tensor[..., half_rot:ROT]
    remainder = tensor[..., ROT:]
    return jnp.concatenate([first_half * cosine - second * sine_val, second * cosine + first_half * sine_val, remainder], axis=-1)

def unrotate(tensor, cosine, sine_val):
    half_rot = ROT // 2
    first_half = tensor[..., :half_rot]
    second = tensor[..., half_rot:ROT]
    remainder = tensor[..., ROT:]
    return jnp.concatenate([first_half * cosine + second * sine_val, second * cosine - first_half * sine_val, remainder], axis=-1)

def reference(block_input, out_cotangent, group_perm, attn_norm_gain, attn_norm_bias, qkv_weight, qkv_bias, out_weight, mlp_norm_gain, mlp_norm_bias, gateup_weight, down_weight):
    f32 = jnp.float32
    bf16 = jnp.bfloat16
    half_group = TOK_DEV // 2
    score_scale = 1.0 / math.sqrt(HEAD_DIM)
    query_block = min(512, LEN)
    block_count = LEN // query_block
    first_norm_scale = attn_norm_gain.astype(f32)
    first_norm_bias = attn_norm_bias.astype(f32)
    second_norm_scale = mlp_norm_gain.astype(f32)
    second_norm_bias = mlp_norm_bias.astype(f32)
    qkv_shift = qkv_bias.astype(f32)

    def one_sequence(grads, inputs):
        seq_in, seq_cot, order_row = inputs
        row_ids = jnp.arange(LEN, dtype=jnp.int32)
        positions = order_row[row_ids // half_group] * half_group + row_ids % half_group
        cosine, sine_val = rope_tables(positions)
        inputs_wide_float = seq_in.astype(f32)
        first_normalized_rows, first_centered_scaled, first_inverse_deviation = apply_layer_norm(inputs_wide_float, first_norm_scale, first_norm_bias)
        normed_one_b = first_normalized_rows.astype(bf16)
        query_raw = jnp.dot(normed_one_b, qkv_weight[0], preferred_element_type=f32) + qkv_shift[0]
        key_raw = jnp.dot(normed_one_b, qkv_weight[1], preferred_element_type=f32) + qkv_shift[1]
        value_raw = jnp.dot(normed_one_b, qkv_weight[2], preferred_element_type=f32) + qkv_shift[2]
        query = rotate(query_raw.reshape(LEN, HEADS, HEAD_DIM), cosine, sine_val).astype(bf16)
        keys_b = rotate(key_raw.reshape(LEN, HEADS, HEAD_DIM), cosine, sine_val).astype(bf16)
        values_b = value_raw.reshape(LEN, HEADS, HEAD_DIM).astype(bf16)
        keys_f = keys_b.astype(f32)
        values_f = values_b.astype(f32)
        query_blocks = query.reshape(block_count, query_block, HEADS, HEAD_DIM)
        pos_blocks = positions.reshape(block_count, query_block)

        def fwd_block(blk):
            query_blk, pos_blk = blk
            scores = jnp.einsum('rhd,nhd->hrn', query_blk.astype(f32), keys_f) * score_scale
            visible = positions[None, None, :] <= pos_blk[None, :, None]
            scores = jnp.where(visible, scores, neg_big)
            peak = lax.optimization_barrier(jnp.max(scores, axis=-1))
            probs = jnp.where(visible, jnp.exp(scores - peak[..., None]), 0.0)
            total = lax.optimization_barrier(jnp.sum(probs, axis=-1))
            accum = jnp.einsum('hrn,nhd->rhd', round_back(probs), values_f)
            return ((accum / total.T[:, :, None]).astype(bf16), peak + jnp.log(total))
        attn_blocks, log_total = lax.map(fwd_block, (query_blocks, pos_blocks))
        attn_val = attn_blocks.reshape(LEN, HEADS, HEAD_DIM)
        attn_flat = attn_val.reshape(LEN, D)
        residual_stream = inputs_wide_float + jnp.dot(attn_flat, out_weight, preferred_element_type=f32)
        second_normalized_rows, second_centered_scaled, second_inverse_deviation = apply_layer_norm(residual_stream, second_norm_scale, second_norm_bias)
        normed_two_b = second_normalized_rows.astype(bf16)
        gate_val = jnp.dot(normed_two_b, gateup_weight[0], preferred_element_type=f32)
        up_val = jnp.dot(normed_two_b, gateup_weight[1], preferred_element_type=f32)
        sigma = jax.nn.sigmoid(gate_val)
        hidden_b = (gate_val * sigma * up_val).astype(bf16)
        seq_out = (residual_stream + jnp.dot(hidden_b, down_weight, preferred_element_type=f32)).astype(bf16)
        cot_b = seq_cot.astype(bf16)
        down_grad = jnp.dot(hidden_b.T, cot_b, preferred_element_type=f32)
        hidden_grad = jnp.dot(cot_b, down_weight.T, preferred_element_type=f32)
        gate_grad = (hidden_grad * up_val * sigma * (1.0 + gate_val * (1.0 - sigma))).astype(bf16)
        up_grad = (hidden_grad * gate_val * sigma).astype(bf16)
        gate_w_grad = jnp.dot(normed_two_b.T, gate_grad, preferred_element_type=f32)
        up_w_grad = jnp.dot(normed_two_b.T, up_grad, preferred_element_type=f32)
        second_normalized_gradient = jnp.dot(gate_grad, gateup_weight[0].T, preferred_element_type=f32) + jnp.dot(up_grad, gateup_weight[1].T, preferred_element_type=f32)
        residual_slice, second_norm_scale_gradient, second_norm_bias_gradient = layer_norm_backward(second_normalized_gradient, second_centered_scaled, second_inverse_deviation, second_norm_scale)
        resid_grad = seq_cot + residual_slice
        resid_b = resid_grad.astype(bf16)
        out_w_grad = jnp.dot(attn_flat.T, resid_b, preferred_element_type=f32)
        attn_val_grad = jnp.dot(resid_b, out_weight.T, preferred_element_type=f32).reshape(LEN, HEADS, HEAD_DIM)
        delta = lax.optimization_barrier(jnp.sum(attn_val_grad * attn_val.astype(f32), axis=-1))
        attn_grad_b = attn_val_grad.astype(bf16)

        def back_block(carry, blk):
            key_grad, value_grad = carry
            query_blk, pos_blk, lse_blk, grad_blk, delta_blk = blk
            query_blk_f = query_blk.astype(f32)
            grad_blk_f = grad_blk.astype(f32)
            scores = jnp.einsum('rhd,nhd->hrn', query_blk_f, keys_f) * score_scale
            visible = positions[None, None, :] <= pos_blk[None, :, None]
            scores = jnp.where(visible, scores, neg_big)
            probs = jnp.where(visible, jnp.exp(scores - lse_blk[..., None]), 0.0)
            value_grad = value_grad + jnp.einsum('hrn,rhd->nhd', round_back(probs), grad_blk_f)
            prob_grad = jnp.einsum('rhd,nhd->hrn', grad_blk_f, values_f)
            score_grad = round_back(probs * (prob_grad - delta_blk.T[:, :, None]))
            query_grad_blk = jnp.einsum('hrn,nhd->rhd', score_grad, keys_f) * score_scale
            key_grad = key_grad + jnp.einsum('hrn,rhd->nhd', score_grad, query_blk_f) * score_scale
            return ((key_grad, value_grad), query_grad_blk)
        zero_kv = jnp.zeros((LEN, HEADS, HEAD_DIM), f32)
        (key_grad, value_grad), query_grads = lax.scan(back_block, (zero_kv, zero_kv), (query_blocks, pos_blocks, log_total, attn_grad_b.reshape(block_count, query_block, HEADS, HEAD_DIM), delta.reshape(block_count, query_block, HEADS)))
        query_grad = query_grads.reshape(LEN, HEADS, HEAD_DIM)
        grad_list = [unrotate(query_grad, cosine, sine_val).reshape(LEN, D), unrotate(key_grad, cosine, sine_val).reshape(LEN, D), value_grad.reshape(LEN, D)]
        shift_grad = jnp.stack([lax.optimization_barrier(jnp.sum(piece, axis=0)) for piece in grad_list])
        grad_list_b = [piece.astype(bf16) for piece in grad_list]
        qkv_w_grad = jnp.stack([jnp.dot(normed_one_b.T, piece, preferred_element_type=f32) for piece in grad_list_b])
        first_normalized_gradient = jnp.dot(grad_list_b[0], qkv_weight[0].T, preferred_element_type=f32) + jnp.dot(grad_list_b[1], qkv_weight[1].T, preferred_element_type=f32) + jnp.dot(grad_list_b[2], qkv_weight[2].T, preferred_element_type=f32)
        input_slice, first_norm_scale_gradient, first_norm_bias_gradient = layer_norm_backward(first_normalized_gradient, first_centered_scaled, first_inverse_deviation, first_norm_scale)
        seq_input_grad = resid_grad + input_slice
        new_grads = (first_norm_scale_gradient, first_norm_bias_gradient, qkv_w_grad, shift_grad, out_w_grad, second_norm_scale_gradient, second_norm_bias_gradient, jnp.stack([gate_w_grad, up_w_grad]), down_grad)
        grads = tuple((old + new for old, new in zip(grads, new_grads)))
        return (grads, (seq_out, seq_input_grad))
    zero_grads = (jnp.zeros((D,), f32), jnp.zeros((D,), f32), jnp.zeros((3, D, D), f32), jnp.zeros((3, D), f32), jnp.zeros((D, D), f32), jnp.zeros((D,), f32), jnp.zeros((D,), f32), jnp.zeros((2, D, FF), f32), jnp.zeros((FF, D), f32))
    grads, (outputs, input_grads) = lax.scan(one_sequence, zero_grads, (block_input.reshape(SEQS, LEN, D), out_cotangent.reshape(SEQS, LEN, D), group_perm))
    return (outputs.reshape(TOKENS, D), input_grads.reshape(TOKENS, D), grads[0], grads[1], grads[2], grads[3], grads[4], grads[5], grads[6], grads[7], grads[8])
```

```python
import functools
import math

import jax
import jax.numpy as jnp
from jax import lax
from jax.experimental import pallas as pl
from jax.experimental.pallas import tpu as pltpu
from jax.sharding import PartitionSpec as P

MESH = pl.DeviceIdType.MESH
VMEM = pl.BlockSpec(memory_space=pltpu.VMEM)
ANY = pl.BlockSpec(memory_space=pl.ANY)
DMA = pltpu.SemaphoreType.DMA

D = 2048
HEADS = 32
HEAD_DIM = 64
ROT = 16


eps_norm = 1e-05
rope_base = 10000.0
neg_big = -1e30


class Place:
    def __init__(self):
        self.ndp = lax.axis_size("dp")
        self.nctx = lax.axis_size("ctx")
        self.nchip = self.nctx // 2
        self.z = lax.axis_index("dp")
        self.c = lax.axis_index("ctx")
        self.p = lax.div(self.c, 2)
        self.k = lax.rem(self.c, 2)

    def chip(self, offset):
        return lax.rem(self.p + offset, self.nchip)

    def at(self, c):
        return {"dp": self.z, "ctx": c}

    def partner(self):
        return self.at(2 * self.p + 1 - self.k)

    def same_core(self, q):
        return self.at(2 * q + self.k)


def greet(place, along_ctx=True, along_dp=False, all_ctx=False):
    barrier = pltpu.get_barrier_semaphore()
    peers = []
    if all_ctx:
        peers += [place.at(lax.rem(place.c + i, place.nctx)) for i in range(1, place.nctx)]
    elif along_ctx:
        peers += [place.partner()] + [place.same_core(place.chip(i)) for i in range(1, place.nchip)]
    if along_dp:
        peers += [{"dp": lax.rem(place.z + i, place.ndp), "ctx": place.c} for i in range(1, place.ndp)]
    for peer in peers:
        pl.semaphore_signal(barrier, inc=1, device_id=peer, device_id_type=MESH)
    pl.semaphore_wait(barrier, len(peers))


def push(src, dst, send, recv, device):
    return pltpu.make_async_remote_copy(
        src_ref=src, dst_ref=dst, send_sem=send, recv_sem=recv, device_id=device, device_id_type=MESH
    )


class RowGather:
    def __init__(self, place, block, whole, send, recv, local):
        self.place, self.block, self.whole = place, block, whole
        self.send, self.recv, self.local = send, recv, local
        self.rows = block.shape[0]

    def slot(self, c):
        return self.whole.at[pl.ds(pl.multiple_of(c * self.rows, self.rows), self.rows)]

    def direct(self, i):
        place = self.place
        q = place.chip(i)
        return push(self.block, self.slot(place.c), self.send.at[i], self.recv.at[place.c], place.same_core(q))

    def own(self):
        place = self.place
        return push(self.block, self.slot(place.c), self.send.at[0], self.recv.at[place.c], place.partner())

    def passed(self, i):
        place = self.place
        c = 2 * place.chip(i) + place.k
        return push(
            self.slot(c), self.slot(c), self.send.at[place.nchip + i - 1], self.recv.at[c], place.partner()
        )

    def arrival(self, c):
        return push(self.block, self.slot(c), self.send.at[0], self.recv.at[c], self.place.partner())

    def keep(self):
        return pltpu.make_async_copy(self.block, self.slot(self.place.c), self.local)

    def start(self):
        for i in range(1, self.place.nchip):
            self.direct(i).start()
        self.own().start()
        self.keep().start()

    def forward(self):
        place = self.place
        for i in range(1, place.nchip):
            self.arrival(2 * place.chip(i) + place.k).wait_recv()
            self.passed(i).start()

    def finish(self):
        place = self.place
        for i in range(place.nchip):
            self.arrival(2 * place.chip(i) + 1 - place.k).wait_recv()
        self.own().wait_send()
        for i in range(1, place.nchip):
            self.direct(i).wait_send()
            self.passed(i).wait_send()
        self.keep().wait()


def gather_sems(nctx):
    return [DMA((nctx,)), DMA((nctx,)), DMA]


class DepthGather:
    def __init__(self, place, piece, whole, where, send, recv, local):
        self.place, self.piece, self.whole, self.where = place, piece, whole, where
        self.send, self.recv, self.local = send, recv, local
        self.line = place.ndp == 4
        self.middle = jnp.logical_or(place.z == 1, place.z == 2)
        self.far = 6 - 3 * place.z

    def copy(self, src, z_src, z_dst, sem):
        return push(
            src, self.where(self.whole, z_src), self.send.at[sem], self.recv.at[z_src], {"dp": z_dst, "ctx": self.place.c}
        )

    def directs(self):
        z, n = self.place.z, self.place.ndp
        if not self.line:
            return [(None, self.copy(self.piece, z, lax.rem(z + i, n), i - 1)) for i in range(1, n)]
        out = []
        for sem, step in enumerate((2, -2, 1, -1)):
            d = z + step
            ok = jnp.logical_and(d >= 0, d < 4)
            out.append((ok, self.copy(self.piece, z, jnp.clip(d, 0, 3), sem)))
        return out

    def keep(self):
        return pltpu.make_async_copy(self.piece, self.where(self.whole, self.place.z), self.local)

    def start(self):
        for ok, copy in self.directs():
            if ok is None:
                copy.start()
            else:
                pl.when(ok)(copy.start)
        self.keep().start()

    def passed(self):
        far = jnp.clip(self.far, 0, 3)
        return self.copy(self.where(self.whole, far), far, jnp.clip(3 * (self.place.z - 1), 0, 3), 4)

    def forward(self):
        if self.line:

            @pl.when(self.middle)
            def _():
                far = jnp.clip(self.far, 0, 3)
                self.copy(self.piece, far, far, 4).wait_recv()
                self.passed().start()

    def finish(self):
        z, n = self.place.z, self.place.ndp
        for i in range(1, n):
            src = lax.rem(z + i, n)
            wait = self.copy(self.piece, src, src, 0).wait_recv
            if self.line:
                pl.when(jnp.logical_not(jnp.logical_and(self.middle, src == self.far)))(wait)
            else:
                wait()
        for ok, copy in self.directs():
            if ok is None:
                copy.wait_send()
            else:
                pl.when(ok)(copy.wait_send)
        if self.line:
            pl.when(self.middle)(self.passed().wait_send)
        self.keep().wait()


def depth_sems(ndp):
    return [DMA((ndp + 1,)), DMA((ndp,)), DMA]


STEP = 16


def row_loop(rows, body):
    def step(i, carry):
        body(pl.ds(pl.multiple_of(i * STEP, STEP), STEP))
        return carry

    lax.fori_loop(0, rows // STEP, step, 0)


def normal(values):
    centred = values - jnp.mean(values, axis=-1, keepdims=True)
    rscale = lax.rsqrt(jnp.mean(centred * centred, axis=-1, keepdims=True) + eps_norm)
    return centred * rscale, rscale


def normal_back(grad_out, normed, rscale, gain):
    scaled = grad_out * gain
    return rscale * (
        scaled
        - jnp.mean(scaled, axis=-1, keepdims=True)
        - normed * jnp.mean(scaled * normed, axis=-1, keepdims=True)
    )


def gather_kernel(
    x_ref, cot_ref, gain_ref, bias_ref, qkv_ref, out_ref,
    rows_all, cot_all, qkv_all, out_all,
    row_block, cot_block, *sems
):
    place = Place()
    greet(place, along_dp=True)
    depth = qkv_ref.shape[1]
    width = out_ref.shape[1]

    def qkv_at(ref, z):
        return ref.at[:, pl.ds(pl.multiple_of(z * depth, depth), depth), :]

    def out_at(ref, z):
        return ref.at[:, pl.ds(pl.multiple_of(z * width, width), width)]

    qkv = DepthGather(place, qkv_ref, qkv_all, qkv_at, *sems[0:3])
    out = DepthGather(place, out_ref, out_all, out_at, *sems[3:6])
    rows = RowGather(place, row_block, rows_all, *sems[6:9])
    cots = RowGather(place, cot_block, cot_all, *sems[9:12])
    qkv.start()
    out.start()
    gain, bias = gain_ref[...].astype(jnp.float32), bias_ref[...].astype(jnp.float32)

    def norm(at):
        normed, _ = normal(x_ref[at, :].astype(jnp.float32))
        row_block[at, :] = (normed * gain + bias).astype(jnp.bfloat16)
        cot_block[at, :] = cot_ref[at, :].astype(jnp.bfloat16)

    row_loop(x_ref.shape[0], norm)
    rows.start()
    cots.start()
    rows.forward()
    cots.forward()
    qkv.forward()
    out.forward()
    rows.finish()
    cots.finish()
    qkv.finish()
    out.finish()


def gather_inputs(x, cot, gain, bias, qkv, out):
    ndp, nctx = lax.axis_size("dp"), lax.axis_size("ctx")
    rows, d = x.shape
    bf16 = jnp.bfloat16
    return pl.pallas_call(
        gather_kernel,
        out_shape=(
            jax.ShapeDtypeStruct((rows * nctx, d), bf16),
            jax.ShapeDtypeStruct((rows * nctx, d), bf16),
            jax.ShapeDtypeStruct((qkv.shape[0], qkv.shape[1] * ndp, qkv.shape[2]), bf16),
            jax.ShapeDtypeStruct((out.shape[0], out.shape[1] * ndp), bf16),
        ),
        in_specs=[VMEM] * 6,
        out_specs=(ANY,) * 4,
        scratch_shapes=[pltpu.VMEM((rows, d), bf16), pltpu.VMEM((rows, d), bf16)]
        + depth_sems(ndp) * 2
        + gather_sems(nctx) * 2,
        compiler_params=pltpu.CompilerParams(collective_id=0, has_side_effects=True),
        cost_estimate=pl.CostEstimate(flops=0, bytes_accessed=200_000_000, transcendentals=0),
        name="gather_inputs",
    )(x, cot, gain[None, :], bias[None, :], qkv, out)


class SumScatter:
    TILE = 512

    def __init__(self, place, rows, product, mine, to_pair, from_pair, to_chip, from_chip, sems):
        self.place, self.rows, self.product = place, rows, product
        self.mine, self.to_pair, self.from_pair = mine, to_pair, from_pair
        self.to_chip, self.from_chip = to_chip, from_chip
        self.pair_send, self.pair_recv, self.chip_send, self.chip_recv = sems

    def pair(self, i):
        return push(
            self.to_pair.at[i], self.from_pair.at[i], self.pair_send.at[i], self.pair_recv.at[i], self.place.partner()
        )

    def chips(self, i):
        return push(
            self.to_chip.at[i],
            self.from_chip.at[i],
            self.chip_send.at[i],
            self.chip_recv.at[i],
            self.place.same_core(self.place.chip(i + 1)),
        )

    def run(self):
        place, rows, tile = self.place, self.rows, self.TILE
        nchip = place.nchip
        width = self.mine.shape[-1]

        def hand_on(i):
            self.pair(i).wait_recv()

            def add(at):
                both = self.mine[i, at, :] + self.from_pair[i, at, :].astype(jnp.float32)
                self.to_chip[i, at, :] = both.astype(jnp.bfloat16)

            row_loop(rows, add)
            self.chips(i).start()

        def step(i, carry):
            q = lax.rem(place.p + 1 + i, nchip)
            first = pl.multiple_of(q * 2 * rows, 2 * rows)

            def columns(j, inner):
                cols = pl.ds(pl.multiple_of(j * tile, tile), tile)
                part = self.product(pl.ds(first, 2 * rows), cols)

                @pl.when(place.k == 0)
                def _():
                    self.mine[i, :, cols] = part[:rows]
                    self.to_pair[i, :, cols] = part[rows:].astype(jnp.bfloat16)

                @pl.when(place.k == 1)
                def _():
                    self.mine[i, :, cols] = part[rows:]
                    self.to_pair[i, :, cols] = part[:rows].astype(jnp.bfloat16)

                return inner

            lax.fori_loop(0, width // tile, columns, 0)
            self.pair(i).start()
            pl.when(i > 0)(lambda: hand_on(i - 1))
            return carry

        lax.fori_loop(0, nchip, step, 0)
        self.pair(nchip - 1).wait_recv()
        for i in range(nchip - 1):
            self.chips(i).wait_recv()

    def total(self, at):
        last = self.place.nchip - 1
        value = self.mine[last, at, :] + self.from_pair[last, at, :].astype(jnp.float32)
        for i in range(last):
            value = value + self.from_chip[i, at, :].astype(jnp.float32)
        return value

    def finish(self):
        for i in range(self.place.nchip):
            self.pair(i).wait_send()
        for i in range(self.place.nchip - 1):
            self.chips(i).wait_send()


def scatter_scratch(nctx, rows, d):
    n = nctx // 2
    bf16 = jnp.bfloat16
    return [
        pltpu.VMEM((n, rows, d), jnp.float32),
        pltpu.VMEM((n, rows, d), bf16),
        pltpu.VMEM((n, rows, d), bf16),
        pltpu.VMEM((n - 1, rows, d), bf16),
        pltpu.VMEM((n - 1, rows, d), bf16),
        DMA((n,)),
        DMA((n,)),
        DMA((n - 1,)),
        DMA((n - 1,)),
    ]


def dot_nn(a, b):
    return jnp.dot(a, b, preferred_element_type=jnp.float32)


def dot_nt(a, b):
    return lax.dot_general(a, b, (((1,), (1,)), ((), ())), preferred_element_type=jnp.float32)


def attn_out_kernel(attn_ref, w_ref, x_ref, gain_ref, bias_ref, resid_ref, normed_all, block, *scratch):
    place = Place()
    greet(place)
    scatter = SumScatter(
        place,
        x_ref.shape[0],
        lambda rows, cols: dot_nn(attn_ref[rows, :], w_ref[:, cols]),
        *scratch[:5],
        scratch[5:9],
    )
    scatter.run()
    gain, bias = gain_ref[...].astype(jnp.float32), bias_ref[...].astype(jnp.float32)

    def norm(at):
        resid = x_ref[at, :].astype(jnp.float32) + scatter.total(at)
        resid_ref[at, :] = resid
        normed, _ = normal(resid)
        block[at, :] = (normed * gain + bias).astype(jnp.bfloat16)

    row_loop(x_ref.shape[0], norm)
    rows = RowGather(place, block, normed_all, *scratch[9:12])
    rows.start()
    rows.forward()
    rows.finish()
    scatter.finish()


def attn_out(attn, w, x, gain, bias):
    nctx = lax.axis_size("ctx")
    rows, d = x.shape
    return pl.pallas_call(
        attn_out_kernel,
        out_shape=(
            jax.ShapeDtypeStruct((rows, d), jnp.float32),
            jax.ShapeDtypeStruct((rows * nctx, d), jnp.bfloat16),
        ),
        in_specs=[VMEM] * 5,
        out_specs=(VMEM, ANY),
        scratch_shapes=[pltpu.VMEM((rows, d), jnp.bfloat16)]
        + scatter_scratch(nctx, rows, d)
        + gather_sems(nctx),
        compiler_params=pltpu.CompilerParams(collective_id=1, has_side_effects=True),
        cost_estimate=pl.CostEstimate(flops=0, bytes_accessed=150_000_000, transcendentals=0),
        name="attn_out",
    )(attn, w, x, gain[None, :], bias[None, :])


def mlp_back_kernel(
    gate_ref, up_ref, w_ref, resid_ref, cot_ref, gain_ref, grad_ref, vec_ref, grad_all, block, *scratch
):
    place = Place()
    greet(place)
    scatter = SumScatter(
        place,
        resid_ref.shape[0],
        lambda rows, cols: dot_nt(gate_ref[rows, :], w_ref[0, cols, :]) + dot_nt(up_ref[rows, :], w_ref[1, cols, :]),
        *scratch[:5],
        scratch[5:9],
    )
    scatter.run()
    gain = gain_ref[...].astype(jnp.float32)
    vec_ref[...] = jnp.zeros_like(vec_ref)

    def back(at):
        grad = scatter.total(at)
        normed, rscale = normal(resid_ref[at, :])
        vec_ref[0:1, :] += jnp.sum(grad * normed, axis=0, keepdims=True)
        vec_ref[1:2, :] += jnp.sum(grad, axis=0, keepdims=True)
        out = cot_ref[at, :] + normal_back(grad, normed, rscale, gain)
        grad_ref[at, :] = out
        block[at, :] = out.astype(jnp.bfloat16)

    row_loop(resid_ref.shape[0], back)
    rows = RowGather(place, block, grad_all, *scratch[9:12])
    rows.start()
    rows.forward()
    rows.finish()
    scatter.finish()


def mlp_back(gate_grad, up_grad, w, resid, cot, gain):
    nctx = lax.axis_size("ctx")
    rows, d = resid.shape
    return pl.pallas_call(
        mlp_back_kernel,
        out_shape=(
            jax.ShapeDtypeStruct((rows, d), jnp.float32),
            jax.ShapeDtypeStruct((2, d), jnp.float32),
            jax.ShapeDtypeStruct((rows * nctx, d), jnp.bfloat16),
        ),
        in_specs=[VMEM] * 6,
        out_specs=(VMEM, VMEM, ANY),
        scratch_shapes=[pltpu.VMEM((rows, d), jnp.bfloat16)]
        + scatter_scratch(nctx, rows, d)
        + gather_sems(nctx),
        compiler_params=pltpu.CompilerParams(collective_id=2, has_side_effects=True),
        cost_estimate=pl.CostEstimate(flops=0, bytes_accessed=150_000_000, transcendentals=0),
        name="mlp_back",
    )(gate_grad, up_grad, w, resid, cot, gain[None, :])


def attn_back_kernel(parts_ref, w_ref, x_ref, grad_ref, gain_ref, out_ref, vec_ref, *scratch):
    place = Place()
    greet(place)

    def product(rows, cols):
        part = dot_nt(parts_ref[0, rows, :], w_ref[0, cols, :])
        part = part + dot_nt(parts_ref[1, rows, :], w_ref[1, cols, :])
        return part + dot_nt(parts_ref[2, rows, :], w_ref[2, cols, :])

    scatter = SumScatter(place, x_ref.shape[0], product, *scratch[:5], scratch[5:9])
    scatter.run()
    gain = gain_ref[...].astype(jnp.float32)
    vec_ref[...] = jnp.zeros_like(vec_ref)

    def back(at):
        grad = scatter.total(at)
        normed, rscale = normal(x_ref[at, :].astype(jnp.float32))
        vec_ref[0:1, :] += jnp.sum(grad * normed, axis=0, keepdims=True)
        vec_ref[1:2, :] += jnp.sum(grad, axis=0, keepdims=True)
        out_ref[at, :] = grad_ref[at, :] + normal_back(grad, normed, rscale, gain)

    row_loop(x_ref.shape[0], back)
    scatter.finish()


def attn_back(parts, w, x, grad, gain):
    nctx = lax.axis_size("ctx")
    rows, d = x.shape
    return pl.pallas_call(
        attn_back_kernel,
        out_shape=(
            jax.ShapeDtypeStruct((rows, d), jnp.float32),
            jax.ShapeDtypeStruct((2, d), jnp.float32),
        ),
        in_specs=[VMEM] * 5,
        out_specs=(VMEM, VMEM),
        scratch_shapes=scatter_scratch(nctx, rows, d),
        compiler_params=pltpu.CompilerParams(collective_id=3, has_side_effects=True),
        cost_estimate=pl.CostEstimate(flops=0, bytes_accessed=100_000_000, transcendentals=0),
        name="attn_back",
    )(parts, w, x, grad, gain[None, :])


def down_kernel(hidden_ref, w_ref, resid_ref, out_ref, *scratch):
    place = Place()
    greet(place)
    scatter = SumScatter(
        place,
        resid_ref.shape[0],
        lambda rows, cols: dot_nn(hidden_ref[rows, :], w_ref[:, cols]),
        *scratch[:5],
        scratch[5:9],
    )
    scatter.run()

    def add(at):
        out_ref[at, :] = (resid_ref[at, :] + scatter.total(at)).astype(jnp.bfloat16)

    row_loop(resid_ref.shape[0], add)
    scatter.finish()


def down(hidden, w, resid):
    nctx = lax.axis_size("ctx")
    rows, d = resid.shape
    return pl.pallas_call(
        down_kernel,
        out_shape=jax.ShapeDtypeStruct((rows, d), jnp.bfloat16),
        in_specs=[VMEM] * 3,
        out_specs=VMEM,
        scratch_shapes=scatter_scratch(nctx, rows, d),
        compiler_params=pltpu.CompilerParams(collective_id=4, has_side_effects=True),
        cost_estimate=pl.CostEstimate(flops=0, bytes_accessed=100_000_000, transcendentals=0),
        name="down_sum",
    )(hidden, w, resid)


def vectors_kernel(v_ref, out_ref, from_ctx, from_dp, plane, ctx_send, ctx_recv, dp_send, dp_recv):
    place = Place()
    greet(place, all_ctx=True, along_dp=True)
    nctx, ndp, c, z = place.nctx, place.ndp, place.c, place.z

    def across(i):
        return push(
            v_ref, from_ctx.at[c], ctx_send.at[i - 1], ctx_recv.at[c], place.at(lax.rem(c + i, nctx))
        )

    def along(i):
        return push(
            plane, from_dp.at[z], dp_send.at[i - 1], dp_recv.at[z], {"dp": lax.rem(z + i, ndp), "ctx": c}
        )

    for i in range(1, nctx):
        across(i).start()
    from_ctx[c] = v_ref[...]
    for i in range(1, nctx):
        s = lax.rem(c + i, nctx)
        push(v_ref, from_ctx.at[s], ctx_send.at[0], ctx_recv.at[s], place.at(s)).wait_recv()
    value = from_ctx[0]
    for i in range(1, nctx):
        value = value + from_ctx[i]
    plane[...] = value
    for i in range(1, ndp):
        along(i).start()
    from_dp[z] = value
    for i in range(1, ndp):
        s = lax.rem(z + i, ndp)
        push(plane, from_dp.at[s], dp_send.at[0], dp_recv.at[s], {"dp": s, "ctx": c}).wait_recv()
    value = from_dp[0]
    for i in range(1, ndp):
        value = value + from_dp[i]
    out_ref[...] = value
    for i in range(1, nctx):
        across(i).wait_send()
    for i in range(1, ndp):
        along(i).wait_send()


def sum_vectors(v):
    ndp, nctx = lax.axis_size("dp"), lax.axis_size("ctx")
    f32 = jnp.float32
    return pl.pallas_call(
        vectors_kernel,
        out_shape=jax.ShapeDtypeStruct(v.shape, f32),
        in_specs=[VMEM],
        out_specs=VMEM,
        scratch_shapes=[
            pltpu.VMEM((nctx,) + v.shape, f32),
            pltpu.VMEM((ndp,) + v.shape, f32),
            pltpu.VMEM(v.shape, f32),
            DMA((nctx - 1,)),
            DMA((nctx,)),
            DMA((ndp - 1,)),
            DMA((ndp,)),
        ],
        compiler_params=pltpu.CompilerParams(collective_id=5, has_side_effects=True),
        cost_estimate=pl.CostEstimate(flops=0, bytes_accessed=30_000_000, transcendentals=0),
        name="sum_vectors",
    )(v)


def rope_tables(positions):
    half_rot = ROT // 2
    exponent = jnp.arange(half_rot, dtype=jnp.float32) * (2.0 / ROT)
    inverse = jnp.exp(-exponent * math.log(rope_base))
    angle_val = positions.astype(jnp.float32)[:, None] * inverse[None, :]
    return (jnp.cos(angle_val)[:, None, :], jnp.sin(angle_val)[:, None, :])


def rotate(tensor, cosine, sine_val):
    half_rot = ROT // 2
    first_half = tensor[..., :half_rot]
    second = tensor[..., half_rot:ROT]
    remainder = tensor[..., ROT:]
    return jnp.concatenate(
        [
            first_half * cosine - second * sine_val,
            second * cosine + first_half * sine_val,
            remainder,
        ],
        axis=-1,
    )


def unrotate(tensor, cosine, sine_val):
    half_rot = ROT // 2
    first_half = tensor[..., :half_rot]
    second = tensor[..., half_rot:ROT]
    remainder = tensor[..., ROT:]
    return jnp.concatenate(
        [
            first_half * cosine + second * sine_val,
            second * cosine - first_half * sine_val,
            remainder,
        ],
        axis=-1,
    )


def group_positions(group_order, count, half_group):
    row_ids = jnp.arange(count, dtype=jnp.int32)
    group_ids = row_ids // half_group
    matches = group_ids[:, None] == jnp.arange(group_order.shape[0], dtype=jnp.int32)[None, :]
    group_start = jnp.sum(jnp.where(matches, group_order[None, :], 0), axis=1)
    return group_start * half_group + row_ids % half_group


def gather_pair(first, second):
    return (
        lax.all_gather(first, "dp", axis=1, tiled=True),
        lax.all_gather(second, "dp", axis=1, tiled=True),
    )


def shard_pair(first, second):
    return (
        lax.psum_scatter(first.astype(jnp.bfloat16), "dp", scatter_dimension=1, tiled=True).astype(
            jnp.float32
        ),
        lax.psum_scatter(second.astype(jnp.bfloat16), "dp", scatter_dimension=1, tiled=True).astype(
            jnp.float32
        ),
    )


def per_device(
    block_input,
    out_cotangent,
    group_perm,
    attn_norm_gain,
    attn_norm_bias,
    qkv_weight,
    qkv_bias,
    out_weight,
    mlp_norm_gain,
    mlp_norm_bias,
    gateup_weight,
    down_weight,
):
    f32 = jnp.float32
    bf16 = jnp.bfloat16
    tok_rows = block_input.shape[0]
    cycle_size = lax.axis_size("ctx")
    cycle_index = lax.axis_index("ctx")
    seq_len = tok_rows * cycle_size
    half_group = tok_rows // 2
    group_order = group_perm[0]
    score_scale = 1.0 / math.sqrt(HEAD_DIM)
    qkv_shift = qkv_bias.astype(f32)
    rows_all, cot_all, qkv_local, out_local = gather_inputs(
        block_input, out_cotangent, attn_norm_gain, attn_norm_bias, qkv_weight, out_weight
    )
    gateup_weight, down_weight, rows_all = lax.optimization_barrier((gateup_weight, down_weight, rows_all))
    gateup_local, down_local = gather_pair(gateup_weight, down_weight)
    all_pos = group_positions(group_order, seq_len, half_group)
    cos_all, sin_all = rope_tables(all_pos)
    local_heads = HEADS // cycle_size
    width_local = local_heads * HEAD_DIM
    head_first = cycle_index * width_local
    shift_local = lax.dynamic_slice_in_dim(qkv_shift, head_first, width_local, 1)
    query_raw = jnp.dot(rows_all, qkv_local[0], preferred_element_type=f32) + shift_local[0]
    key_raw = jnp.dot(rows_all, qkv_local[1], preferred_element_type=f32) + shift_local[1]
    value_raw = jnp.dot(rows_all, qkv_local[2], preferred_element_type=f32) + shift_local[2]
    query = rotate(query_raw.reshape(seq_len, local_heads, HEAD_DIM), cos_all, sin_all).astype(bf16)
    keys_b = rotate(key_raw.reshape(seq_len, local_heads, HEAD_DIM), cos_all, sin_all).astype(bf16)
    values_b = value_raw.reshape(seq_len, local_heads, HEAD_DIM).astype(bf16)
    query_block = min(512, seq_len)
    block_count = seq_len // query_block
    query_blocks = query.reshape(block_count, query_block, local_heads, HEAD_DIM)
    pos_blocks = all_pos.reshape(block_count, query_block)

    def forward_block(inputs):
        query_blk, pos_blk = inputs
        scores = (
            jnp.einsum("rhd,nhd->hrn", query_blk, keys_b, preferred_element_type=f32) * score_scale
        )
        visible = all_pos[None, None, :] <= pos_blk[None, :, None]
        scores = jnp.where(visible, scores, neg_big)
        peak = jnp.max(scores, axis=-1)
        probs = jnp.where(visible, jnp.exp(scores - peak[..., None]), 0.0)
        total = jnp.sum(probs, axis=-1)
        accum = jnp.einsum("hrn,nhd->rhd", probs.astype(bf16), values_b, preferred_element_type=f32)
        return ((accum / total.T[:, :, None]).astype(bf16), peak + jnp.log(total))

    attn_blocks, lse_blocks = lax.map(forward_block, (query_blocks, pos_blocks))
    attn_local = attn_blocks.reshape(seq_len, width_local)
    residual_stream, mlp_all = attn_out(attn_local, out_local, block_input, mlp_norm_gain, mlp_norm_bias)
    gate_val = jnp.dot(mlp_all, gateup_local[0], preferred_element_type=f32)
    up_val = jnp.dot(mlp_all, gateup_local[1], preferred_element_type=f32)
    sigma = jax.nn.sigmoid(gate_val)
    hidden_b = (gate_val * sigma * up_val).astype(bf16)
    hidden_grad = jnp.dot(cot_all, down_local.T, preferred_element_type=f32)
    gate_grad = (hidden_grad * up_val * sigma * (1.0 + gate_val * (1.0 - sigma))).astype(bf16)
    up_grad = (hidden_grad * gate_val * sigma).astype(bf16)
    down_w_grad = jnp.dot(hidden_b.T, cot_all, preferred_element_type=f32)
    gateup_w_grad = jnp.einsum(
        "td,ktf->kdf", mlp_all, jnp.stack([gate_grad, up_grad]), preferred_element_type=f32
    )
    gateup_grads, down_grads = shard_pair(gateup_w_grad, down_w_grad)
    resid_grad, second_vectors, resid_all = mlp_back(
        gate_grad, up_grad, gateup_local, residual_stream, out_cotangent, mlp_norm_gain
    )
    out_w_grad = jnp.dot(attn_local.T, resid_all, preferred_element_type=f32)
    attn_val_grad = jnp.dot(resid_all, out_local.T, preferred_element_type=f32).reshape(
        seq_len, local_heads, HEAD_DIM
    )
    delta = jnp.sum(
        attn_val_grad * attn_local.reshape(seq_len, local_heads, HEAD_DIM).astype(f32), axis=-1
    )
    attn_grad_b = attn_val_grad.astype(bf16)

    def backward_block(carry, inputs):
        key_grad, value_grad = carry
        query_blk, pos_blk, lse_blk, grad_blk, delta_blk = inputs
        scores = (
            jnp.einsum("rhd,nhd->hrn", query_blk, keys_b, preferred_element_type=f32) * score_scale
        )
        visible = all_pos[None, None, :] <= pos_blk[None, :, None]
        scores = jnp.where(visible, scores, neg_big)
        probs = jnp.where(visible, jnp.exp(scores - lse_blk[..., None]), 0.0)
        value_grad = value_grad + jnp.einsum(
            "hrn,rhd->nhd", probs.astype(bf16), grad_blk, preferred_element_type=f32
        )
        prob_grad = jnp.einsum("rhd,nhd->hrn", grad_blk, values_b, preferred_element_type=f32)
        score_grad = (probs * (prob_grad - delta_blk.T[:, :, None])).astype(bf16)
        query_grad_blk = (
            jnp.einsum("hrn,nhd->rhd", score_grad, keys_b, preferred_element_type=f32) * score_scale
        )
        key_grad = (
            key_grad
            + jnp.einsum("hrn,rhd->nhd", score_grad, query_blk, preferred_element_type=f32)
            * score_scale
        )
        return ((key_grad, value_grad), query_grad_blk)

    zero_kv = jnp.zeros((seq_len, local_heads, HEAD_DIM), f32)
    (key_grad, value_grad), query_grads = lax.scan(
        backward_block,
        (zero_kv, zero_kv),
        (
            query_blocks,
            pos_blocks,
            lse_blocks,
            attn_grad_b.reshape(block_count, query_block, local_heads, HEAD_DIM),
            delta.reshape(block_count, query_block, local_heads),
        ),
    )
    query_grad = query_grads.reshape(seq_len, local_heads, HEAD_DIM)
    grad_parts = jnp.stack(
        [
            unrotate(query_grad, cos_all, sin_all).reshape(seq_len, width_local),
            unrotate(key_grad, cos_all, sin_all).reshape(seq_len, width_local),
            value_grad.reshape(seq_len, width_local),
        ],
        axis=0,
    )
    shift_part = jnp.sum(grad_parts, axis=1)
    shift_grad = lax.dynamic_update_slice_in_dim(jnp.zeros((3, D), f32), shift_part, head_first, 1)
    grad_parts_b = grad_parts.astype(bf16)
    qkv_w_grad = jnp.einsum("td,ktc->kdc", rows_all, grad_parts_b, preferred_element_type=f32)
    qkv_grads, out_grads = shard_pair(qkv_w_grad, out_w_grad)
    input_grad, first_vectors = attn_back(grad_parts_b, qkv_local, block_input, resid_grad, attn_norm_gain)
    hidden_late, first_vectors = lax.optimization_barrier((hidden_b, first_vectors))
    block_output = down(hidden_late, down_local, residual_stream)
    small = sum_vectors(
        jnp.concatenate([first_vectors, second_vectors, shift_grad, jnp.zeros((1, D), f32)], axis=0)
    )
    return (
        block_output,
        input_grad,
        small[0],
        small[1],
        qkv_grads,
        small[4:7],
        out_grads,
        small[2],
        small[3],
        gateup_grads,
        down_grads,
    )


def solution(mesh):
    return jax.shard_map(
        per_device,
        mesh=mesh,
        in_specs=(
            P(("dp", "ctx"), None),
            P(("dp", "ctx"), None),
            P("dp", None),
            P(),
            P(),
            P(None, "dp", "ctx"),
            P(),
            P("ctx", "dp"),
            P(),
            P(),
            P(None, "dp", "ctx"),
            P("ctx", "dp"),
        ),
        out_specs=(
            P(("dp", "ctx"), None),
            P(("dp", "ctx"), None),
            P(),
            P(),
            P(None, "dp", "ctx"),
            P(),
            P("ctx", "dp"),
            P(),
            P(),
            P(None, "dp", "ctx"),
            P("ctx", "dp"),
        ),
        check_vma=False,
    )
```

```python
import functools
import math

import jax
import jax.numpy as jnp
from jax import lax
from jax.experimental import pallas as pl
from jax.experimental.pallas import tpu as pltpu
from jax.sharding import PartitionSpec as P

MESH = pl.DeviceIdType.MESH
VMEM = pl.BlockSpec(memory_space=pltpu.VMEM)
ANY = pl.BlockSpec(memory_space=pl.ANY)
DMA = pltpu.SemaphoreType.DMA

D = 2048
HEADS = 32
HEAD_DIM = 64
ROT = 16


eps_norm = 1e-05
rope_base = 10000.0
neg_big = -1e30


class Place:
    def __init__(self):
        self.ndp = lax.axis_size("dp")
        self.nctx = lax.axis_size("ctx")
        self.nchip = self.nctx // 2
        self.z = lax.axis_index("dp")
        self.c = lax.axis_index("ctx")
        self.p = lax.div(self.c, 2)
        self.k = lax.rem(self.c, 2)

    def chip(self, offset):
        return lax.rem(self.p + offset, self.nchip)

    def at(self, c):
        return {"dp": self.z, "ctx": c}

    def partner(self):
        return self.at(2 * self.p + 1 - self.k)

    def same_core(self, q):
        return self.at(2 * q + self.k)


def greet(place, along_ctx=True, along_dp=False, all_ctx=False):
    barrier = pltpu.get_barrier_semaphore()
    peers = []
    if all_ctx:
        peers += [place.at(lax.rem(place.c + i, place.nctx)) for i in range(1, place.nctx)]
    elif along_ctx:
        peers += [place.partner()] + [place.same_core(place.chip(i)) for i in range(1, place.nchip)]
    if along_dp:
        peers += [{"dp": lax.rem(place.z + i, place.ndp), "ctx": place.c} for i in range(1, place.ndp)]
    for peer in peers:
        pl.semaphore_signal(barrier, inc=1, device_id=peer, device_id_type=MESH)
    pl.semaphore_wait(barrier, len(peers))


def push(src, dst, send, recv, device):
    return pltpu.make_async_remote_copy(
        src_ref=src, dst_ref=dst, send_sem=send, recv_sem=recv, device_id=device, device_id_type=MESH
    )


class RowGather:
    def __init__(self, place, block, whole, send, recv, local):
        self.place, self.block, self.whole = place, block, whole
        self.send, self.recv, self.local = send, recv, local
        self.rows = block.shape[0]

    def slot(self, c):
        return self.whole.at[pl.ds(pl.multiple_of(c * self.rows, self.rows), self.rows)]

    def direct(self, i):
        place = self.place
        q = place.chip(i)
        return push(self.block, self.slot(place.c), self.send.at[i], self.recv.at[place.c], place.same_core(q))

    def own(self):
        place = self.place
        return push(self.block, self.slot(place.c), self.send.at[0], self.recv.at[place.c], place.partner())

    def passed(self, i):
        place = self.place
        c = 2 * place.chip(i) + place.k
        return push(
            self.slot(c), self.slot(c), self.send.at[place.nchip + i - 1], self.recv.at[c], place.partner()
        )

    def arrival(self, c):
        return push(self.block, self.slot(c), self.send.at[0], self.recv.at[c], self.place.partner())

    def keep(self):
        return pltpu.make_async_copy(self.block, self.slot(self.place.c), self.local)

    def start(self):
        for i in range(1, self.place.nchip):
            self.direct(i).start()
        self.own().start()
        self.keep().start()

    def forward(self):
        place = self.place
        for i in range(1, place.nchip):
            self.arrival(2 * place.chip(i) + place.k).wait_recv()
            self.passed(i).start()

    def finish(self):
        place = self.place
        for i in range(place.nchip):
            self.arrival(2 * place.chip(i) + 1 - place.k).wait_recv()
        self.own().wait_send()
        for i in range(1, place.nchip):
            self.direct(i).wait_send()
            self.passed(i).wait_send()
        self.keep().wait()


def gather_sems(nctx):
    return [DMA((nctx,)), DMA((nctx,)), DMA]


class DepthGather:
    def __init__(self, place, piece, whole, where, send, recv, local):
        self.place, self.piece, self.whole, self.where = place, piece, whole, where
        self.send, self.recv, self.local = send, recv, local
        self.line = place.ndp == 4
        self.middle = jnp.logical_or(place.z == 1, place.z == 2)
        self.far = 6 - 3 * place.z

    def copy(self, src, z_src, z_dst, sem):
        return push(
            src, self.where(self.whole, z_src), self.send.at[sem], self.recv.at[z_src], {"dp": z_dst, "ctx": self.place.c}
        )

    def directs(self):
        z, n = self.place.z, self.place.ndp
        if not self.line:
            return [(None, self.copy(self.piece, z, lax.rem(z + i, n), i - 1)) for i in range(1, n)]
        out = []
        for sem, step in enumerate((2, -2, 1, -1)):
            d = z + step
            ok = jnp.logical_and(d >= 0, d < 4)
            out.append((ok, self.copy(self.piece, z, jnp.clip(d, 0, 3), sem)))
        return out

    def keep(self):
        return pltpu.make_async_copy(self.piece, self.where(self.whole, self.place.z), self.local)

    def start(self):
        for ok, copy in self.directs():
            if ok is None:
                copy.start()
            else:
                pl.when(ok)(copy.start)
        self.keep().start()

    def passed(self):
        far = jnp.clip(self.far, 0, 3)
        return self.copy(self.where(self.whole, far), far, jnp.clip(3 * (self.place.z - 1), 0, 3), 4)

    def forward(self):
        if self.line:

            @pl.when(self.middle)
            def _():
                far = jnp.clip(self.far, 0, 3)
                self.copy(self.piece, far, far, 4).wait_recv()
                self.passed().start()

    def finish(self):
        z, n = self.place.z, self.place.ndp
        for i in range(1, n):
            src = lax.rem(z + i, n)
            wait = self.copy(self.piece, src, src, 0).wait_recv
            if self.line:
                pl.when(jnp.logical_not(jnp.logical_and(self.middle, src == self.far)))(wait)
            else:
                wait()
        for ok, copy in self.directs():
            if ok is None:
                copy.wait_send()
            else:
                pl.when(ok)(copy.wait_send)
        if self.line:
            pl.when(self.middle)(self.passed().wait_send)
        self.keep().wait()


def depth_sems(ndp):
    return [DMA((ndp + 1,)), DMA((ndp,)), DMA]


STEP = 16


def row_loop(rows, body):
    def step(i, carry):
        body(pl.ds(pl.multiple_of(i * STEP, STEP), STEP))
        return carry

    lax.fori_loop(0, rows // STEP, step, 0)


def normal(values):
    centred = values - jnp.mean(values, axis=-1, keepdims=True)
    rscale = lax.rsqrt(jnp.mean(centred * centred, axis=-1, keepdims=True) + eps_norm)
    return centred * rscale, rscale


def normal_back(grad_out, normed, rscale, gain):
    scaled = grad_out * gain
    return rscale * (
        scaled
        - jnp.mean(scaled, axis=-1, keepdims=True)
        - normed * jnp.mean(scaled * normed, axis=-1, keepdims=True)
    )


def gather_kernel(
    x_ref, cot_ref, gain_ref, bias_ref, qkv_ref, out_ref,
    rows_all, cot_all, qkv_all, out_all,
    row_block, cot_block, *sems
):
    place = Place()
    greet(place, along_dp=True)
    depth = qkv_ref.shape[1]
    width = out_ref.shape[1]

    def qkv_at(ref, z):
        return ref.at[:, pl.ds(pl.multiple_of(z * depth, depth), depth), :]

    def out_at(ref, z):
        return ref.at[:, pl.ds(pl.multiple_of(z * width, width), width)]

    qkv = DepthGather(place, qkv_ref, qkv_all, qkv_at, *sems[0:3])
    out = DepthGather(place, out_ref, out_all, out_at, *sems[3:6])
    rows = RowGather(place, row_block, rows_all, *sems[6:9])
    cots = RowGather(place, cot_block, cot_all, *sems[9:12])
    qkv.start()
    out.start()
    gain, bias = gain_ref[...].astype(jnp.float32), bias_ref[...].astype(jnp.float32)

    def norm(at):
        normed, _ = normal(x_ref[at, :].astype(jnp.float32))
        row_block[at, :] = (normed * gain + bias).astype(jnp.bfloat16)
        cot_block[at, :] = cot_ref[at, :].astype(jnp.bfloat16)

    row_loop(x_ref.shape[0], norm)
    rows.start()
    cots.start()
    rows.forward()
    qkv.forward()
    cots.forward()
    out.forward()
    rows.finish()
    cots.finish()
    qkv.finish()
    out.finish()


def gather_inputs(x, cot, gain, bias, qkv, out):
    ndp, nctx = lax.axis_size("dp"), lax.axis_size("ctx")
    rows, d = x.shape
    bf16 = jnp.bfloat16
    return pl.pallas_call(
        gather_kernel,
        out_shape=(
            jax.ShapeDtypeStruct((rows * nctx, d), bf16),
            jax.ShapeDtypeStruct((rows * nctx, d), bf16),
            jax.ShapeDtypeStruct((qkv.shape[0], qkv.shape[1] * ndp, qkv.shape[2]), bf16),
            jax.ShapeDtypeStruct((out.shape[0], out.shape[1] * ndp), bf16),
        ),
        in_specs=[VMEM] * 6,
        out_specs=(ANY,) * 4,
        scratch_shapes=[pltpu.VMEM((rows, d), bf16), pltpu.VMEM((rows, d), bf16)]
        + depth_sems(ndp) * 2
        + gather_sems(nctx) * 2,
        compiler_params=pltpu.CompilerParams(collective_id=0, has_side_effects=True),
        cost_estimate=pl.CostEstimate(flops=0, bytes_accessed=200_000_000, transcendentals=0),
        name="gather_inputs",
    )(x, cot, gain[None, :], bias[None, :], qkv, out)


class SumScatter:
    TILE = 512

    def __init__(self, place, rows, product, mine, to_pair, from_pair, to_chip, from_chip, sems):
        self.place, self.rows, self.product = place, rows, product
        self.mine, self.to_pair, self.from_pair = mine, to_pair, from_pair
        self.to_chip, self.from_chip = to_chip, from_chip
        self.pair_send, self.pair_recv, self.chip_send, self.chip_recv = sems

    def pair(self, i):
        return push(
            self.to_pair.at[i], self.from_pair.at[i], self.pair_send.at[i], self.pair_recv.at[i], self.place.partner()
        )

    def chips(self, i):
        return push(
            self.to_chip.at[i],
            self.from_chip.at[i],
            self.chip_send.at[i],
            self.chip_recv.at[i],
            self.place.same_core(self.place.chip(i + 1)),
        )

    def run(self):
        place, rows, tile = self.place, self.rows, self.TILE
        nchip = place.nchip
        width = self.mine.shape[-1]

        def hand_on(i):
            self.pair(i).wait_recv()

            def add(at):
                both = self.mine[i, at, :] + self.from_pair[i, at, :].astype(jnp.float32)
                self.to_chip[i, at, :] = both.astype(jnp.bfloat16)

            row_loop(rows, add)
            self.chips(i).start()

        def step(i, carry):
            q = lax.rem(place.p + 1 + i, nchip)
            first = pl.multiple_of(q * 2 * rows, 2 * rows)

            def columns(j, inner):
                cols = pl.ds(pl.multiple_of(j * tile, tile), tile)
                part = self.product(pl.ds(first, 2 * rows), cols)

                @pl.when(place.k == 0)
                def _():
                    self.mine[i, :, cols] = part[:rows]
                    self.to_pair[i, :, cols] = part[rows:].astype(jnp.bfloat16)

                @pl.when(place.k == 1)
                def _():
                    self.mine[i, :, cols] = part[rows:]
                    self.to_pair[i, :, cols] = part[:rows].astype(jnp.bfloat16)

                return inner

            lax.fori_loop(0, width // tile, columns, 0)
            self.pair(i).start()
            pl.when(i > 0)(lambda: hand_on(i - 1))
            return carry

        lax.fori_loop(0, nchip, step, 0)
        self.pair(nchip - 1).wait_recv()
        for i in range(nchip - 1):
            self.chips(i).wait_recv()

    def total(self, at):
        last = self.place.nchip - 1
        value = self.mine[last, at, :] + self.from_pair[last, at, :].astype(jnp.float32)
        for i in range(last):
            value = value + self.from_chip[i, at, :].astype(jnp.float32)
        return value

    def finish(self):
        for i in range(self.place.nchip):
            self.pair(i).wait_send()
        for i in range(self.place.nchip - 1):
            self.chips(i).wait_send()


def scatter_scratch(nctx, rows, d):
    n = nctx // 2
    bf16 = jnp.bfloat16
    return [
        pltpu.VMEM((n, rows, d), jnp.float32),
        pltpu.VMEM((n, rows, d), bf16),
        pltpu.VMEM((n, rows, d), bf16),
        pltpu.VMEM((n - 1, rows, d), bf16),
        pltpu.VMEM((n - 1, rows, d), bf16),
        DMA((n,)),
        DMA((n,)),
        DMA((n - 1,)),
        DMA((n - 1,)),
    ]


def dot_nn(a, b):
    return jnp.dot(a, b, preferred_element_type=jnp.float32)


def dot_nt(a, b):
    return lax.dot_general(a, b, (((1,), (1,)), ((), ())), preferred_element_type=jnp.float32)


def attn_out_kernel(attn_ref, w_ref, x_ref, gain_ref, bias_ref, resid_ref, normed_all, block, *scratch):
    place = Place()
    greet(place)
    scatter = SumScatter(
        place,
        x_ref.shape[0],
        lambda rows, cols: dot_nn(attn_ref[rows, :], w_ref[:, cols]),
        *scratch[:5],
        scratch[5:9],
    )
    scatter.run()
    gain, bias = gain_ref[...].astype(jnp.float32), bias_ref[...].astype(jnp.float32)

    def norm(at):
        resid = x_ref[at, :].astype(jnp.float32) + scatter.total(at)
        resid_ref[at, :] = resid
        normed, _ = normal(resid)
        block[at, :] = (normed * gain + bias).astype(jnp.bfloat16)

    row_loop(x_ref.shape[0], norm)
    rows = RowGather(place, block, normed_all, *scratch[9:12])
    rows.start()
    rows.forward()
    rows.finish()
    scatter.finish()


def attn_out(attn, w, x, gain, bias):
    nctx = lax.axis_size("ctx")
    rows, d = x.shape
    return pl.pallas_call(
        attn_out_kernel,
        out_shape=(
            jax.ShapeDtypeStruct((rows, d), jnp.float32),
            jax.ShapeDtypeStruct((rows * nctx, d), jnp.bfloat16),
        ),
        in_specs=[VMEM] * 5,
        out_specs=(VMEM, ANY),
        scratch_shapes=[pltpu.VMEM((rows, d), jnp.bfloat16)]
        + scatter_scratch(nctx, rows, d)
        + gather_sems(nctx),
        compiler_params=pltpu.CompilerParams(collective_id=1, has_side_effects=True),
        cost_estimate=pl.CostEstimate(flops=0, bytes_accessed=150_000_000, transcendentals=0),
        name="attn_out",
    )(attn, w, x, gain[None, :], bias[None, :])


def mlp_back_kernel(
    gate_ref, up_ref, w_ref, resid_ref, cot_ref, gain_ref, grad_ref, vec_ref, grad_all, block, *scratch
):
    place = Place()
    greet(place)
    scatter = SumScatter(
        place,
        resid_ref.shape[0],
        lambda rows, cols: dot_nt(gate_ref[rows, :], w_ref[0, cols, :]) + dot_nt(up_ref[rows, :], w_ref[1, cols, :]),
        *scratch[:5],
        scratch[5:9],
    )
    scatter.run()
    gain = gain_ref[...].astype(jnp.float32)
    vec_ref[...] = jnp.zeros_like(vec_ref)

    def back(at):
        grad = scatter.total(at)
        normed, rscale = normal(resid_ref[at, :])
        vec_ref[0:1, :] += jnp.sum(grad * normed, axis=0, keepdims=True)
        vec_ref[1:2, :] += jnp.sum(grad, axis=0, keepdims=True)
        out = cot_ref[at, :] + normal_back(grad, normed, rscale, gain)
        grad_ref[at, :] = out
        block[at, :] = out.astype(jnp.bfloat16)

    row_loop(resid_ref.shape[0], back)
    rows = RowGather(place, block, grad_all, *scratch[9:12])
    rows.start()
    rows.forward()
    rows.finish()
    scatter.finish()


def mlp_back(gate_grad, up_grad, w, resid, cot, gain):
    nctx = lax.axis_size("ctx")
    rows, d = resid.shape
    return pl.pallas_call(
        mlp_back_kernel,
        out_shape=(
            jax.ShapeDtypeStruct((rows, d), jnp.float32),
            jax.ShapeDtypeStruct((2, d), jnp.float32),
            jax.ShapeDtypeStruct((rows * nctx, d), jnp.bfloat16),
        ),
        in_specs=[VMEM] * 6,
        out_specs=(VMEM, VMEM, ANY),
        scratch_shapes=[pltpu.VMEM((rows, d), jnp.bfloat16)]
        + scatter_scratch(nctx, rows, d)
        + gather_sems(nctx),
        compiler_params=pltpu.CompilerParams(collective_id=2, has_side_effects=True),
        cost_estimate=pl.CostEstimate(flops=0, bytes_accessed=150_000_000, transcendentals=0),
        name="mlp_back",
    )(gate_grad, up_grad, w, resid, cot, gain[None, :])


def attn_back_kernel(parts_ref, w_ref, x_ref, grad_ref, gain_ref, out_ref, vec_ref, *scratch):
    place = Place()
    greet(place)

    def product(rows, cols):
        part = dot_nt(parts_ref[0, rows, :], w_ref[0, cols, :])
        part = part + dot_nt(parts_ref[1, rows, :], w_ref[1, cols, :])
        return part + dot_nt(parts_ref[2, rows, :], w_ref[2, cols, :])

    scatter = SumScatter(place, x_ref.shape[0], product, *scratch[:5], scratch[5:9])
    scatter.run()
    gain = gain_ref[...].astype(jnp.float32)
    vec_ref[...] = jnp.zeros_like(vec_ref)

    def back(at):
        grad = scatter.total(at)
        normed, rscale = normal(x_ref[at, :].astype(jnp.float32))
        vec_ref[0:1, :] += jnp.sum(grad * normed, axis=0, keepdims=True)
        vec_ref[1:2, :] += jnp.sum(grad, axis=0, keepdims=True)
        out_ref[at, :] = grad_ref[at, :] + normal_back(grad, normed, rscale, gain)

    row_loop(x_ref.shape[0], back)
    scatter.finish()


def attn_back(parts, w, x, grad, gain):
    nctx = lax.axis_size("ctx")
    rows, d = x.shape
    return pl.pallas_call(
        attn_back_kernel,
        out_shape=(
            jax.ShapeDtypeStruct((rows, d), jnp.float32),
            jax.ShapeDtypeStruct((2, d), jnp.float32),
        ),
        in_specs=[VMEM] * 5,
        out_specs=(VMEM, VMEM),
        scratch_shapes=scatter_scratch(nctx, rows, d),
        compiler_params=pltpu.CompilerParams(collective_id=3, has_side_effects=True),
        cost_estimate=pl.CostEstimate(flops=0, bytes_accessed=100_000_000, transcendentals=0),
        name="attn_back",
    )(parts, w, x, grad, gain[None, :])


def down_kernel(hidden_ref, w_ref, resid_ref, out_ref, *scratch):
    place = Place()
    greet(place)
    scatter = SumScatter(
        place,
        resid_ref.shape[0],
        lambda rows, cols: dot_nn(hidden_ref[rows, :], w_ref[:, cols]),
        *scratch[:5],
        scratch[5:9],
    )
    scatter.run()

    def add(at):
        out_ref[at, :] = (resid_ref[at, :] + scatter.total(at)).astype(jnp.bfloat16)

    row_loop(resid_ref.shape[0], add)
    scatter.finish()


def down(hidden, w, resid):
    nctx = lax.axis_size("ctx")
    rows, d = resid.shape
    return pl.pallas_call(
        down_kernel,
        out_shape=jax.ShapeDtypeStruct((rows, d), jnp.bfloat16),
        in_specs=[VMEM] * 3,
        out_specs=VMEM,
        scratch_shapes=scatter_scratch(nctx, rows, d),
        compiler_params=pltpu.CompilerParams(collective_id=4, has_side_effects=True),
        cost_estimate=pl.CostEstimate(flops=0, bytes_accessed=100_000_000, transcendentals=0),
        name="down_sum",
    )(hidden, w, resid)


def vectors_kernel(v_ref, out_ref, from_ctx, from_dp, plane, ctx_send, ctx_recv, dp_send, dp_recv):
    place = Place()
    greet(place, all_ctx=True, along_dp=True)
    nctx, ndp, c, z = place.nctx, place.ndp, place.c, place.z

    def across(i):
        return push(
            v_ref, from_ctx.at[c], ctx_send.at[i - 1], ctx_recv.at[c], place.at(lax.rem(c + i, nctx))
        )

    def along(i):
        return push(
            plane, from_dp.at[z], dp_send.at[i - 1], dp_recv.at[z], {"dp": lax.rem(z + i, ndp), "ctx": c}
        )

    for i in range(1, nctx):
        across(i).start()
    from_ctx[c] = v_ref[...]
    for i in range(1, nctx):
        s = lax.rem(c + i, nctx)
        push(v_ref, from_ctx.at[s], ctx_send.at[0], ctx_recv.at[s], place.at(s)).wait_recv()
    value = from_ctx[0]
    for i in range(1, nctx):
        value = value + from_ctx[i]
    plane[...] = value
    for i in range(1, ndp):
        along(i).start()
    from_dp[z] = value
    for i in range(1, ndp):
        s = lax.rem(z + i, ndp)
        push(plane, from_dp.at[s], dp_send.at[0], dp_recv.at[s], {"dp": s, "ctx": c}).wait_recv()
    value = from_dp[0]
    for i in range(1, ndp):
        value = value + from_dp[i]
    out_ref[...] = value
    for i in range(1, nctx):
        across(i).wait_send()
    for i in range(1, ndp):
        along(i).wait_send()


def sum_vectors(v):
    ndp, nctx = lax.axis_size("dp"), lax.axis_size("ctx")
    f32 = jnp.float32
    return pl.pallas_call(
        vectors_kernel,
        out_shape=jax.ShapeDtypeStruct(v.shape, f32),
        in_specs=[VMEM],
        out_specs=VMEM,
        scratch_shapes=[
            pltpu.VMEM((nctx,) + v.shape, f32),
            pltpu.VMEM((ndp,) + v.shape, f32),
            pltpu.VMEM(v.shape, f32),
            DMA((nctx - 1,)),
            DMA((nctx,)),
            DMA((ndp - 1,)),
            DMA((ndp,)),
        ],
        compiler_params=pltpu.CompilerParams(collective_id=5, has_side_effects=True),
        cost_estimate=pl.CostEstimate(flops=0, bytes_accessed=30_000_000, transcendentals=0),
        name="sum_vectors",
    )(v)


HALF = ROT // 2
PAIR = 256


def tiles(count, body):
    def step(i, carry):
        body(i)
        return carry

    lax.fori_loop(0, count, step, 0)


def span(i, size):
    return pl.ds(pl.multiple_of(i * size, size), size)


def turn(columns, cosine, sine, heads):
    out = []
    for h in range(heads):
        at = h * HEAD_DIM
        a, b = columns[at : at + HALF], columns[at + HALF : at + ROT]
        out += [a * cosine - b * sine, b * cosine + a * sine, columns[at + ROT : at + HEAD_DIM]]
    return jnp.concatenate(out, axis=0)


def attend(rows_ref, w_ref, shift_ref, cos_ref, sin_ref, pos_col, pos_row, q_t, k_t, v_t, attn_t, lse, k_n, bias, attn):
    seq = rows_ref.shape[0]
    width = w_ref.shape[2]
    heads = width // HEAD_DIM
    bf16 = jnp.bfloat16

    def project(t):
        at = span(t, PAIR)
        cosine, sine = cos_ref[:, at], sin_ref[:, at]
        for i, ref in enumerate((q_t, k_t, v_t)):
            raw = (dot_nn(rows_ref[at, :], w_ref[i]) + shift_ref[i : i + 1, :]).T
            if i < 2:
                raw = turn(raw, cosine, sine, heads)
            raw = raw.astype(bf16)
            if i == 0:
                raw = raw * jnp.asarray(1.0 / math.sqrt(HEAD_DIM), bf16)
            ref[:, at] = raw

    tiles(seq // PAIR, project)
    for h in range(heads):
        k_n[h] = k_t[h * HEAD_DIM : (h + 1) * HEAD_DIM, :].T

    def queries(t):
        at = span(t, PAIR)
        bias[...] = jnp.where(pos_col[...] <= pos_row[:, at], 0.0, neg_big)

        for h in range(heads):
            feats = slice(h * HEAD_DIM, (h + 1) * HEAD_DIM)
            scores = dot_nn(k_n[h], q_t[feats, at]) + bias[...]
            peak = jnp.max(scores, axis=0, keepdims=True)
            probs = jnp.exp(scores - peak)
            total = jnp.sum(probs, axis=0, keepdims=True)
            out = dot_nn(v_t[feats, :], probs.astype(bf16)) / total
            attn_t[feats, at] = out.astype(bf16)
            lse[h : h + 1, at] = peak + jnp.log(total)
        attn[at, :] = attn_t[:, at].T

    tiles(seq // PAIR, queries)


def attend_kernel(rows_ref, w_ref, shift_ref, cos_ref, sin_ref, pos_col, pos_row, *rest):
    attend(rows_ref, w_ref, shift_ref, cos_ref, sin_ref, pos_col, pos_row, *rest[:5], rest[6], rest[7], rest[5])


def attention(rows_all, w, shift, cosine, sine, pos_col, pos_row):
    seq, width = rows_all.shape[0], w.shape[2]
    bf16 = jnp.bfloat16
    heads = width // HEAD_DIM
    return pl.pallas_call(
        attend_kernel,
        out_shape=tuple(jax.ShapeDtypeStruct((width, seq), bf16) for _ in range(4))
        + (jax.ShapeDtypeStruct((8, seq), jnp.float32), jax.ShapeDtypeStruct((seq, width), bf16)),
        in_specs=[VMEM] * 7,
        out_specs=(VMEM,) * 6,
        scratch_shapes=[pltpu.VMEM((heads, seq, HEAD_DIM), bf16), pltpu.VMEM((seq, PAIR), jnp.float32)],
        cost_estimate=pl.CostEstimate(flops=0, bytes_accessed=40_000_000, transcendentals=0),
        name="attention",
    )(rows_all, w, shift, cosine, sine, pos_col, pos_row)


def attend_back_kernel(
    grad_ref, w_ref, rows_ref, cos_ref, sin_ref, pos_col, pos_row, q_t, k_t, v_t, attn_t, lse,
    parts_ref, sums_ref, w_grads, g_t, delta, q_grad, kv_grad, bias, flat
):
    seq, d = grad_ref.shape
    width = w_ref.shape[0]
    heads = width // HEAD_DIM
    bf16, f32 = jnp.bfloat16, jnp.float32

    def first(t):
        at = span(t, PAIR)
        grad = dot_nt(w_ref[...], grad_ref[at, :])
        both = grad * attn_t[:, at].astype(f32)
        for h in range(heads):
            delta[h : h + 1, at] = jnp.sum(both[h * HEAD_DIM : (h + 1) * HEAD_DIM], axis=0, keepdims=True)
        g_t[:, at] = grad.astype(bf16)

    tiles(seq // PAIR, first)
    q_grad[...] = jnp.zeros_like(q_grad)

    def keys(t):
        at = span(t, PAIR)
        bias[...] = jnp.where(pos_col[at, :] <= pos_row[...], 0.0, neg_big)
        for h in range(heads):
            feats = slice(h * HEAD_DIM, (h + 1) * HEAD_DIM)
            keys_t = k_t[feats, at]
            probs = jnp.exp(dot_nn(keys_t.T, q_t[feats, :]) + bias[...] - lse[h : h + 1, :])
            kv_grad[1, feats, at] = dot_nt(g_t[feats, :], probs.astype(bf16))
            back = dot_nn(v_t[feats, at].T, g_t[feats, :])
            scores = (probs * (back - delta[h : h + 1, :])).astype(bf16)
            kv_grad[0, feats, at] = dot_nt(q_t[feats, :], scores)
            q_grad[feats, :] += dot_nn(keys_t, scores)

    tiles(seq // PAIR, keys)
    sums_ref[...] = jnp.zeros_like(sums_ref)

    def part(t):
        at = span(t, PAIR)
        cosine, sine = cos_ref[:, at], sin_ref[:, at]
        for i in range(3):
            if i == 0:
                grad = turn(q_grad[:, at] * (1.0 / math.sqrt(HEAD_DIM)), cosine, -sine, heads)
            elif i == 1:
                grad = turn(kv_grad[0, :, at], cosine, -sine, heads)
            else:
                grad = kv_grad[1, :, at]
            natural = grad.T
            sums_ref[i : i + 1, :] += jnp.sum(natural, axis=0, keepdims=True)
            parts_ref[i, at, :] = natural.astype(bf16)
            flat[i, :, at] = grad.astype(bf16)

    tiles(seq // PAIR, part)

    def weights(j):
        cols = span(j, 2 * PAIR)
        rows = rows_ref[:, cols]
        for i in range(3):
            w_grads[i, cols, :] = dot_nn(flat[i], rows).T.astype(bf16)
        w_grads[3, cols, :] = dot_nn(attn_t[...], grad_ref[:, cols]).T.astype(bf16)

    tiles(d // (2 * PAIR), weights)


def attention_back(grad_all, w, rows_all, cosine, sine, pos_col, pos_row, q_t, k_t, v_t, attn_t, lse):
    seq, d = rows_all.shape
    width = w.shape[0]
    bf16, f32 = jnp.bfloat16, jnp.float32
    return pl.pallas_call(
        attend_back_kernel,
        out_shape=(
            jax.ShapeDtypeStruct((3, seq, width), bf16),
            jax.ShapeDtypeStruct((3, width), f32),
            jax.ShapeDtypeStruct((4, d, width), bf16),
        ),
        in_specs=[VMEM] * 12,
        out_specs=(VMEM,) * 3,
        scratch_shapes=[
            pltpu.VMEM((width, seq), bf16),
            pltpu.VMEM((8, seq), f32),
            pltpu.VMEM((width, seq), f32),
            pltpu.VMEM((2, width, seq), f32),
            pltpu.VMEM((PAIR, seq), f32),
            pltpu.VMEM((3, width, seq), bf16),
        ],
        cost_estimate=pl.CostEstimate(flops=0, bytes_accessed=120_000_000, transcendentals=0),
        name="attention_back",
    )(grad_all, w, rows_all, cosine, sine, pos_col, pos_row, q_t, k_t, v_t, attn_t, lse)


def rope_tables(positions):
    exponent = jnp.arange(HALF, dtype=jnp.float32) * (2.0 / ROT)
    inverse = jnp.exp(-exponent * math.log(rope_base))
    angle_val = inverse[:, None] * positions.astype(jnp.float32)[None, :]
    return (jnp.cos(angle_val), jnp.sin(angle_val))


def group_positions(group_order, count, half_group):
    row_ids = jnp.arange(count, dtype=jnp.int32)
    group_ids = row_ids // half_group
    matches = group_ids[:, None] == jnp.arange(group_order.shape[0], dtype=jnp.int32)[None, :]
    group_start = jnp.sum(jnp.where(matches, group_order[None, :], 0), axis=1)
    return group_start * half_group + row_ids % half_group


def shard(grad):
    return lax.psum_scatter(grad, "dp", scatter_dimension=1, tiled=True)


def per_device(
    block_input,
    out_cotangent,
    group_perm,
    attn_norm_gain,
    attn_norm_bias,
    qkv_weight,
    qkv_bias,
    out_weight,
    mlp_norm_gain,
    mlp_norm_bias,
    gateup_weight,
    down_weight,
):
    f32 = jnp.float32
    bf16 = jnp.bfloat16
    tok_rows = block_input.shape[0]
    cycle_size = lax.axis_size("ctx")
    cycle_index = lax.axis_index("ctx")
    seq_len = tok_rows * cycle_size
    half_group = tok_rows // 2
    group_order = group_perm[0]
    qkv_shift = qkv_bias.astype(f32)
    rows_all, cot_all, qkv_local, out_local = gather_inputs(
        block_input, out_cotangent, attn_norm_gain, attn_norm_bias, qkv_weight, out_weight
    )
    down_local = lax.all_gather(down_weight, "dp", axis=1, tiled=True)
    gateup_local = lax.all_gather(gateup_weight, "dp", axis=1, tiled=True)
    all_pos = group_positions(group_order, seq_len, half_group)
    cos_all, sin_all = rope_tables(all_pos)
    pos_f = all_pos.astype(f32)
    pos_col, pos_row = pos_f[:, None], pos_f[None, :]
    width_local = qkv_weight.shape[2]
    head_first = cycle_index * width_local
    shift_local = lax.dynamic_slice_in_dim(qkv_shift, head_first, width_local, 1)
    q_t, k_t, v_t, attn_t, lse, attn_local = attention(
        rows_all, qkv_local, shift_local, cos_all, sin_all, pos_col, pos_row
    )
    attn_local, down_local = lax.optimization_barrier((attn_local, down_local))
    residual_stream, mlp_all = attn_out(attn_local, out_local, block_input, mlp_norm_gain, mlp_norm_bias)
    gate_val = jnp.dot(mlp_all, gateup_local[0], preferred_element_type=f32)
    up_val = jnp.dot(mlp_all, gateup_local[1], preferred_element_type=f32)
    sigma = jax.nn.sigmoid(gate_val)
    hidden_b = (gate_val * sigma * up_val).astype(bf16)
    down_w_grad = jnp.dot(hidden_b.T, cot_all, preferred_element_type=f32).astype(bf16)
    down_local, down_w_grad = lax.optimization_barrier((down_local, down_w_grad))
    down_grads = shard(down_w_grad)
    hidden_grad = jnp.dot(cot_all, down_local.T, preferred_element_type=f32)
    gate_grad = (hidden_grad * up_val * sigma * (1.0 + gate_val * (1.0 - sigma))).astype(bf16)
    up_grad = (hidden_grad * gate_val * sigma).astype(bf16)
    gateup_w_grad = jnp.einsum(
        "td,ktf->kdf", mlp_all, jnp.stack([gate_grad, up_grad]), preferred_element_type=f32
    ).astype(bf16)
    gate_grad, up_grad, gateup_w_grad = lax.optimization_barrier((gate_grad, up_grad, gateup_w_grad))
    gateup_grads = shard(gateup_w_grad)
    resid_grad, second_vectors, resid_all = mlp_back(
        gate_grad, up_grad, gateup_local, residual_stream, out_cotangent, mlp_norm_gain
    )
    resid_all, down_grads = lax.optimization_barrier((resid_all, down_grads))
    grad_parts_b, shift_part, attn_grads = attention_back(
        resid_all, out_local, rows_all, cos_all, sin_all, pos_col, pos_row, q_t, k_t, v_t, attn_t, lse
    )
    shift_grad = lax.dynamic_update_slice_in_dim(jnp.zeros((3, D), f32), shift_part, head_first, 1)
    attn_grads = shard(attn_grads).astype(f32)
    input_grad, first_vectors = attn_back(grad_parts_b, qkv_local, block_input, resid_grad, attn_norm_gain)
    hidden_late, first_vectors, gateup_grads = lax.optimization_barrier((hidden_b, first_vectors, gateup_grads))
    block_output = down(hidden_late, down_local, residual_stream)
    small = sum_vectors(
        jnp.concatenate([first_vectors, second_vectors, shift_grad, jnp.zeros((1, D), f32)], axis=0)
    )
    return (
        block_output,
        input_grad,
        small[0],
        small[1],
        attn_grads[:3],
        small[4:7],
        attn_grads[3].T,
        small[2],
        small[3],
        gateup_grads.astype(f32),
        down_grads.astype(f32),
    )


def solution(mesh):
    return jax.shard_map(
        per_device,
        mesh=mesh,
        in_specs=(
            P(("dp", "ctx"), None),
            P(("dp", "ctx"), None),
            P("dp", None),
            P(),
            P(),
            P(None, "dp", "ctx"),
            P(),
            P("ctx", "dp"),
            P(),
            P(),
            P(None, "dp", "ctx"),
            P("ctx", "dp"),
        ),
        out_specs=(
            P(("dp", "ctx"), None),
            P(("dp", "ctx"), None),
            P(),
            P(),
            P(None, "dp", "ctx"),
            P(),
            P("ctx", "dp"),
            P(),
            P(),
            P(None, "dp", "ctx"),
            P("ctx", "dp"),
        ),
        check_vma=False,
    )
```

```python
import functools
import math

import jax
import jax.numpy as jnp
from jax import lax
from jax.experimental import pallas as pl
from jax.experimental.pallas import tpu as pltpu
from jax.sharding import PartitionSpec as P

MESH = pl.DeviceIdType.MESH
VMEM = pl.BlockSpec(memory_space=pltpu.VMEM)
ANY = pl.BlockSpec(memory_space=pl.ANY)
DMA = pltpu.SemaphoreType.DMA

D = 2048
HEADS = 32
HEAD_DIM = 64
ROT = 16


eps_norm = 1e-05
rope_base = 10000.0
neg_big = -1e30


class Place:
    def __init__(self):
        self.ndp = lax.axis_size("dp")
        self.nctx = lax.axis_size("ctx")
        self.nchip = self.nctx // 2
        self.z = lax.axis_index("dp")
        self.c = lax.axis_index("ctx")
        self.p = lax.div(self.c, 2)
        self.k = lax.rem(self.c, 2)

    def chip(self, offset):
        return lax.rem(self.p + offset, self.nchip)

    def at(self, c):
        return {"dp": self.z, "ctx": c}

    def partner(self):
        return self.at(2 * self.p + 1 - self.k)

    def same_core(self, q):
        return self.at(2 * q + self.k)


def greet(place, along_ctx=True, along_dp=False, all_ctx=False):
    barrier = pltpu.get_barrier_semaphore()
    peers = []
    if all_ctx:
        peers += [place.at(lax.rem(place.c + i, place.nctx)) for i in range(1, place.nctx)]
    elif along_ctx:
        peers += [place.partner()] + [place.same_core(place.chip(i)) for i in range(1, place.nchip)]
    if along_dp:
        peers += [{"dp": lax.rem(place.z + i, place.ndp), "ctx": place.c} for i in range(1, place.ndp)]
    for peer in peers:
        pl.semaphore_signal(barrier, inc=1, device_id=peer, device_id_type=MESH)
    pl.semaphore_wait(barrier, len(peers))


def push(src, dst, send, recv, device):
    return pltpu.make_async_remote_copy(
        src_ref=src, dst_ref=dst, send_sem=send, recv_sem=recv, device_id=device, device_id_type=MESH
    )


class RowGather:
    def __init__(self, place, block, whole, send, recv, local):
        self.place, self.block, self.whole = place, block, whole
        self.send, self.recv, self.local = send, recv, local
        self.rows = block.shape[0]

    def slot(self, c):
        return self.whole.at[pl.ds(pl.multiple_of(c * self.rows, self.rows), self.rows)]

    def direct(self, i):
        place = self.place
        q = place.chip(i)
        return push(self.block, self.slot(place.c), self.send.at[i], self.recv.at[place.c], place.same_core(q))

    def own(self):
        place = self.place
        return push(self.block, self.slot(place.c), self.send.at[0], self.recv.at[place.c], place.partner())

    def passed(self, i):
        place = self.place
        c = 2 * place.chip(i) + place.k
        return push(
            self.slot(c), self.slot(c), self.send.at[place.nchip + i - 1], self.recv.at[c], place.partner()
        )

    def arrival(self, c):
        return push(self.block, self.slot(c), self.send.at[0], self.recv.at[c], self.place.partner())

    def keep(self):
        return pltpu.make_async_copy(self.block, self.slot(self.place.c), self.local)

    def start(self):
        for i in range(1, self.place.nchip):
            self.direct(i).start()
        self.own().start()
        self.keep().start()

    def forward(self):
        place = self.place
        for i in range(1, place.nchip):
            self.arrival(2 * place.chip(i) + place.k).wait_recv()
            self.passed(i).start()

    def finish(self):
        place = self.place
        for i in range(place.nchip):
            self.arrival(2 * place.chip(i) + 1 - place.k).wait_recv()
        self.own().wait_send()
        for i in range(1, place.nchip):
            self.direct(i).wait_send()
            self.passed(i).wait_send()
        self.keep().wait()


def gather_sems(nctx):
    return [DMA((nctx,)), DMA((nctx,)), DMA]


class DepthGather:
    def __init__(self, place, piece, whole, where, send, recv, local):
        self.place, self.piece, self.whole, self.where = place, piece, whole, where
        self.send, self.recv, self.local = send, recv, local
        self.line = place.ndp == 4
        self.middle = jnp.logical_or(place.z == 1, place.z == 2)
        self.far = 6 - 3 * place.z

    def copy(self, src, z_src, z_dst, sem):
        return push(
            src, self.where(self.whole, z_src), self.send.at[sem], self.recv.at[z_src], {"dp": z_dst, "ctx": self.place.c}
        )

    def directs(self):
        z, n = self.place.z, self.place.ndp
        if not self.line:
            return [(None, self.copy(self.piece, z, lax.rem(z + i, n), i - 1)) for i in range(1, n)]
        out = []
        for sem, step in enumerate((2, -2, 1, -1)):
            d = z + step
            ok = jnp.logical_and(d >= 0, d < 4)
            out.append((ok, self.copy(self.piece, z, jnp.clip(d, 0, 3), sem)))
        return out

    def keep(self):
        return pltpu.make_async_copy(self.piece, self.where(self.whole, self.place.z), self.local)

    def start(self):
        for ok, copy in self.directs():
            if ok is None:
                copy.start()
            else:
                pl.when(ok)(copy.start)
        self.keep().start()

    def passed(self):
        far = jnp.clip(self.far, 0, 3)
        return self.copy(self.where(self.whole, far), far, jnp.clip(3 * (self.place.z - 1), 0, 3), 4)

    def forward(self):
        if self.line:

            @pl.when(self.middle)
            def _():
                far = jnp.clip(self.far, 0, 3)
                self.copy(self.piece, far, far, 4).wait_recv()
                self.passed().start()

    def finish(self):
        z, n = self.place.z, self.place.ndp
        for i in range(1, n):
            src = lax.rem(z + i, n)
            wait = self.copy(self.piece, src, src, 0).wait_recv
            if self.line:
                pl.when(jnp.logical_not(jnp.logical_and(self.middle, src == self.far)))(wait)
            else:
                wait()
        for ok, copy in self.directs():
            if ok is None:
                copy.wait_send()
            else:
                pl.when(ok)(copy.wait_send)
        if self.line:
            pl.when(self.middle)(self.passed().wait_send)
        self.keep().wait()


def depth_sems(ndp):
    return [DMA((ndp + 1,)), DMA((ndp,)), DMA]


STEP = 16


def row_loop(rows, body):
    def step(i, carry):
        body(pl.ds(pl.multiple_of(i * STEP, STEP), STEP))
        return carry

    lax.fori_loop(0, rows // STEP, step, 0)


def normal(values):
    centred = values - jnp.mean(values, axis=-1, keepdims=True)
    rscale = lax.rsqrt(jnp.mean(centred * centred, axis=-1, keepdims=True) + eps_norm)
    return centred * rscale, rscale


def normal_back(grad_out, normed, rscale, gain):
    scaled = grad_out * gain
    return rscale * (
        scaled
        - jnp.mean(scaled, axis=-1, keepdims=True)
        - normed * jnp.mean(scaled * normed, axis=-1, keepdims=True)
    )


class SumScatter:
    TILE = 512

    def __init__(self, place, rows, product, mine, to_pair, from_pair, to_chip, from_chip, sems):
        self.place, self.rows, self.product = place, rows, product
        self.mine, self.to_pair, self.from_pair = mine, to_pair, from_pair
        self.to_chip, self.from_chip = to_chip, from_chip
        self.pair_send, self.pair_recv, self.chip_send, self.chip_recv = sems

    def pair(self, i):
        return push(
            self.to_pair.at[lax.rem(i, 2)], self.from_pair.at[i], self.pair_send.at[i], self.pair_recv.at[i], self.place.partner()
        )

    def chips(self, i):
        return push(
            self.to_chip.at[i],
            self.from_chip.at[i],
            self.chip_send.at[i],
            self.chip_recv.at[i],
            self.place.same_core(self.place.chip(i + 1)),
        )

    def run(self):
        place, rows, tile = self.place, self.rows, self.TILE
        nchip = place.nchip
        width = self.mine.shape[-1]

        def hand_on(i):
            self.pair(i).wait_recv()

            def add(at):
                both = self.mine[lax.rem(i, 2), at, :] + self.from_pair[i, at, :].astype(jnp.float32)
                self.to_chip[i, at, :] = both.astype(jnp.bfloat16)

            row_loop(rows, add)
            self.chips(i).start()

        def step(i, carry):
            q = lax.rem(place.p + 1 + i, nchip)
            first = pl.multiple_of(q * 2 * rows, 2 * rows)
            slot = lax.rem(i, 2)
            pl.when(i >= 2)(lambda: self.pair(i - 2).wait_send())

            def columns(j, inner):
                cols = pl.ds(pl.multiple_of(j * tile, tile), tile)
                part = self.product(pl.ds(first, 2 * rows), cols)

                @pl.when(place.k == 0)
                def _():
                    self.mine[slot, :, cols] = part[:rows]
                    self.to_pair[slot, :, cols] = part[rows:].astype(jnp.bfloat16)

                @pl.when(place.k == 1)
                def _():
                    self.mine[slot, :, cols] = part[rows:]
                    self.to_pair[slot, :, cols] = part[:rows].astype(jnp.bfloat16)

                return inner

            lax.fori_loop(0, width // tile, columns, 0)
            self.pair(i).start()
            pl.when(i > 0)(lambda: hand_on(i - 1))
            return carry

        lax.fori_loop(0, nchip, step, 0)
        self.pair(nchip - 1).wait_recv()
        for i in range(nchip - 1):
            self.chips(i).wait_recv()

    def total(self, at):
        last = self.place.nchip - 1
        value = self.mine[last % 2, at, :] + self.from_pair[last, at, :].astype(jnp.float32)
        for i in range(last):
            value = value + self.from_chip[i, at, :].astype(jnp.float32)
        return value

    def finish(self):
        for i in range(max(self.place.nchip - 2, 0), self.place.nchip):
            self.pair(i).wait_send()
        for i in range(self.place.nchip - 1):
            self.chips(i).wait_send()


def scatter_scratch(nctx, rows, d):
    n = nctx // 2
    bf16 = jnp.bfloat16
    return [
        pltpu.VMEM((2, rows, d), jnp.float32),
        pltpu.VMEM((2, rows, d), bf16),
        pltpu.VMEM((n, rows, d), bf16),
        pltpu.VMEM((n - 1, rows, d), bf16),
        pltpu.VMEM((n - 1, rows, d), bf16),
        DMA((n,)),
        DMA((n,)),
        DMA((n - 1,)),
        DMA((n - 1,)),
    ]


def dot_nn(a, b):
    return jnp.dot(a, b, preferred_element_type=jnp.float32)


def dot_nt(a, b):
    return lax.dot_general(a, b, (((1,), (1,)), ((), ())), preferred_element_type=jnp.float32)


def mlp_back_kernel(
    gate_ref, up_ref, w_ref, resid_ref, cot_ref, gain_ref, grad_ref, vec_ref, grad_all, block, *scratch
):
    place = Place()
    greet(place)
    scatter = SumScatter(
        place,
        resid_ref.shape[0],
        lambda rows, cols: dot_nt(gate_ref[rows, :], w_ref[0, cols, :]) + dot_nt(up_ref[rows, :], w_ref[1, cols, :]),
        *scratch[:5],
        scratch[5:9],
    )
    scatter.run()
    gain = gain_ref[...].astype(jnp.float32)
    vec_ref[...] = jnp.zeros_like(vec_ref)

    def back(at):
        grad = scatter.total(at)
        normed, rscale = normal(resid_ref[at, :])
        vec_ref[0:1, :] += jnp.sum(grad * normed, axis=0, keepdims=True)
        vec_ref[1:2, :] += jnp.sum(grad, axis=0, keepdims=True)
        out = cot_ref[at, :] + normal_back(grad, normed, rscale, gain)
        grad_ref[at, :] = out
        block[at, :] = out.astype(jnp.bfloat16)

    row_loop(resid_ref.shape[0], back)
    rows = RowGather(place, block, grad_all, *scratch[9:12])
    rows.start()
    rows.forward()
    rows.finish()
    scatter.finish()


def mlp_back(gate_grad, up_grad, w, resid, cot, gain):
    nctx = lax.axis_size("ctx")
    rows, d = resid.shape
    return pl.pallas_call(
        mlp_back_kernel,
        out_shape=(
            jax.ShapeDtypeStruct((rows, d), jnp.float32),
            jax.ShapeDtypeStruct((2, d), jnp.float32),
            jax.ShapeDtypeStruct((rows * nctx, d), jnp.bfloat16),
        ),
        in_specs=[VMEM] * 6,
        out_specs=(VMEM, VMEM, ANY),
        scratch_shapes=[pltpu.VMEM((rows, d), jnp.bfloat16)]
        + scatter_scratch(nctx, rows, d)
        + gather_sems(nctx),
        compiler_params=pltpu.CompilerParams(collective_id=2, has_side_effects=True),
        cost_estimate=pl.CostEstimate(flops=0, bytes_accessed=150_000_000, transcendentals=0),
        name="mlp_back",
    )(gate_grad, up_grad, w, resid, cot, gain[None, :])


def attn_back_kernel(parts_ref, w_ref, x_ref, grad_ref, gain_ref, out_ref, vec_ref, *scratch):
    place = Place()
    greet(place)

    def product(rows, cols):
        part = dot_nt(parts_ref[0, rows, :], w_ref[0, cols, :])
        part = part + dot_nt(parts_ref[1, rows, :], w_ref[1, cols, :])
        return part + dot_nt(parts_ref[2, rows, :], w_ref[2, cols, :])

    scatter = SumScatter(place, x_ref.shape[0], product, *scratch[:5], scratch[5:9])
    scatter.run()
    gain = gain_ref[...].astype(jnp.float32)
    vec_ref[...] = jnp.zeros_like(vec_ref)

    def back(at):
        grad = scatter.total(at)
        normed, rscale = normal(x_ref[at, :].astype(jnp.float32))
        vec_ref[0:1, :] += jnp.sum(grad * normed, axis=0, keepdims=True)
        vec_ref[1:2, :] += jnp.sum(grad, axis=0, keepdims=True)
        out_ref[at, :] = grad_ref[at, :] + normal_back(grad, normed, rscale, gain)

    row_loop(x_ref.shape[0], back)
    scatter.finish()


def attn_back(parts, w, x, grad, gain):
    nctx = lax.axis_size("ctx")
    rows, d = x.shape
    return pl.pallas_call(
        attn_back_kernel,
        out_shape=(
            jax.ShapeDtypeStruct((rows, d), jnp.float32),
            jax.ShapeDtypeStruct((2, d), jnp.float32),
        ),
        in_specs=[VMEM] * 5,
        out_specs=(VMEM, VMEM),
        scratch_shapes=scatter_scratch(nctx, rows, d),
        compiler_params=pltpu.CompilerParams(collective_id=3, has_side_effects=True),
        cost_estimate=pl.CostEstimate(flops=0, bytes_accessed=100_000_000, transcendentals=0),
        name="attn_back",
    )(parts, w, x, grad, gain[None, :])


def down_kernel(hidden_ref, w_ref, resid_ref, out_ref, *scratch):
    place = Place()
    greet(place)
    scatter = SumScatter(
        place,
        resid_ref.shape[0],
        lambda rows, cols: dot_nn(hidden_ref[rows, :], w_ref[:, cols]),
        *scratch[:5],
        scratch[5:9],
    )
    scatter.run()

    def add(at):
        out_ref[at, :] = (resid_ref[at, :] + scatter.total(at)).astype(jnp.bfloat16)

    row_loop(resid_ref.shape[0], add)
    scatter.finish()


def down(hidden, w, resid):
    nctx = lax.axis_size("ctx")
    rows, d = resid.shape
    return pl.pallas_call(
        down_kernel,
        out_shape=jax.ShapeDtypeStruct((rows, d), jnp.bfloat16),
        in_specs=[VMEM] * 3,
        out_specs=VMEM,
        scratch_shapes=scatter_scratch(nctx, rows, d),
        compiler_params=pltpu.CompilerParams(collective_id=4, has_side_effects=True),
        cost_estimate=pl.CostEstimate(flops=0, bytes_accessed=100_000_000, transcendentals=0),
        name="down_sum",
    )(hidden, w, resid)


def vectors_kernel(v_ref, out_ref, from_ctx, from_dp, plane, ctx_send, ctx_recv, dp_send, dp_recv):
    place = Place()
    greet(place, all_ctx=True, along_dp=True)
    nctx, ndp, c, z = place.nctx, place.ndp, place.c, place.z

    def across(i):
        return push(
            v_ref, from_ctx.at[c], ctx_send.at[i - 1], ctx_recv.at[c], place.at(lax.rem(c + i, nctx))
        )

    def along(i):
        return push(
            plane, from_dp.at[z], dp_send.at[i - 1], dp_recv.at[z], {"dp": lax.rem(z + i, ndp), "ctx": c}
        )

    for i in range(1, nctx):
        across(i).start()
    from_ctx[c] = v_ref[...]
    for i in range(1, nctx):
        s = lax.rem(c + i, nctx)
        push(v_ref, from_ctx.at[s], ctx_send.at[0], ctx_recv.at[s], place.at(s)).wait_recv()
    value = from_ctx[0]
    for i in range(1, nctx):
        value = value + from_ctx[i]
    plane[...] = value
    for i in range(1, ndp):
        along(i).start()
    from_dp[z] = value
    for i in range(1, ndp):
        s = lax.rem(z + i, ndp)
        push(plane, from_dp.at[s], dp_send.at[0], dp_recv.at[s], {"dp": s, "ctx": c}).wait_recv()
    value = from_dp[0]
    for i in range(1, ndp):
        value = value + from_dp[i]
    out_ref[...] = value
    for i in range(1, nctx):
        across(i).wait_send()
    for i in range(1, ndp):
        along(i).wait_send()


def sum_vectors(v):
    ndp, nctx = lax.axis_size("dp"), lax.axis_size("ctx")
    f32 = jnp.float32
    return pl.pallas_call(
        vectors_kernel,
        out_shape=jax.ShapeDtypeStruct(v.shape, f32),
        in_specs=[VMEM],
        out_specs=VMEM,
        scratch_shapes=[
            pltpu.VMEM((nctx,) + v.shape, f32),
            pltpu.VMEM((ndp,) + v.shape, f32),
            pltpu.VMEM(v.shape, f32),
            DMA((nctx - 1,)),
            DMA((nctx,)),
            DMA((ndp - 1,)),
            DMA((ndp,)),
        ],
        compiler_params=pltpu.CompilerParams(collective_id=5, has_side_effects=True),
        cost_estimate=pl.CostEstimate(flops=0, bytes_accessed=30_000_000, transcendentals=0),
        name="sum_vectors",
    )(v)


HALF = ROT // 2
PAIR = 256


def tiles(count, body):
    def step(i, carry):
        body(i)
        return carry

    lax.fori_loop(0, count, step, 0)


def span(i, size):
    return pl.ds(pl.multiple_of(i * size, size), size)


def turn(columns, cosine, sine, heads):
    out = []
    for h in range(heads):
        at = h * HEAD_DIM
        a, b = columns[at : at + HALF], columns[at + HALF : at + ROT]
        out += [a * cosine - b * sine, b * cosine + a * sine, columns[at + ROT : at + HEAD_DIM]]
    return jnp.concatenate(out, axis=0)


def attend(rows_ref, w_ref, shift_ref, cos_ref, sin_ref, pos_col, pos_row, q_t, k_t, v_t, attn_t, lse, k_n, bias, attn):
    seq = rows_ref.shape[0]
    width = w_ref.shape[2]
    heads = width // HEAD_DIM
    bf16 = jnp.bfloat16

    def project(t):
        at = span(t, PAIR)
        cosine, sine = cos_ref[:, at], sin_ref[:, at]
        for i, ref in enumerate((q_t, k_t, v_t)):
            raw = (dot_nn(rows_ref[at, :], w_ref[i]) + shift_ref[i : i + 1, :]).T
            if i < 2:
                raw = turn(raw, cosine, sine, heads)
            raw = raw.astype(bf16)
            if i == 0:
                raw = raw * jnp.asarray(1.0 / math.sqrt(HEAD_DIM), bf16)
            ref[:, at] = raw

    tiles(seq // PAIR, project)
    for h in range(heads):
        k_n[h] = k_t[h * HEAD_DIM : (h + 1) * HEAD_DIM, :].T

    def queries(t):
        at = span(t, PAIR)
        bias[...] = jnp.where(pos_col[...] <= pos_row[:, at], 0.0, neg_big)

        for h in range(heads):
            feats = slice(h * HEAD_DIM, (h + 1) * HEAD_DIM)
            scores = dot_nn(k_n[h], q_t[feats, at]) + bias[...]
            peak = jnp.max(scores, axis=0, keepdims=True)
            probs = jnp.exp(scores - peak)
            total = jnp.sum(probs, axis=0, keepdims=True)
            out = dot_nn(v_t[feats, :], probs.astype(bf16)) / total
            attn_t[feats, at] = out.astype(bf16)
            lse[h : h + 1, at] = peak + jnp.log(total)
        attn[at, :] = attn_t[:, at].T

    tiles(seq // PAIR, queries)


class DepthScatter:
    def __init__(self, place, part, got, both, width, send, recv):
        self.place, self.part, self.got, self.both, self.width = place, part, got, both, width
        self.send, self.recv = send, recv
        self.line = place.ndp == 4
        z = place.z
        self.end = jnp.logical_or(z == 0, z == 3)
        self.middle = jnp.logical_not(self.end)
        self.next = jnp.where(z == 3, 2, 1)
        self.other = jnp.clip(3 - z, 1, 2)
        self.near = jnp.clip(3 * (z - 1), 0, 3)

    def block(self, z):
        return self.part.at[:, pl.ds(pl.multiple_of(z * self.width, self.width), self.width)]

    def copy(self, src, slot, sem, z):
        return push(src, self.got.at[slot], self.send.at[sem], self.recv.at[slot], {"dp": z, "ctx": self.place.c})

    def from_end(self):
        far = 3 - self.place.z
        return [
            self.copy(self.block(far), 2, 0, self.next),
            self.copy(self.block(3 - self.next), 3, 1, self.next),
            self.copy(self.block(self.next), 0, 2, self.next),
        ]

    def from_middle(self):
        return [
            self.copy(self.block(self.near), 0, 0, self.near),
            self.copy(self.both.at[0], 1, 1, 3 - self.near),
            self.copy(self.both.at[1], 1, 2, self.other),
        ]

    def across(self):
        z, n = self.place.z, self.place.ndp
        return [self.copy(self.block(lax.rem(z + i, n)), i - 1, i - 1, lax.rem(z + i, n)) for i in range(1, n)]

    def start(self):
        if not self.line:
            for copy in self.across():
                copy.start()
            return

        @pl.when(self.end)
        def _():
            for copy in self.from_end():
                copy.start()

        @pl.when(self.middle)
        def _():
            self.from_middle()[0].start()

    def hand_on(self):
        if not self.line:
            return

        @pl.when(self.middle)
        def _():
            for j, owner in enumerate((3 - self.near, self.other)):
                self.copy(self.both.at[0], 2 + j, 0, self.near).wait_recv()
                cols = pl.ds(pl.multiple_of(owner * self.width, self.width), self.width)

                def add(at, j=j, cols=cols):
                    total = self.part[at, cols].astype(jnp.float32) + self.got[2 + j, at, :].astype(jnp.float32)
                    self.both[j, at, :] = total.astype(jnp.bfloat16)

                row_loop(self.part.shape[0], add)
                self.from_middle()[1 + j].start()

    def finish(self, out_ref):
        count = 2 if self.line else self.place.ndp - 1
        for slot in range(count):
            self.copy(self.got.at[slot], slot, 0, self.next).wait_recv()
        cols = pl.ds(pl.multiple_of(self.place.z * self.width, self.width), self.width)

        def add(at):
            value = self.part[at, cols].astype(jnp.float32)
            for slot in range(count):
                value = value + self.got[slot, at, :].astype(jnp.float32)
            out_ref[at, :] = value

        row_loop(self.part.shape[0], add)
        if not self.line:
            for copy in self.across():
                copy.wait_send()
            return

        @pl.when(self.end)
        def _():
            for copy in self.from_end():
                copy.wait_send()

        @pl.when(self.middle)
        def _():
            for copy in self.from_middle():
                copy.wait_send()


def depth_scatter_scratch(ndp, rows, width):
    slots = 4 if ndp == 4 else ndp - 1
    return [
        pltpu.VMEM((slots, rows, width), jnp.bfloat16),
        pltpu.VMEM((2, rows, width), jnp.bfloat16),
        DMA((max(slots, 3),)),
        DMA((slots,)),
    ]


def forward_kernel(
    x_ref, cot_ref, gain1_ref, bias1_ref, gain2_ref, bias2_ref, shift_ref, cos_ref, sin_ref, pos_col, pos_row,
    qkv_ref, out_ref, gateup_ref, down_ref,
    resid_ref, q_t, k_t, v_t, attn_t, lse, hidden_ref, gate_side, up_side, down_grads,
    rows_out, cots_out, qkv_out, out_out, normed_out, gateup_out, down_all,
    row_block, cot_block, rows_all, cot_all, qkv_all, out_all, gateup_all,
    k_n, bias, attn, gate_f, hidden_t, *sems
):
    f32, bf16 = jnp.float32, jnp.bfloat16
    place = Place()
    greet(place, along_dp=True)
    sems = list(sems)

    def take(n):
        head = sems[:n]
        del sems[:n]
        return head

    def along_rows(size):
        return lambda ref, z: ref.at[:, pl.ds(pl.multiple_of(z * size, size), size), :]

    def along_lanes(size):
        return lambda ref, z: ref.at[:, pl.ds(pl.multiple_of(z * size, size), size)]

    depth, width = qkv_ref.shape[1], out_ref.shape[1]

    def half(i):
        return lambda ref, z: ref.at[i, pl.ds(pl.multiple_of(z * depth, depth), depth), :]

    qkv = DepthGather(place, qkv_ref, qkv_all, along_rows(depth), *take(3))
    out = DepthGather(place, out_ref, out_all, along_lanes(width), *take(3))
    gate = DepthGather(place, gateup_ref.at[0], gateup_all, half(0), *take(3))
    up = DepthGather(place, gateup_ref.at[1], gateup_all, half(1), *take(3))
    down = DepthGather(place, down_ref, down_all, along_lanes(width), *take(3))
    rows = RowGather(place, row_block, rows_all, *take(3))
    cots = RowGather(place, cot_block, cot_all, *take(3))
    normeds = RowGather(place, row_block, rows_all, *take(3))
    scatter_refs = take(9)
    got, both, dsend, drecv = take(4)
    (save_sem,) = take(1)
    seq = rows_all.shape[0]

    def save(i, src, dst):
        return pltpu.make_async_copy(src, dst, save_sem.at[i])

    saves = [
        save(0, rows_all, rows_out),
        save(1, cot_all, cots_out),
        save(2, qkv_all, qkv_out),
        save(3, out_all, out_out),
        save(4, rows_all, normed_out),
        save(5, gateup_all, gateup_out),
    ]

    qkv.start()
    out.start()
    gain, shift = gain1_ref[...].astype(f32), bias1_ref[...].astype(f32)

    def norm1(at):
        normed, _ = normal(x_ref[at, :].astype(f32))
        row_block[at, :] = (normed * gain + shift).astype(bf16)
        cot_block[at, :] = cot_ref[at, :].astype(bf16)

    row_loop(x_ref.shape[0], norm1)
    rows.start()
    cots.start()
    rows.forward()
    qkv.forward()
    cots.forward()
    out.forward()
    gate.start()
    up.start()
    rows.finish()
    saves[0].start()
    cots.finish()
    saves[1].start()
    qkv.finish()
    saves[2].start()
    attend(rows_all, qkv_all, shift_ref, cos_ref, sin_ref, pos_col, pos_row, q_t, k_t, v_t, attn_t, lse, k_n, bias, attn)
    out.finish()
    saves[3].start()
    saves[0].wait()
    scatter = SumScatter(
        place,
        x_ref.shape[0],
        lambda at, cols: dot_nn(attn[at, :], out_all[:, cols]),
        *scatter_refs[:5],
        scatter_refs[5:9],
    )
    scatter.run()
    gain2, shift2 = gain2_ref[...].astype(f32), bias2_ref[...].astype(f32)

    def norm2(at):
        resid = x_ref[at, :].astype(f32) + scatter.total(at)
        resid_ref[at, :] = resid
        normed, _ = normal(resid)
        row_block[at, :] = (normed * gain2 + shift2).astype(bf16)

    row_loop(x_ref.shape[0], norm2)
    normeds.start()
    gate.forward()
    normeds.forward()
    up.forward()
    down.start()
    normeds.finish()
    saves[4].start()
    scatter.finish()
    gate.finish()

    def gates(t):
        at = span(t, PAIR)
        gate_f[at, :] = dot_nn(rows_all[at, :], gateup_all[0])

    tiles(seq // PAIR, gates)
    up.finish()
    saves[5].start()

    def ups(t):
        at = span(t, PAIR)
        value = dot_nn(rows_all[at, :], gateup_all[1])
        g = gate_f[at, :]
        sigma = jax.nn.sigmoid(g)
        swish = g * sigma
        hidden = (swish * value).astype(bf16)
        hidden_ref[at, :] = hidden
        hidden_t[:, at] = hidden.T
        gate_side[at, :] = (value * sigma * (1.0 + g * (1.0 - sigma))).astype(bf16)
        up_side[at, :] = swish.astype(bf16)

    tiles(seq // PAIR, ups)
    saves[4].wait()
    part = rows_all.at[: hidden_t.shape[0]]

    def weights(j):
        cols = span(j, 2 * PAIR)
        part[:, cols] = dot_nn(hidden_t[...], cot_all[:, cols]).astype(bf16)

    tiles(cot_all.shape[1] // (2 * PAIR), weights)
    summed = DepthScatter(place, part, got, both, width, dsend, drecv)
    summed.start()
    down.forward()
    summed.hand_on()
    summed.finish(down_grads)
    down.finish()
    for i in (1, 2, 3, 5):
        saves[i].wait()


def forward(x, cot, gain1, bias1, gain2, bias2, shift, cosine, sine, pos_col, pos_row, qkv, out, gateup, down):
    ndp, nctx = lax.axis_size("dp"), lax.axis_size("ctx")
    rows, d = x.shape
    seq, width, ff = rows * nctx, qkv.shape[2], gateup.shape[2]
    heads = width // HEAD_DIM
    bf16, f32 = jnp.bfloat16, jnp.float32
    row = [v[None, :] for v in (gain1, bias1, gain2, bias2)]

    def shaped(shape, dtype=bf16):
        return jax.ShapeDtypeStruct(shape, dtype)

    return pl.pallas_call(
        forward_kernel,
        out_shape=(
            shaped((rows, d), f32),
            shaped((width, seq)),
            shaped((width, seq)),
            shaped((width, seq)),
            shaped((width, seq)),
            shaped((8, seq), f32),
            shaped((seq, ff)),
            shaped((seq, ff)),
            shaped((seq, ff)),
            shaped(down.shape, f32),
            shaped((seq, d)),
            shaped((seq, d)),
            shaped((3, d, width)),
            shaped((width, d)),
            shaped((seq, d)),
            shaped((2, d, ff)),
            shaped((ff, d)),
        ),
        in_specs=[VMEM] * 15,
        out_specs=(VMEM,) * 10 + (ANY,) * 7,
        scratch_shapes=[
            pltpu.VMEM((rows, d), bf16),
            pltpu.VMEM((rows, d), bf16),
            pltpu.VMEM((seq, d), bf16),
            pltpu.VMEM((seq, d), bf16),
            pltpu.VMEM((3, d, width), bf16),
            pltpu.VMEM((width, d), bf16),
            pltpu.VMEM((2, d, ff), bf16),
            pltpu.VMEM((heads, seq, HEAD_DIM), bf16),
            pltpu.VMEM((seq, PAIR), f32),
            pltpu.VMEM((seq, width), bf16),
            pltpu.VMEM((seq, ff), f32),
            pltpu.VMEM((ff, seq), bf16),
        ]
        + depth_sems(ndp) * 5
        + gather_sems(nctx) * 3
        + scatter_scratch(nctx, rows, d)
        + depth_scatter_scratch(ndp, ff, d // ndp)
        + [DMA((6,))],
        compiler_params=pltpu.CompilerParams(
            collective_id=0, has_side_effects=True, vmem_limit_bytes=67_000_000
        ),
        cost_estimate=pl.CostEstimate(flops=0, bytes_accessed=700_000_000, transcendentals=0),
        name="forward",
    )(x, cot, *row, shift, cosine, sine, pos_col, pos_row, qkv, out, gateup, down)


def attend_back_kernel(
    grad_ref, w_ref, rows_ref, cos_ref, sin_ref, pos_col, pos_row, q_t, k_t, v_t, attn_t, lse,
    parts_ref, sums_ref, w_grads, g_t, delta, q_grad, kv_grad, bias, flat
):
    seq, d = grad_ref.shape
    width = w_ref.shape[0]
    heads = width // HEAD_DIM
    bf16, f32 = jnp.bfloat16, jnp.float32

    def first(t):
        at = span(t, PAIR)
        grad = dot_nt(w_ref[...], grad_ref[at, :])
        both = grad * attn_t[:, at].astype(f32)
        for h in range(heads):
            delta[h : h + 1, at] = jnp.sum(both[h * HEAD_DIM : (h + 1) * HEAD_DIM], axis=0, keepdims=True)
        g_t[:, at] = grad.astype(bf16)

    tiles(seq // PAIR, first)
    q_grad[...] = jnp.zeros_like(q_grad)

    def keys(t):
        at = span(t, PAIR)
        bias[...] = jnp.where(pos_col[at, :] <= pos_row[...], 0.0, neg_big)
        for h in range(heads):
            feats = slice(h * HEAD_DIM, (h + 1) * HEAD_DIM)
            keys_t = k_t[feats, at]
            probs = jnp.exp(dot_nn(keys_t.T, q_t[feats, :]) + bias[...] - lse[h : h + 1, :])
            kv_grad[1, feats, at] = dot_nt(g_t[feats, :], probs.astype(bf16))
            back = dot_nn(v_t[feats, at].T, g_t[feats, :])
            scores = (probs * (back - delta[h : h + 1, :])).astype(bf16)
            kv_grad[0, feats, at] = dot_nt(q_t[feats, :], scores)
            q_grad[feats, :] += dot_nn(keys_t, scores)

    tiles(seq // PAIR, keys)
    sums_ref[...] = jnp.zeros_like(sums_ref)

    def part(t):
        at = span(t, PAIR)
        cosine, sine = cos_ref[:, at], sin_ref[:, at]
        for i in range(3):
            if i == 0:
                grad = turn(q_grad[:, at] * (1.0 / math.sqrt(HEAD_DIM)), cosine, -sine, heads)
            elif i == 1:
                grad = turn(kv_grad[0, :, at], cosine, -sine, heads)
            else:
                grad = kv_grad[1, :, at]
            natural = grad.T
            sums_ref[i : i + 1, :] += jnp.sum(natural, axis=0, keepdims=True)
            parts_ref[i, at, :] = natural.astype(bf16)
            flat[i, :, at] = grad.astype(bf16)

    tiles(seq // PAIR, part)

    def weights(j):
        cols = span(j, 2 * PAIR)
        rows = rows_ref[:, cols]
        for i in range(3):
            w_grads[i, cols, :] = dot_nn(flat[i], rows).T.astype(bf16)
        w_grads[3, cols, :] = dot_nn(attn_t[...], grad_ref[:, cols]).T.astype(bf16)

    tiles(d // (2 * PAIR), weights)


def attention_back(grad_all, w, rows_all, cosine, sine, pos_col, pos_row, q_t, k_t, v_t, attn_t, lse):
    seq, d = rows_all.shape
    width = w.shape[0]
    bf16, f32 = jnp.bfloat16, jnp.float32
    return pl.pallas_call(
        attend_back_kernel,
        out_shape=(
            jax.ShapeDtypeStruct((3, seq, width), bf16),
            jax.ShapeDtypeStruct((3, width), f32),
            jax.ShapeDtypeStruct((4, d, width), bf16),
        ),
        in_specs=[VMEM] * 12,
        out_specs=(VMEM,) * 3,
        scratch_shapes=[
            pltpu.VMEM((width, seq), bf16),
            pltpu.VMEM((8, seq), f32),
            pltpu.VMEM((width, seq), f32),
            pltpu.VMEM((2, width, seq), f32),
            pltpu.VMEM((PAIR, seq), f32),
            pltpu.VMEM((3, width, seq), bf16),
        ],
        cost_estimate=pl.CostEstimate(flops=0, bytes_accessed=120_000_000, transcendentals=0),
        name="attention_back",
    )(grad_all, w, rows_all, cosine, sine, pos_col, pos_row, q_t, k_t, v_t, attn_t, lse)


def rope_tables(positions):
    exponent = jnp.arange(HALF, dtype=jnp.float32) * (2.0 / ROT)
    inverse = jnp.exp(-exponent * math.log(rope_base))
    angle_val = inverse[:, None] * positions.astype(jnp.float32)[None, :]
    return (jnp.cos(angle_val), jnp.sin(angle_val))


def group_positions(group_order, count, half_group):
    row_ids = jnp.arange(count, dtype=jnp.int32)
    group_ids = row_ids // half_group
    matches = group_ids[:, None] == jnp.arange(group_order.shape[0], dtype=jnp.int32)[None, :]
    group_start = jnp.sum(jnp.where(matches, group_order[None, :], 0), axis=1)
    return group_start * half_group + row_ids % half_group


def shard(grad):
    return lax.psum_scatter(grad, "dp", scatter_dimension=1, tiled=True)


def per_device(
    block_input,
    out_cotangent,
    group_perm,
    attn_norm_gain,
    attn_norm_bias,
    qkv_weight,
    qkv_bias,
    out_weight,
    mlp_norm_gain,
    mlp_norm_bias,
    gateup_weight,
    down_weight,
):
    f32 = jnp.float32
    bf16 = jnp.bfloat16
    tok_rows = block_input.shape[0]
    cycle_size = lax.axis_size("ctx")
    cycle_index = lax.axis_index("ctx")
    seq_len = tok_rows * cycle_size
    half_group = tok_rows // 2
    group_order = group_perm[0]
    qkv_shift = qkv_bias.astype(f32)
    all_pos = group_positions(group_order, seq_len, half_group)
    cos_all, sin_all = rope_tables(all_pos)
    pos_f = all_pos.astype(f32)
    pos_col, pos_row = pos_f[:, None], pos_f[None, :]
    width_local = qkv_weight.shape[2]
    head_first = cycle_index * width_local
    shift_local = lax.dynamic_slice_in_dim(qkv_shift, head_first, width_local, 1)
    (
        residual_stream, q_t, k_t, v_t, attn_t, lse, hidden_b, gate_side, up_side, down_grads,
        rows_all, cot_all, qkv_local, out_local, mlp_all, gateup_local, down_local,
    ) = forward(
        block_input, out_cotangent, attn_norm_gain, attn_norm_bias, mlp_norm_gain, mlp_norm_bias, shift_local,
        cos_all, sin_all, pos_col, pos_row, qkv_weight, out_weight, gateup_weight, down_weight,
    )
    hidden_grad = jnp.dot(cot_all, down_local.T, preferred_element_type=f32)
    gate_grad = (hidden_grad * gate_side.astype(f32)).astype(bf16)
    up_grad = (hidden_grad * up_side.astype(f32)).astype(bf16)
    gateup_w_grad = jnp.einsum(
        "td,ktf->kdf", mlp_all, jnp.stack([gate_grad, up_grad]), preferred_element_type=f32
    ).astype(bf16)
    gate_grad, up_grad, gateup_w_grad = lax.optimization_barrier((gate_grad, up_grad, gateup_w_grad))
    gateup_grads = shard(gateup_w_grad)
    resid_grad, second_vectors, resid_all = mlp_back(
        gate_grad, up_grad, gateup_local, residual_stream, out_cotangent, mlp_norm_gain
    )
    grad_parts_b, shift_part, attn_grads = attention_back(
        resid_all, out_local, rows_all, cos_all, sin_all, pos_col, pos_row, q_t, k_t, v_t, attn_t, lse
    )
    shift_grad = lax.dynamic_update_slice_in_dim(jnp.zeros((3, D), f32), shift_part, head_first, 1)
    attn_grads = shard(attn_grads)
    input_grad, first_vectors = attn_back(grad_parts_b, qkv_local, block_input, resid_grad, attn_norm_gain)
    hidden_late, first_vectors, gateup_grads = lax.optimization_barrier((hidden_b, first_vectors, gateup_grads))
    block_output = down(hidden_late, down_local, residual_stream)
    small = sum_vectors(
        jnp.concatenate([first_vectors, second_vectors, shift_grad, jnp.zeros((1, D), f32)], axis=0)
    )
    small, block_output, attn_grads = lax.optimization_barrier((small, block_output, attn_grads))
    attn_grads = attn_grads.astype(f32)
    return (
        block_output,
        input_grad,
        small[0],
        small[1],
        attn_grads[:3],
        small[4:7],
        attn_grads[3].T,
        small[2],
        small[3],
        gateup_grads.astype(f32),
        down_grads,
    )


def solution(mesh):
    return jax.shard_map(
        per_device,
        mesh=mesh,
        in_specs=(
            P(("dp", "ctx"), None),
            P(("dp", "ctx"), None),
            P("dp", None),
            P(),
            P(),
            P(None, "dp", "ctx"),
            P(),
            P("ctx", "dp"),
            P(),
            P(),
            P(None, "dp", "ctx"),
            P("ctx", "dp"),
        ),
        out_specs=(
            P(("dp", "ctx"), None),
            P(("dp", "ctx"), None),
            P(),
            P(),
            P(None, "dp", "ctx"),
            P(),
            P("ctx", "dp"),
            P(),
            P(),
            P(None, "dp", "ctx"),
            P("ctx", "dp"),
        ),
        check_vma=False,
    )
```

```python
import functools
import math

import jax
import jax.numpy as jnp
from jax import lax
from jax.experimental import pallas as pl
from jax.experimental.pallas import tpu as pltpu
from jax.sharding import PartitionSpec as P

MESH = pl.DeviceIdType.MESH
VMEM = pl.BlockSpec(memory_space=pltpu.VMEM)
ANY = pl.BlockSpec(memory_space=pl.ANY)
DMA = pltpu.SemaphoreType.DMA

D = 2048
HEADS = 32
HEAD_DIM = 64
ROT = 16


eps_norm = 1e-05
rope_base = 10000.0
neg_big = -1e30


class Place:
    def __init__(self):
        self.ndp = lax.axis_size("dp")
        self.nctx = lax.axis_size("ctx")
        self.nchip = self.nctx // 2
        self.z = lax.axis_index("dp")
        self.c = lax.axis_index("ctx")
        self.p = lax.div(self.c, 2)
        self.k = lax.rem(self.c, 2)

    def chip(self, offset):
        return lax.rem(self.p + offset, self.nchip)

    def at(self, c):
        return {"dp": self.z, "ctx": c}

    def partner(self):
        return self.at(2 * self.p + 1 - self.k)

    def same_core(self, q):
        return self.at(2 * q + self.k)


def greet(place, along_ctx=True, along_dp=False, all_ctx=False):
    barrier = pltpu.get_barrier_semaphore()
    peers = []
    if all_ctx:
        peers += [place.at(lax.rem(place.c + i, place.nctx)) for i in range(1, place.nctx)]
    elif along_ctx:
        peers += [place.partner()] + [place.same_core(place.chip(i)) for i in range(1, place.nchip)]
    if along_dp:
        peers += [{"dp": lax.rem(place.z + i, place.ndp), "ctx": place.c} for i in range(1, place.ndp)]
    for peer in peers:
        pl.semaphore_signal(barrier, inc=1, device_id=peer, device_id_type=MESH)
    pl.semaphore_wait(barrier, len(peers))


def push(src, dst, send, recv, device):
    return pltpu.make_async_remote_copy(
        src_ref=src, dst_ref=dst, send_sem=send, recv_sem=recv, device_id=device, device_id_type=MESH
    )


class RowGather:
    def __init__(self, place, block, whole, send, recv, local):
        self.place, self.block, self.whole = place, block, whole
        self.send, self.recv, self.local = send, recv, local
        self.rows = block.shape[0]

    def slot(self, c):
        return self.whole.at[pl.ds(pl.multiple_of(c * self.rows, self.rows), self.rows)]

    def direct(self, i):
        place = self.place
        q = place.chip(i)
        return push(self.block, self.slot(place.c), self.send.at[i], self.recv.at[place.c], place.same_core(q))

    def own(self):
        place = self.place
        return push(self.block, self.slot(place.c), self.send.at[0], self.recv.at[place.c], place.partner())

    def passed(self, i):
        place = self.place
        c = 2 * place.chip(i) + place.k
        return push(
            self.slot(c), self.slot(c), self.send.at[place.nchip + i - 1], self.recv.at[c], place.partner()
        )

    def arrival(self, c):
        return push(self.block, self.slot(c), self.send.at[0], self.recv.at[c], self.place.partner())

    def keep(self):
        return pltpu.make_async_copy(self.block, self.slot(self.place.c), self.local)

    def start(self):
        for i in range(1, self.place.nchip):
            self.direct(i).start()
        self.own().start()
        self.keep().start()

    def forward(self):
        place = self.place
        for i in range(1, place.nchip):
            self.arrival(2 * place.chip(i) + place.k).wait_recv()
            self.passed(i).start()

    def finish(self):
        place = self.place
        for i in range(place.nchip):
            self.arrival(2 * place.chip(i) + 1 - place.k).wait_recv()
        self.own().wait_send()
        for i in range(1, place.nchip):
            self.direct(i).wait_send()
            self.passed(i).wait_send()
        self.keep().wait()


class BoxGather(RowGather):
    def part(self, c, half):
        size = self.rows // 2
        return self.whole.at[pl.ds(pl.multiple_of(c * self.rows + half * size, size), size)]

    def near(self, axis):
        place = self.place
        other = 1 - lax.rem(place.p, 2) if axis == 0 else 1 - lax.div(place.p, 2)
        q = 2 * lax.div(place.p, 2) + other if axis == 0 else 2 * other + lax.rem(place.p, 2)
        return 2 * q + place.k

    def across(self):
        return 2 * (3 - self.place.p) + self.place.k

    def piece(self, c, half, sem, to, own=False):
        size = self.rows // 2
        src = self.block.at[pl.ds(half * size, size)] if own else self.part(c, half)
        return push(src, self.part(c, half), self.send.at[sem], self.recv.at[2 * c + half], self.place.at(to))

    def own(self):
        place = self.place
        return push(self.block, self.slot(place.c), self.send.at[0], self.recv.at[2 * place.c], place.partner())

    def first(self):
        c = self.place.c
        return [self.piece(c, h, 1 + n, self.near(a), True) for n, (a, h) in enumerate(((0, 0), (1, 1), (0, 1), (1, 0)))]

    def second(self):
        return [self.piece(self.near(a), a, 5 + a, self.near(1 - a)) for a in (0, 1)]

    def to_partner(self):
        place = self.place
        pair = 2 * place.p + 1 - place.k
        return [
            self.piece(c, h, 7 + n, pair)
            for n, (c, h) in enumerate(
                ((self.near(0), 0), (self.near(1), 1), (self.near(0), 1), (self.near(1), 0), (self.across(), 0), (self.across(), 1))
            )
        ]

    def start(self):
        for copy in self.first():
            copy.start()
        self.own().start()
        self.keep().start()

    def forward(self):
        second, pair = self.second(), self.to_partner()
        for n, copy in enumerate(pair):
            copy.wait_recv()
            if n < 2:
                second[n].start()
            copy.start()

    def finish(self):
        place = self.place
        pair = 2 * place.p + 1 - place.k
        self.arrival_pair().wait_recv()
        for n in range(6):
            c = (self.near(0), self.near(1), self.near(0), self.near(1), self.across(), self.across())[n]
            half = (0, 1, 1, 0, 0, 1)[n]
            twin = c + 1 - 2 * place.k
            self.piece(twin, half, 7 + n, pair).wait_recv()
        self.own().wait_send()
        for copy in self.first() + self.second() + self.to_partner():
            copy.wait_send()
        self.keep().wait()

    def arrival_pair(self):
        c = self.place.c + 1 - 2 * self.place.k
        return push(self.block, self.slot(c), self.send.at[0], self.recv.at[2 * c], self.place.partner())


def row_gather(place, *args):
    return (BoxGather if place.nchip == 4 else RowGather)(place, *args)


def gather_sems(nctx):
    return [DMA((13,)), DMA((2 * nctx,)), DMA] if nctx == 8 else [DMA((nctx,)), DMA((nctx,)), DMA]


class DepthGather:
    def __init__(self, place, piece, whole, where, send, recv, local, passing=True):
        self.place, self.piece, self.whole, self.where = place, piece, whole, where
        self.send, self.recv, self.local = send, recv, local
        self.line = place.ndp == 4 and passing
        z = place.z
        self.end = jnp.logical_or(z == 0, z == 3)
        self.middle = jnp.logical_not(self.end)
        self.near = jnp.clip(3 * (z - 1), 0, 3)
        self.far = 3 - self.near
        self.other = jnp.clip(3 - z, 1, 2)

    def copy(self, src, z_src, z_dst, sem):
        return push(
            src, self.where(self.whole, z_src), self.send.at[sem], self.recv.at[z_src], {"dp": z_dst, "ctx": self.place.c}
        )

    def directs(self):
        z, n = self.place.z, self.place.ndp
        if not self.line:
            return [(None, self.copy(self.piece, z, lax.rem(z + i, n), i - 1)) for i in range(1, n)]
        out = []
        for sem, step in enumerate((1, -1, 2, -2)):
            d = z + step
            ok = jnp.logical_and(d >= 0, d < 4)
            if abs(step) == 2:
                ok = jnp.logical_and(ok, self.end)
            out.append((ok, self.copy(self.piece, z, jnp.clip(d, 0, 3), sem)))
        return out

    def keep(self):
        return pltpu.make_async_copy(self.piece, self.where(self.whole, self.place.z), self.local)

    def start(self):
        for ok, copy in self.directs():
            if ok is None:
                copy.start()
            else:
                pl.when(ok)(copy.start)
        self.keep().start()

    def passed(self, src, sem):
        return self.copy(self.where(self.whole, src), src, self.near, sem)

    def forward_next(self):
        self.forward(self.other, 4)

    def forward_far(self):
        self.forward(self.far, 5)

    def forward(self, src, sem):
        if self.line:

            @pl.when(self.middle)
            def _():
                self.copy(self.piece, src, src, sem).wait_recv()
                self.passed(src, sem).start()

    def finish(self):
        z, n = self.place.z, self.place.ndp
        for i in range(1, n):
            src = lax.rem(z + i, n)
            wait = self.copy(self.piece, src, src, 0).wait_recv
            if self.line:
                pl.when(jnp.logical_or(self.end, src == self.near))(wait)
            else:
                wait()
        for ok, copy in self.directs():
            if ok is None:
                copy.wait_send()
            else:
                pl.when(ok)(copy.wait_send)
        if self.line:

            @pl.when(self.middle)
            def _():
                self.passed(self.other, 4).wait_send()
                self.passed(self.far, 5).wait_send()

        self.keep().wait()


def depth_sems(ndp):
    return [DMA((max(ndp, 6),)), DMA((ndp,)), DMA]


STEP = 16


def row_loop(rows, body):
    def step(i, carry):
        body(pl.ds(pl.multiple_of(i * STEP, STEP), STEP))
        return carry

    lax.fori_loop(0, rows // STEP, step, 0)


def normal(values):
    centred = values - jnp.mean(values, axis=-1, keepdims=True)
    rscale = lax.rsqrt(jnp.mean(centred * centred, axis=-1, keepdims=True) + eps_norm)
    return centred * rscale, rscale


def normal_back(grad_out, normed, rscale, gain):
    scaled = grad_out * gain
    return rscale * (
        scaled
        - jnp.mean(scaled, axis=-1, keepdims=True)
        - normed * jnp.mean(scaled * normed, axis=-1, keepdims=True)
    )


class SumScatter:
    TILE = 512

    def __init__(self, place, rows, product, mine, to_pair, from_pair, to_chip, from_chip, sems):
        self.place, self.rows, self.product = place, rows, product
        self.mine, self.to_pair, self.from_pair = mine, to_pair, from_pair
        self.to_chip, self.from_chip = to_chip, from_chip
        self.pair_send, self.pair_recv, self.chip_send, self.chip_recv = sems

    def pair(self, i):
        return push(
            self.to_pair.at[lax.rem(i, 2)], self.from_pair.at[i], self.pair_send.at[i], self.pair_recv.at[i], self.place.partner()
        )

    def chips(self, i):
        return push(
            self.to_chip.at[i],
            self.from_chip.at[i],
            self.chip_send.at[i],
            self.chip_recv.at[i],
            self.place.same_core(self.place.chip(i + 1)),
        )

    def chip_of(self, i):
        return lax.rem(self.place.p + 1 + i, self.place.nchip)

    def hand_on(self, i):
        self.pair(i).wait_recv()

        def add(at):
            both = self.mine[lax.rem(i, 2), at, :] + self.from_pair[i, at, :].astype(jnp.float32)
            self.to_chip[i, at, :] = both.astype(jnp.bfloat16)

        row_loop(self.rows, add)
        self.chips(i).start()

    def last(self):
        nchip = self.place.nchip
        self.pair(nchip - 1).wait_recv()
        for i in range(nchip - 1):
            self.chips(i).wait_recv()

    def run(self):
        place, rows, tile = self.place, self.rows, self.TILE
        nchip = place.nchip
        width = self.mine.shape[-1]

        def step(i, carry):
            first = pl.multiple_of(self.chip_of(i) * 2 * rows, 2 * rows)
            slot = lax.rem(i, 2)
            pl.when(i >= 2)(lambda: self.pair(i - 2).wait_send())

            def columns(j, inner):
                cols = pl.ds(pl.multiple_of(j * tile, tile), tile)
                part = self.product(pl.ds(first, 2 * rows), cols)

                @pl.when(place.k == 0)
                def _():
                    self.mine[slot, :, cols] = part[:rows]
                    self.to_pair[slot, :, cols] = part[rows:].astype(jnp.bfloat16)

                @pl.when(place.k == 1)
                def _():
                    self.mine[slot, :, cols] = part[rows:]
                    self.to_pair[slot, :, cols] = part[:rows].astype(jnp.bfloat16)

                return inner

            lax.fori_loop(0, width // tile, columns, 0)
            self.pair(i).start()
            pl.when(i > 0)(lambda: self.hand_on(i - 1))
            return carry

        lax.fori_loop(0, nchip, step, 0)
        self.last()

    def total(self, at):
        last = self.place.nchip - 1
        value = self.mine[last % 2, at, :] + self.from_pair[last, at, :].astype(jnp.float32)
        for i in range(last):
            value = value + self.from_chip[i, at, :].astype(jnp.float32)
        return value

    def finish(self):
        for i in range(max(self.place.nchip - 2, 0), self.place.nchip):
            self.pair(i).wait_send()
        for i in range(self.place.nchip - 1):
            self.chips(i).wait_send()


class BoxScatter(SumScatter):
    def near(self, axis):
        p = self.place.p
        x, y = lax.rem(p, 2), lax.div(p, 2)
        return self.place.same_core(2 * y + 1 - x if axis == 0 else 2 * (1 - y) + x)

    def half(self, src, dst, rows, sem, axis):
        size = self.rows // 2
        at = pl.ds(rows * size, size)
        return push(
            self.to_chip.at[src, at], self.from_chip.at[dst, at], self.chip_send.at[sem], self.chip_recv.at[sem], self.near(axis)
        )

    def moves(self):
        return [
            self.half(0, 2, 0, 0, 0),
            self.half(0, 2, 1, 1, 1),
            self.half(1, 0, 0, 2, 0),
            self.half(2, 1, 1, 3, 1),
            self.half(1, 0, 1, 4, 0),
            self.half(2, 1, 0, 5, 1),
        ]

    def chip_of(self, i):
        p = self.place.p
        x, y = lax.rem(p, 2), lax.div(p, 2)
        other_x = jnp.logical_or(i == 0, i == 1)
        other_y = jnp.logical_or(i == 0, i == 2)
        return 2 * jnp.where(other_y, 1 - y, y) + jnp.where(other_x, 1 - x, x)

    def hand_on(self, i):
        self.pair(i).wait_recv()
        slot = lax.rem(i, 2)

        def add(at):
            both = self.mine[slot, at, :] + self.from_pair[i, at, :].astype(jnp.float32)
            self.to_chip[i, at, :] = both.astype(jnp.bfloat16)

        row_loop(self.rows, add)
        moves = self.moves()

        @pl.when(i == 0)
        def _():
            moves[0].start()
            moves[1].start()

        pl.when(i == 1)(moves[2].start)
        pl.when(i == 2)(moves[3].start)

    def last(self):
        moves = self.moves()
        size = self.rows // 2
        for arrived, src, first, onward in ((1, 1, size, 4), (0, 2, 0, 5)):
            moves[arrived].wait_recv()

            def add(at, src=src, first=first):
                at = pl.ds(pl.multiple_of(first + at.start, STEP), STEP)
                both = self.to_chip[src, at, :].astype(jnp.float32) + self.from_chip[2, at, :].astype(jnp.float32)
                self.to_chip[src, at, :] = both.astype(jnp.bfloat16)

            row_loop(size, add)
            moves[onward].start()
        self.pair(3).wait_recv()
        for n in (2, 3, 4, 5):
            moves[n].wait_recv()

    def total(self, at):
        value = self.mine[1, at, :] + self.from_pair[3, at, :].astype(jnp.float32)
        return value + self.from_chip[0, at, :].astype(jnp.float32) + self.from_chip[1, at, :].astype(jnp.float32)

    def finish(self):
        for i in (2, 3):
            self.pair(i).wait_send()
        for copy in self.moves():
            copy.wait_send()


def sum_scatter(place, *args):
    return (BoxScatter if place.nchip == 4 else SumScatter)(place, *args)


def scatter_scratch(nctx, rows, d):
    n = nctx // 2
    bf16 = jnp.bfloat16
    return [
        pltpu.VMEM((2, rows, d), jnp.float32),
        pltpu.VMEM((2, rows, d), bf16),
        pltpu.VMEM((n, rows, d), bf16),
        pltpu.VMEM((n - 1, rows, d), bf16),
        pltpu.VMEM((n - 1, rows, d), bf16),
        DMA((n,)),
        DMA((n,)),
        DMA((6 if n == 4 else n - 1,)),
        DMA((6 if n == 4 else n - 1,)),
    ]


def dot_nn(a, b):
    return jnp.dot(a, b, preferred_element_type=jnp.float32)


def dot_nt(a, b):
    return lax.dot_general(a, b, (((1,), (1,)), ((), ())), preferred_element_type=jnp.float32)


def mlp_back_kernel(
    gate_ref, up_ref, w_ref, resid_ref, cot_ref, gain_ref, grad_ref, vec_ref, grad_all, block, *scratch
):
    place = Place()
    greet(place)
    scatter = sum_scatter(
        place,
        resid_ref.shape[0],
        lambda rows, cols: dot_nn(gate_ref[rows, :], w_ref[0, :, cols]) + dot_nn(up_ref[rows, :], w_ref[1, :, cols]),
        *scratch[:5],
        scratch[5:9],
    )
    scatter.run()
    gain = gain_ref[...].astype(jnp.float32)[None, :]
    vec_ref[...] = jnp.zeros_like(vec_ref)

    def back(at):
        grad = scatter.total(at)
        normed, rscale = normal(resid_ref[at, :])
        vec_ref[0:1, :] += jnp.sum(grad * normed, axis=0, keepdims=True)
        vec_ref[1:2, :] += jnp.sum(grad, axis=0, keepdims=True)
        out = cot_ref[at, :] + normal_back(grad, normed, rscale, gain)
        grad_ref[at, :] = out
        block[at, :] = out.astype(jnp.bfloat16)

    row_loop(resid_ref.shape[0], back)
    rows = row_gather(place, block, grad_all, *scratch[9:12])
    rows.start()
    rows.forward()
    rows.finish()
    scatter.finish()


def mlp_back(gate_grad, up_grad, w, resid, cot, gain):
    nctx = lax.axis_size("ctx")
    rows, d = resid.shape
    return pl.pallas_call(
        mlp_back_kernel,
        out_shape=(
            jax.ShapeDtypeStruct((rows, d), jnp.float32),
            jax.ShapeDtypeStruct((2, d), jnp.float32),
            jax.ShapeDtypeStruct((rows * nctx, d), jnp.bfloat16),
        ),
        in_specs=[VMEM] * 6,
        out_specs=(VMEM, VMEM, ANY),
        scratch_shapes=[pltpu.VMEM((rows, d), jnp.bfloat16)]
        + scatter_scratch(nctx, rows, d)
        + gather_sems(nctx),
        compiler_params=pltpu.CompilerParams(collective_id=2, has_side_effects=True),
        cost_estimate=pl.CostEstimate(flops=0, bytes_accessed=150_000_000, transcendentals=0),
        name="mlp_back",
    )(gate_grad, up_grad, w, resid, cot, gain)


def attn_back_kernel(parts_ref, w_ref, x_ref, grad_ref, gain_ref, out_ref, vec_ref, *scratch):
    place = Place()
    greet(place)

    def product(rows, cols):
        part = dot_nt(parts_ref[0, rows, :], w_ref[0, cols, :])
        part = part + dot_nt(parts_ref[1, rows, :], w_ref[1, cols, :])
        return part + dot_nt(parts_ref[2, rows, :], w_ref[2, cols, :])

    scatter = sum_scatter(place, x_ref.shape[0], product, *scratch[:5], scratch[5:9])
    scatter.run()
    gain = gain_ref[...].astype(jnp.float32)[None, :]
    vec_ref[...] = jnp.zeros_like(vec_ref)

    def back(at):
        grad = scatter.total(at)
        normed, rscale = normal(x_ref[at, :].astype(jnp.float32))
        vec_ref[0:1, :] += jnp.sum(grad * normed, axis=0, keepdims=True)
        vec_ref[1:2, :] += jnp.sum(grad, axis=0, keepdims=True)
        out_ref[at, :] = grad_ref[at, :] + normal_back(grad, normed, rscale, gain)

    row_loop(x_ref.shape[0], back)
    scatter.finish()


def attn_back(parts, w, x, grad, gain):
    nctx = lax.axis_size("ctx")
    rows, d = x.shape
    return pl.pallas_call(
        attn_back_kernel,
        out_shape=(
            jax.ShapeDtypeStruct((rows, d), jnp.float32),
            jax.ShapeDtypeStruct((2, d), jnp.float32),
        ),
        in_specs=[VMEM] * 5,
        out_specs=(VMEM, VMEM),
        scratch_shapes=scatter_scratch(nctx, rows, d),
        compiler_params=pltpu.CompilerParams(collective_id=3, has_side_effects=True),
        cost_estimate=pl.CostEstimate(flops=0, bytes_accessed=100_000_000, transcendentals=0),
        name="attn_back",
    )(parts, w, x, grad, gain)


def down_kernel(hidden_ref, w_ref, resid_ref, out_ref, *scratch):
    place = Place()
    greet(place)
    scatter = sum_scatter(
        place,
        resid_ref.shape[0],
        lambda rows, cols: dot_nn(hidden_ref[rows, :], w_ref[:, cols]),
        *scratch[:5],
        scratch[5:9],
    )
    scatter.run()

    def add(at):
        out_ref[at, :] = (resid_ref[at, :] + scatter.total(at)).astype(jnp.bfloat16)

    row_loop(resid_ref.shape[0], add)
    scatter.finish()


def down(hidden, w, resid):
    nctx = lax.axis_size("ctx")
    rows, d = resid.shape
    return pl.pallas_call(
        down_kernel,
        out_shape=jax.ShapeDtypeStruct((rows, d), jnp.bfloat16),
        in_specs=[VMEM] * 3,
        out_specs=VMEM,
        scratch_shapes=scatter_scratch(nctx, rows, d),
        compiler_params=pltpu.CompilerParams(collective_id=4, has_side_effects=True),
        cost_estimate=pl.CostEstimate(flops=0, bytes_accessed=100_000_000, transcendentals=0),
        name="down_sum",
    )(hidden, w, resid)


def vectors_kernel(v_ref, out_ref, from_ctx, from_dp, plane, ctx_send, ctx_recv, dp_send, dp_recv):
    place = Place()
    greet(place, all_ctx=True, along_dp=True)
    nctx, ndp, c, z = place.nctx, place.ndp, place.c, place.z

    def across(i):
        return push(
            v_ref, from_ctx.at[c], ctx_send.at[i - 1], ctx_recv.at[c], place.at(lax.rem(c + i, nctx))
        )

    def along(i):
        return push(
            plane, from_dp.at[z], dp_send.at[i - 1], dp_recv.at[z], {"dp": lax.rem(z + i, ndp), "ctx": c}
        )

    for i in range(1, nctx):
        across(i).start()
    from_ctx[c] = v_ref[...]
    for i in range(1, nctx):
        s = lax.rem(c + i, nctx)
        push(v_ref, from_ctx.at[s], ctx_send.at[0], ctx_recv.at[s], place.at(s)).wait_recv()
    value = from_ctx[0]
    for i in range(1, nctx):
        value = value + from_ctx[i]
    plane[...] = value
    for i in range(1, ndp):
        along(i).start()
    from_dp[z] = value
    for i in range(1, ndp):
        s = lax.rem(z + i, ndp)
        push(plane, from_dp.at[s], dp_send.at[0], dp_recv.at[s], {"dp": s, "ctx": c}).wait_recv()
    value = from_dp[0]
    for i in range(1, ndp):
        value = value + from_dp[i]
    out_ref[...] = value
    for i in range(1, nctx):
        across(i).wait_send()
    for i in range(1, ndp):
        along(i).wait_send()


def sum_vectors(v):
    ndp, nctx = lax.axis_size("dp"), lax.axis_size("ctx")
    f32 = jnp.float32
    return pl.pallas_call(
        vectors_kernel,
        out_shape=jax.ShapeDtypeStruct(v.shape, f32),
        in_specs=[VMEM],
        out_specs=VMEM,
        scratch_shapes=[
            pltpu.VMEM((nctx,) + v.shape, f32),
            pltpu.VMEM((ndp,) + v.shape, f32),
            pltpu.VMEM(v.shape, f32),
            DMA((nctx - 1,)),
            DMA((nctx,)),
            DMA((ndp - 1,)),
            DMA((ndp,)),
        ],
        compiler_params=pltpu.CompilerParams(collective_id=5, has_side_effects=True),
        cost_estimate=pl.CostEstimate(flops=0, bytes_accessed=30_000_000, transcendentals=0),
        name="sum_vectors",
    )(v)


HALF = ROT // 2
PAIR = 256


def tiles(count, body):
    def step(i, carry):
        body(i)
        return carry

    lax.fori_loop(0, count, step, 0)


def span(i, size):
    return pl.ds(pl.multiple_of(i * size, size), size)


def turn(columns, cosine, sine, heads):
    out = []
    for h in range(heads):
        at = h * HEAD_DIM
        a, b = columns[at : at + HALF], columns[at + HALF : at + ROT]
        out += [a * cosine - b * sine, b * cosine + a * sine, columns[at + ROT : at + HEAD_DIM]]
    return jnp.concatenate(out, axis=0)


def attend(rows_ref, w_ref, shift_ref, cos_ref, sin_ref, pos_col, pos_row, q_t, k_t, v_t, attn_t, lse, k_n, bias, attn):
    seq = rows_ref.shape[0]
    width = w_ref.shape[2]
    heads = width // HEAD_DIM
    bf16 = jnp.bfloat16

    def project(t):
        at = span(t, PAIR)
        cosine, sine = cos_ref[:, at], sin_ref[:, at]
        for i, ref in enumerate((q_t, k_t, v_t)):
            raw = (dot_nn(rows_ref[at, :], w_ref[i]) + shift_ref[i : i + 1, :]).T
            if i < 2:
                raw = turn(raw, cosine, sine, heads)
            raw = raw.astype(bf16)
            if i == 0:
                raw = raw * jnp.asarray(1.0 / math.sqrt(HEAD_DIM), bf16)
            ref[:, at] = raw

    tiles(seq // PAIR, project)
    for h in range(heads):
        k_n[h] = k_t[h * HEAD_DIM : (h + 1) * HEAD_DIM, :].T

    def queries(t):
        at = span(t, PAIR)
        bias[...] = jnp.where(pos_col[...] <= pos_row[:, at], 0.0, neg_big)

        for h in range(heads):
            feats = slice(h * HEAD_DIM, (h + 1) * HEAD_DIM)
            scores = dot_nn(k_n[h], q_t[feats, at]) + bias[...]
            peak = jnp.max(scores, axis=0, keepdims=True)
            probs = jnp.exp(scores - peak)
            total = jnp.sum(probs, axis=0, keepdims=True)
            out = dot_nn(v_t[feats, :], probs.astype(bf16)) / total
            attn_t[feats, at] = out.astype(bf16)
            lse[h : h + 1, at] = peak + jnp.log(total)
        attn[at, :] = attn_t[:, at].T

    tiles(seq // PAIR, queries)


class DepthScatter:
    def __init__(self, place, part, got, both, width, send, recv):
        self.place, self.part, self.got, self.both, self.width = place, part, got, both, width
        self.send, self.recv = send, recv
        self.line = place.ndp == 4
        z = place.z
        self.end = jnp.logical_or(z == 0, z == 3)
        self.middle = jnp.logical_not(self.end)
        self.next = jnp.where(z == 3, 2, 1)
        self.other = jnp.clip(3 - z, 1, 2)
        self.near = jnp.clip(3 * (z - 1), 0, 3)

    def block(self, z):
        return self.part.at[:, pl.ds(pl.multiple_of(z * self.width, self.width), self.width)]

    def copy(self, src, slot, sem, z):
        return push(src, self.got.at[slot], self.send.at[sem], self.recv.at[slot], {"dp": z, "ctx": self.place.c})

    def from_end(self):
        far = 3 - self.place.z
        return [
            self.copy(self.block(far), 2, 0, self.next),
            self.copy(self.block(3 - self.next), 3, 1, self.next),
            self.copy(self.block(self.next), 0, 2, self.next),
        ]

    def from_middle(self):
        return [
            self.copy(self.both.at[0], 4, 0, self.other),
            self.copy(self.both.at[1], 1, 1, self.other),
            self.copy(self.both.at[2], 0, 2, self.near),
        ]

    def across(self):
        z, n = self.place.z, self.place.ndp
        return [self.copy(self.block(lax.rem(z + i, n)), i - 1, i - 1, lax.rem(z + i, n)) for i in range(1, n)]

    def start(self):
        if not self.line:
            for copy in self.across():
                copy.start()
            return

        @pl.when(self.end)
        def _():
            for copy in self.from_end():
                copy.start()

    def hand_on(self, n):
        if not self.line:
            return

        @pl.when(self.middle)
        def _():
            owner, slot = ((3 - self.near, 2), (self.other, 3), (self.near, 4))[n]
            self.copy(self.both.at[0], slot, 0, self.near).wait_recv()
            cols = pl.ds(pl.multiple_of(owner * self.width, self.width), self.width)

            def add(at):
                total = self.part[at, cols].astype(jnp.float32) + self.got[slot, at, :].astype(jnp.float32)
                self.both[n, at, :] = total.astype(jnp.bfloat16)

            row_loop(self.part.shape[0], add)
            self.from_middle()[n].start()

    def collect(self, count, out_ref):
        for slot in range(count):
            self.copy(self.got.at[slot], slot, 0, self.next).wait_recv()
        cols = pl.ds(pl.multiple_of(self.place.z * self.width, self.width), self.width)

        def add(at):
            value = self.part[at, cols].astype(jnp.float32)
            for slot in range(count):
                value = value + self.got[slot, at, :].astype(jnp.float32)
            out_ref[at, :] = value

        row_loop(self.part.shape[0], add)

    def finish(self, out_ref):
        if not self.line:
            self.collect(self.place.ndp - 1, out_ref)
            for copy in self.across():
                copy.wait_send()
            return

        @pl.when(self.end)
        def _():
            self.collect(1, out_ref)
            for copy in self.from_end():
                copy.wait_send()

        @pl.when(self.middle)
        def _():
            self.collect(2, out_ref)
            for copy in self.from_middle():
                copy.wait_send()


def depth_scatter_scratch(ndp, rows, width):
    slots = 5 if ndp == 4 else ndp - 1
    return [
        pltpu.VMEM((slots, rows, width), jnp.bfloat16),
        pltpu.VMEM((3, rows, width), jnp.bfloat16),
        DMA((max(slots, 3),)),
        DMA((slots,)),
    ]


def tables(perm_ref, cos_ref, sin_ref, pos_col, pos_row, size):
    seq = pos_row.shape[1]
    lane = lax.broadcasted_iota(jnp.int32, (8, seq), 1)
    group = lane // size
    start = jnp.zeros((8, seq), jnp.int32)
    for g in range(seq // size):
        start = jnp.where(group == g, perm_ref[0, g], start)
    pos = (start * size + lane - group * size).astype(jnp.float32)
    pos_row[...] = pos[0:1]
    pos_col[...] = pos.T[:, 0:1]
    step = lax.broadcasted_iota(jnp.int32, (8, seq), 0).astype(jnp.float32)
    angle = pos * jnp.exp(step * (-2.0 / ROT * math.log(rope_base)))
    cos_ref[...] = jnp.cos(angle)
    sin_ref[...] = jnp.sin(angle)


def forward_kernel(
    perm_ref, x_ref, cot_ref, gain1_ref, bias1_ref, gain2_ref, bias2_ref, shift_ref,
    qkv_ref, out_ref, gateup_ref, down_ref,
    resid_ref, q_t, k_t, v_t, attn_t, lse, hidden_ref, gate_side, up_side, down_grads, cos_ref, sin_ref, pos_col, pos_row,
    rows_out, qkv_out, out_out, gateup_out, down_out, grads_out,
    row_block, cot_block, rows_all, cot_all, qkv_all, out_all, gateup_all, down_all,
    k_n, bias, attn, gate_f, hidden_t, up_t, part, shifts, *sems
):
    f32, bf16 = jnp.float32, jnp.bfloat16
    place = Place()
    greet(place, along_dp=True)
    sems = list(sems)

    def take(n):
        head = sems[:n]
        del sems[:n]
        return head

    def along_rows(size):
        return lambda ref, z: ref.at[:, pl.ds(pl.multiple_of(z * size, size), size), :]

    def along_lanes(size):
        return lambda ref, z: ref.at[:, pl.ds(pl.multiple_of(z * size, size), size)]

    depth, width = qkv_ref.shape[1], out_ref.shape[1]

    def half(i):
        return lambda ref, z: ref.at[i, :, pl.ds(pl.multiple_of(z * depth, depth), depth)]

    qkv = DepthGather(place, qkv_ref, qkv_all, along_rows(depth), *take(3))
    out = DepthGather(place, out_ref, out_all, along_lanes(width), *take(3), passing=False)
    gate = DepthGather(place, gateup_ref.at[0], gateup_all, half(0), *take(3))
    up = DepthGather(place, gateup_ref.at[1], gateup_all, half(1), *take(3))
    down = DepthGather(place, down_ref, down_all, along_lanes(width), *take(3))
    rows = row_gather(place, row_block, rows_all, *take(3))
    cots = row_gather(place, cot_block, cot_all, *take(3))
    normeds = row_gather(place, row_block, rows_all, *take(3))
    scatter_refs = take(9)
    got, both, dsend, drecv = take(4)
    (save_sem,) = take(1)
    seq, d = rows_all.shape

    def save(i, src, dst):
        return pltpu.make_async_copy(src, dst, save_sem.at[i])

    saves = [
        save(0, rows_all, rows_out),
        save(1, qkv_all, qkv_out),
        save(2, out_all, out_out),
        save(3, gateup_all, gateup_out),
        save(4, down_all, down_out),
        save(5, gateup_all, grads_out),
    ]

    qkv.start()
    gain, shift = gain1_ref[...].astype(f32)[None, :], bias1_ref[...].astype(f32)[None, :]

    def norm1(at):
        normed, _ = normal(x_ref[at, :].astype(f32))
        row_block[at, :] = (normed * gain + shift).astype(bf16)
        cot_block[at, :] = cot_ref[at, :].astype(bf16)

    row_loop(x_ref.shape[0], norm1)
    rows.start()
    cots.start()
    head = qkv_ref.shape[2]
    shifts[...] = shift_ref[:, pl.ds(pl.multiple_of(place.c * head, head), head)].astype(f32)
    tables(perm_ref, cos_ref, sin_ref, pos_col, pos_row, x_ref.shape[0] // 2)
    rows.forward()
    qkv.forward_next()
    cots.forward()
    qkv.forward_far()
    out.start()
    gate.start()
    up.start()
    rows.finish()
    saves[0].start()
    cots.finish()
    qkv.finish()
    saves[1].start()
    attend(rows_all, qkv_all, shifts, cos_ref, sin_ref, pos_col, pos_row, q_t, k_t, v_t, attn_t, lse, k_n, bias, attn)
    gate.forward_next()
    out.finish()
    saves[2].start()
    saves[0].wait()
    scatter = sum_scatter(
        place,
        x_ref.shape[0],
        lambda at, cols: dot_nn(attn[at, :], out_all[:, cols]),
        *scatter_refs[:5],
        scatter_refs[5:9],
    )
    scatter.run()
    up.forward_next()
    gain2, shift2 = gain2_ref[...].astype(f32)[None, :], bias2_ref[...].astype(f32)[None, :]

    def norm2(at):
        resid = x_ref[at, :].astype(f32) + scatter.total(at)
        resid_ref[at, :] = resid
        normed, _ = normal(resid)
        row_block[at, :] = (normed * gain2 + shift2).astype(bf16)

    row_loop(x_ref.shape[0], norm2)
    normeds.start()
    gate.forward_far()
    normeds.forward()
    up.forward_far()
    down.start()
    normeds.finish()
    scatter.finish()
    gate.finish()

    def gates(t):
        at = span(t, PAIR)
        gate_f[at, :] = dot_nt(rows_all[at, :], gateup_all[0])

    tiles(seq // PAIR, gates)
    down.forward_next()
    up.finish()
    saves[3].start()

    def ups(t):
        at = span(t, PAIR)
        value = dot_nt(rows_all[at, :], gateup_all[1])
        g = gate_f[at, :]
        sigma = jax.nn.sigmoid(g)
        swish = g * sigma
        hidden = (swish * value).astype(bf16)
        hidden_ref[at, :] = hidden
        hidden_t[:, at] = hidden.T
        gate_side[at, :] = (value * sigma * (1.0 + g * (1.0 - sigma))).astype(bf16)
        up_side[at, :] = swish.astype(bf16)

    tiles(seq // PAIR, ups)

    def down_weights(j):
        cols = span(j, 2 * PAIR)
        part[:, cols] = dot_nn(hidden_t[...], cot_all[:, cols]).astype(bf16)

    tiles(d // (2 * PAIR), down_weights)
    summed = DepthScatter(place, part, got, both, width, dsend, drecv)
    summed.start()
    down.forward_far()
    summed.hand_on(0)
    summed.hand_on(1)
    down.finish()
    saves[4].start()
    summed.hand_on(2)
    saves[3].wait()

    def sides(t):
        at = span(t, PAIR)
        grad = dot_nt(cot_all[at, :], down_all[...])
        gate_grad = (grad * gate_side[at, :].astype(f32)).astype(bf16)
        up_grad = (grad * up_side[at, :].astype(f32)).astype(bf16)
        gate_side[at, :] = gate_grad
        up_side[at, :] = up_grad
        hidden_t[:, at] = gate_grad.T
        up_t[:, at] = up_grad.T

    tiles(seq // PAIR, sides)

    def gateup_weights(j):
        cols = span(j, 2 * PAIR)
        normed = rows_all[:, cols]
        gateup_all[0, :, cols] = dot_nn(hidden_t[...], normed).astype(bf16)
        gateup_all[1, :, cols] = dot_nn(up_t[...], normed).astype(bf16)

    tiles(d // (2 * PAIR), gateup_weights)
    saves[5].start()
    summed.finish(down_grads)
    for i in (1, 2, 4, 5):
        saves[i].wait()


def forward(perm, x, cot, gain1, bias1, gain2, bias2, shift, qkv, out, gateup, down):
    ndp, nctx = lax.axis_size("dp"), lax.axis_size("ctx")
    rows, d = x.shape
    seq, width, ff = rows * nctx, qkv.shape[2], gateup.shape[1]
    heads = width // HEAD_DIM
    bf16, f32 = jnp.bfloat16, jnp.float32
    row = [gain1, bias1, gain2, bias2]

    def shaped(shape, dtype=bf16):
        return jax.ShapeDtypeStruct(shape, dtype)

    return pl.pallas_call(
        forward_kernel,
        out_shape=(
            shaped((rows, d), f32),
            shaped((width, seq)),
            shaped((width, seq)),
            shaped((width, seq)),
            shaped((width, seq)),
            shaped((8, seq), f32),
            shaped((seq, ff)),
            shaped((seq, ff)),
            shaped((seq, ff)),
            shaped(down.shape, f32),
            shaped((8, seq), f32),
            shaped((8, seq), f32),
            shaped((seq, 1), f32),
            shaped((1, seq), f32),
            shaped((seq, d)),
            shaped((3, d, width)),
            shaped((width, d)),
            shaped((2, ff, d)),
            shaped((ff, d)),
            shaped((2, ff, d)),
        ),
        in_specs=[pl.BlockSpec(memory_space=pltpu.SMEM)] + [VMEM] * 7 + [ANY] * 4,
        out_specs=(VMEM,) * 14 + (ANY,) * 6,
        scratch_shapes=[
            pltpu.VMEM((rows, d), bf16),
            pltpu.VMEM((rows, d), bf16),
            pltpu.VMEM((seq, d), bf16),
            pltpu.VMEM((seq, d), bf16),
            pltpu.VMEM((3, d, width), bf16),
            pltpu.VMEM((width, d), bf16),
            pltpu.VMEM((2, ff, d), bf16),
            pltpu.VMEM((ff, d), bf16),
            pltpu.VMEM((heads, seq, HEAD_DIM), bf16),
            pltpu.VMEM((seq, PAIR), f32),
            pltpu.VMEM((seq, width), bf16),
            pltpu.VMEM((seq, ff), f32),
            pltpu.VMEM((ff, seq), bf16),
            pltpu.VMEM((ff, seq), bf16),
            pltpu.VMEM((ff, d), bf16),
            pltpu.VMEM((3, width), f32),
        ]
        + depth_sems(ndp) * 5
        + gather_sems(nctx) * 3
        + scatter_scratch(nctx, rows, d)
        + depth_scatter_scratch(ndp, ff, d // ndp)
        + [DMA((6,))],
        compiler_params=pltpu.CompilerParams(
            collective_id=0, has_side_effects=True, vmem_limit_bytes=67_000_000
        ),
        cost_estimate=pl.CostEstimate(flops=0, bytes_accessed=700_000_000, transcendentals=0),
        name="forward",
    )(perm, x, cot, *row, shift, qkv, out, gateup, down)


def attend_back_kernel(
    grad_ref, w_ref, rows_ref, cos_ref, sin_ref, pos_col, pos_row, q_t, k_t, v_t, attn_t, lse,
    parts_ref, sums_ref, w_grads, g_t, delta, q_grad, kv_grad, bias, flat
):
    seq, d = grad_ref.shape
    width = w_ref.shape[0]
    heads = width // HEAD_DIM
    bf16, f32 = jnp.bfloat16, jnp.float32

    def first(t):
        at = span(t, PAIR)
        grad = dot_nt(w_ref[...], grad_ref[at, :])
        both = grad * attn_t[:, at].astype(f32)
        for h in range(heads):
            delta[h : h + 1, at] = jnp.sum(both[h * HEAD_DIM : (h + 1) * HEAD_DIM], axis=0, keepdims=True)
        g_t[:, at] = grad.astype(bf16)

    tiles(seq // PAIR, first)
    q_grad[...] = jnp.zeros_like(q_grad)

    def keys(t):
        at = span(t, PAIR)
        bias[...] = jnp.where(pos_col[at, :] <= pos_row[...], 0.0, neg_big)
        for h in range(heads):
            feats = slice(h * HEAD_DIM, (h + 1) * HEAD_DIM)
            keys_t = k_t[feats, at]
            probs = jnp.exp(dot_nn(keys_t.T, q_t[feats, :]) + bias[...] - lse[h : h + 1, :])
            kv_grad[1, feats, at] = dot_nt(g_t[feats, :], probs.astype(bf16))
            back = dot_nn(v_t[feats, at].T, g_t[feats, :])
            scores = (probs * (back - delta[h : h + 1, :])).astype(bf16)
            kv_grad[0, feats, at] = dot_nt(q_t[feats, :], scores)
            q_grad[feats, :] += dot_nn(keys_t, scores)

    tiles(seq // PAIR, keys)
    sums_ref[...] = jnp.zeros_like(sums_ref)

    def part(t):
        at = span(t, PAIR)
        cosine, sine = cos_ref[:, at], sin_ref[:, at]
        for i in range(3):
            if i == 0:
                grad = turn(q_grad[:, at] * (1.0 / math.sqrt(HEAD_DIM)), cosine, -sine, heads)
            elif i == 1:
                grad = turn(kv_grad[0, :, at], cosine, -sine, heads)
            else:
                grad = kv_grad[1, :, at]
            natural = grad.T
            sums_ref[i : i + 1, :] += jnp.sum(natural, axis=0, keepdims=True)
            parts_ref[i, at, :] = natural.astype(bf16)
            flat[i, :, at] = grad.astype(bf16)

    tiles(seq // PAIR, part)

    def weights(j):
        cols = span(j, 2 * PAIR)
        rows = rows_ref[:, cols]
        for i in range(3):
            w_grads[i, cols, :] = dot_nn(flat[i], rows).T.astype(bf16)
        w_grads[3, cols, :] = dot_nn(attn_t[...], grad_ref[:, cols]).T.astype(bf16)

    tiles(d // (2 * PAIR), weights)


def attention_back(grad_all, w, rows_all, cosine, sine, pos_col, pos_row, q_t, k_t, v_t, attn_t, lse):
    seq, d = rows_all.shape
    width = w.shape[0]
    bf16, f32 = jnp.bfloat16, jnp.float32
    return pl.pallas_call(
        attend_back_kernel,
        out_shape=(
            jax.ShapeDtypeStruct((3, seq, width), bf16),
            jax.ShapeDtypeStruct((3, width), f32),
            jax.ShapeDtypeStruct((4, d, width), bf16),
        ),
        in_specs=[VMEM] * 12,
        out_specs=(VMEM,) * 3,
        scratch_shapes=[
            pltpu.VMEM((width, seq), bf16),
            pltpu.VMEM((8, seq), f32),
            pltpu.VMEM((width, seq), f32),
            pltpu.VMEM((2, width, seq), f32),
            pltpu.VMEM((PAIR, seq), f32),
            pltpu.VMEM((3, width, seq), bf16),
        ],
        cost_estimate=pl.CostEstimate(flops=0, bytes_accessed=120_000_000, transcendentals=0),
        name="attention_back",
    )(grad_all, w, rows_all, cosine, sine, pos_col, pos_row, q_t, k_t, v_t, attn_t, lse)


def shard(grad, dim):
    return lax.psum_scatter(grad, "dp", scatter_dimension=dim, tiled=True)


def per_device(
    block_input,
    out_cotangent,
    group_perm,
    attn_norm_gain,
    attn_norm_bias,
    qkv_weight,
    qkv_bias,
    out_weight,
    mlp_norm_gain,
    mlp_norm_bias,
    gateup_weight,
    down_weight,
):
    width_local = qkv_weight.shape[2]
    (
        residual_stream, q_t, k_t, v_t, attn_t, lse, hidden_b, gate_grad, up_grad, down_grads, cos_all, sin_all, pos_col, pos_row,
        rows_all, qkv_local, out_local, gateup_local, down_local, gateup_grads,
    ) = forward(
        group_perm, block_input, out_cotangent, attn_norm_gain, attn_norm_bias, mlp_norm_gain, mlp_norm_bias, qkv_bias,
        qkv_weight, out_weight, gateup_weight.transpose(0, 2, 1), down_weight,
    )
    gateup_grads = shard(gateup_grads, 2)
    resid_grad, second_vectors, resid_all = mlp_back(
        gate_grad, up_grad, gateup_local, residual_stream, out_cotangent, mlp_norm_gain
    )
    grad_parts_b, shift_part, attn_grads = attention_back(
        resid_all, out_local, rows_all, cos_all, sin_all, pos_col, pos_row, q_t, k_t, v_t, attn_t, lse
    )
    head_first = lax.axis_index("ctx") * width_local
    f32 = jnp.float32
    shift_grad = lax.dynamic_update_slice_in_dim(jnp.zeros((3, D), f32), shift_part, head_first, 1)
    attn_grads = shard(attn_grads, 1)
    input_grad, first_vectors = attn_back(grad_parts_b, qkv_local, block_input, resid_grad, attn_norm_gain)
    hidden_late, first_vectors, gateup_grads = lax.optimization_barrier((hidden_b, first_vectors, gateup_grads))
    block_output = down(hidden_late, down_local, residual_stream)
    small = sum_vectors(
        jnp.concatenate([first_vectors, second_vectors, shift_grad, jnp.zeros((1, D), f32)], axis=0)
    )
    small, block_output, attn_grads = lax.optimization_barrier((small, block_output, attn_grads))
    attn_grads = attn_grads.astype(f32)
    return (
        block_output,
        input_grad,
        small[0],
        small[1],
        attn_grads[:3],
        small[4:7],
        attn_grads[3].T,
        small[2],
        small[3],
        gateup_grads.astype(f32).transpose(0, 2, 1),
        down_grads,
    )


def solution(mesh):
    return jax.shard_map(
        per_device,
        mesh=mesh,
        in_specs=(
            P(("dp", "ctx"), None),
            P(("dp", "ctx"), None),
            P("dp", None),
            P(),
            P(),
            P(None, "dp", "ctx"),
            P(),
            P("ctx", "dp"),
            P(),
            P(),
            P(None, "dp", "ctx"),
            P("ctx", "dp"),
        ),
        out_specs=(
            P(("dp", "ctx"), None),
            P(("dp", "ctx"), None),
            P(),
            P(),
            P(None, "dp", "ctx"),
            P(),
            P("ctx", "dp"),
            P(),
            P(),
            P(None, "dp", "ctx"),
            P("ctx", "dp"),
        ),
        check_vma=False,
    )
```

```python
import functools
import math

import jax
import jax.numpy as jnp
from jax import lax
from jax.experimental import pallas as pl
from jax.experimental.pallas import tpu as pltpu
from jax.sharding import PartitionSpec as P

MESH = pl.DeviceIdType.MESH
VMEM = pl.BlockSpec(memory_space=pltpu.VMEM)
ANY = pl.BlockSpec(memory_space=pl.ANY)
DMA = pltpu.SemaphoreType.DMA

D = 2048
HEADS = 32
HEAD_DIM = 64
ROT = 16


eps_norm = 1e-05
rope_base = 10000.0
neg_big = -1e30


class Place:
    def __init__(self):
        self.ndp = lax.axis_size("dp")
        self.nctx = lax.axis_size("ctx")
        self.nchip = self.nctx // 2
        self.z = lax.axis_index("dp")
        self.c = lax.axis_index("ctx")
        self.p = lax.div(self.c, 2)
        self.k = lax.rem(self.c, 2)

    def chip(self, offset):
        return lax.rem(self.p + offset, self.nchip)

    def at(self, c):
        return {"dp": self.z, "ctx": c}

    def partner(self):
        return self.at(2 * self.p + 1 - self.k)

    def same_core(self, q):
        return self.at(2 * q + self.k)


def greet(place, along_ctx=True, along_dp=False, all_ctx=False):
    barrier = pltpu.get_barrier_semaphore()
    peers = []
    if all_ctx:
        peers += [place.at(lax.rem(place.c + i, place.nctx)) for i in range(1, place.nctx)]
    elif along_ctx:
        peers += [place.partner()] + [place.same_core(place.chip(i)) for i in range(1, place.nchip)]
    if along_dp:
        peers += [{"dp": lax.rem(place.z + i, place.ndp), "ctx": place.c} for i in range(1, place.ndp)]
    for peer in peers:
        pl.semaphore_signal(barrier, inc=1, device_id=peer, device_id_type=MESH)
    pl.semaphore_wait(barrier, len(peers))


def push(src, dst, send, recv, device):
    return pltpu.make_async_remote_copy(
        src_ref=src, dst_ref=dst, send_sem=send, recv_sem=recv, device_id=device, device_id_type=MESH
    )


class RowGather:
    def __init__(self, place, block, whole, send, recv, local):
        self.place, self.block, self.whole = place, block, whole
        self.send, self.recv, self.local = send, recv, local
        self.rows = block.shape[0]

    def slot(self, c):
        return self.whole.at[pl.ds(pl.multiple_of(c * self.rows, self.rows), self.rows)]

    def direct(self, i):
        place = self.place
        q = place.chip(i)
        return push(self.block, self.slot(place.c), self.send.at[i], self.recv.at[place.c], place.same_core(q))

    def own(self):
        place = self.place
        return push(self.block, self.slot(place.c), self.send.at[0], self.recv.at[place.c], place.partner())

    def passed(self, i):
        place = self.place
        c = 2 * place.chip(i) + place.k
        return push(
            self.slot(c), self.slot(c), self.send.at[place.nchip + i - 1], self.recv.at[c], place.partner()
        )

    def arrival(self, c):
        return push(self.block, self.slot(c), self.send.at[0], self.recv.at[c], self.place.partner())

    def keep(self):
        return pltpu.make_async_copy(self.block, self.slot(self.place.c), self.local)

    def start(self):
        for i in range(1, self.place.nchip):
            self.direct(i).start()
        self.own().start()
        self.keep().start()

    def forward(self):
        place = self.place
        for i in range(1, place.nchip):
            self.arrival(2 * place.chip(i) + place.k).wait_recv()
            self.passed(i).start()

    def finish(self):
        place = self.place
        for i in range(place.nchip):
            self.arrival(2 * place.chip(i) + 1 - place.k).wait_recv()
        self.own().wait_send()
        for i in range(1, place.nchip):
            self.direct(i).wait_send()
            self.passed(i).wait_send()
        self.keep().wait()


class BoxGather(RowGather):
    def part(self, c, half):
        size = self.rows // 2
        return self.whole.at[pl.ds(pl.multiple_of(c * self.rows + half * size, size), size)]

    def near(self, axis):
        place = self.place
        other = 1 - lax.rem(place.p, 2) if axis == 0 else 1 - lax.div(place.p, 2)
        q = 2 * lax.div(place.p, 2) + other if axis == 0 else 2 * other + lax.rem(place.p, 2)
        return 2 * q + place.k

    def across(self):
        return 2 * (3 - self.place.p) + self.place.k

    def piece(self, c, half, sem, to, own=False):
        size = self.rows // 2
        src = self.block.at[pl.ds(half * size, size)] if own else self.part(c, half)
        return push(src, self.part(c, half), self.send.at[sem], self.recv.at[2 * c + half], self.place.at(to))

    def own(self):
        place = self.place
        return push(self.block, self.slot(place.c), self.send.at[0], self.recv.at[2 * place.c], place.partner())

    def first(self):
        c = self.place.c
        return [self.piece(c, h, 1 + n, self.near(a), True) for n, (a, h) in enumerate(((0, 0), (1, 1), (0, 1), (1, 0)))]

    def second(self):
        return [self.piece(self.near(a), a, 5 + a, self.near(1 - a)) for a in (0, 1)]

    def to_partner(self):
        place = self.place
        pair = 2 * place.p + 1 - place.k
        return [
            self.piece(c, h, 7 + n, pair)
            for n, (c, h) in enumerate(
                ((self.near(0), 0), (self.near(1), 1), (self.near(0), 1), (self.near(1), 0), (self.across(), 0), (self.across(), 1))
            )
        ]

    def start(self):
        for copy in self.first():
            copy.start()
        self.own().start()
        self.keep().start()

    def forward(self):
        second, pair = self.second(), self.to_partner()
        for n, copy in enumerate(pair):
            copy.wait_recv()
            if n < 2:
                second[n].start()
            copy.start()

    def finish(self):
        place = self.place
        pair = 2 * place.p + 1 - place.k
        self.arrival_pair().wait_recv()
        for n in range(6):
            c = (self.near(0), self.near(1), self.near(0), self.near(1), self.across(), self.across())[n]
            half = (0, 1, 1, 0, 0, 1)[n]
            twin = c + 1 - 2 * place.k
            self.piece(twin, half, 7 + n, pair).wait_recv()
        self.own().wait_send()
        for copy in self.first() + self.second() + self.to_partner():
            copy.wait_send()
        self.keep().wait()

    def arrival_pair(self):
        c = self.place.c + 1 - 2 * self.place.k
        return push(self.block, self.slot(c), self.send.at[0], self.recv.at[2 * c], self.place.partner())


def row_gather(place, *args):
    return (BoxGather if place.nchip == 4 else RowGather)(place, *args)


def gather_sems(nctx):
    return [DMA((13,)), DMA((2 * nctx,)), DMA] if nctx == 8 else [DMA((nctx,)), DMA((nctx,)), DMA]


class DepthGather:
    def __init__(self, place, piece, whole, where, send, recv, local, passing=True):
        self.place, self.piece, self.whole, self.where = place, piece, whole, where
        self.send, self.recv, self.local = send, recv, local
        self.line = place.ndp == 4 and passing
        z = place.z
        self.end = jnp.logical_or(z == 0, z == 3)
        self.middle = jnp.logical_not(self.end)
        self.near = jnp.clip(3 * (z - 1), 0, 3)
        self.far = 3 - self.near
        self.other = jnp.clip(3 - z, 1, 2)

    def copy(self, src, z_src, z_dst, sem):
        return push(
            src, self.where(self.whole, z_src), self.send.at[sem], self.recv.at[z_src], {"dp": z_dst, "ctx": self.place.c}
        )

    def directs(self):
        z, n = self.place.z, self.place.ndp
        if not self.line:
            return [(None, self.copy(self.piece, z, lax.rem(z + i, n), i - 1)) for i in range(1, n)]
        out = []
        for sem, step in enumerate((1, -1, 2, -2)):
            d = z + step
            ok = jnp.logical_and(d >= 0, d < 4)
            if abs(step) == 2:
                ok = jnp.logical_and(ok, self.end)
            out.append((ok, self.copy(self.piece, z, jnp.clip(d, 0, 3), sem)))
        return out

    def keep(self):
        return pltpu.make_async_copy(self.piece, self.where(self.whole, self.place.z), self.local)

    def start(self):
        for ok, copy in self.directs():
            if ok is None:
                copy.start()
            else:
                pl.when(ok)(copy.start)
        self.keep().start()

    def passed(self, src, sem):
        return self.copy(self.where(self.whole, src), src, self.near, sem)

    def forward_next(self):
        self.forward(self.other, 4)

    def forward_far(self):
        self.forward(self.far, 5)

    def forward(self, src, sem):
        if self.line:

            @pl.when(self.middle)
            def _():
                self.copy(self.piece, src, src, sem).wait_recv()
                self.passed(src, sem).start()

    def finish(self):
        z, n = self.place.z, self.place.ndp
        for i in range(1, n):
            src = lax.rem(z + i, n)
            wait = self.copy(self.piece, src, src, 0).wait_recv
            if self.line:
                pl.when(jnp.logical_or(self.end, src == self.near))(wait)
            else:
                wait()
        for ok, copy in self.directs():
            if ok is None:
                copy.wait_send()
            else:
                pl.when(ok)(copy.wait_send)
        if self.line:

            @pl.when(self.middle)
            def _():
                self.passed(self.other, 4).wait_send()
                self.passed(self.far, 5).wait_send()

        self.keep().wait()


def depth_sems(ndp):
    return [DMA((max(ndp, 6),)), DMA((ndp,)), DMA]


STEP = 16


def row_loop(rows, body):
    def step(i, carry):
        body(pl.ds(pl.multiple_of(i * STEP, STEP), STEP))
        return carry

    lax.fori_loop(0, rows // STEP, step, 0)


def normal(values):
    centred = values - jnp.mean(values, axis=-1, keepdims=True)
    rscale = lax.rsqrt(jnp.mean(centred * centred, axis=-1, keepdims=True) + eps_norm)
    return centred * rscale, rscale


def normal_back(grad_out, normed, rscale, gain):
    scaled = grad_out * gain
    return rscale * (
        scaled
        - jnp.mean(scaled, axis=-1, keepdims=True)
        - normed * jnp.mean(scaled * normed, axis=-1, keepdims=True)
    )


class SumScatter:
    TILE = 512

    def __init__(self, place, rows, product, mine, to_pair, from_pair, to_chip, from_chip, sems):
        self.place, self.rows, self.product = place, rows, product
        self.mine, self.to_pair, self.from_pair = mine, to_pair, from_pair
        self.to_chip, self.from_chip = to_chip, from_chip
        self.pair_send, self.pair_recv, self.chip_send, self.chip_recv = sems

    def pair(self, i):
        return push(
            self.to_pair.at[lax.rem(i, 2)], self.from_pair.at[i], self.pair_send.at[i], self.pair_recv.at[i], self.place.partner()
        )

    def chips(self, i):
        return push(
            self.to_chip.at[i],
            self.from_chip.at[i],
            self.chip_send.at[i],
            self.chip_recv.at[i],
            self.place.same_core(self.place.chip(i + 1)),
        )

    def chip_of(self, i):
        return lax.rem(self.place.p + 1 + i, self.place.nchip)

    def hand_on(self, i):
        self.pair(i).wait_recv()

        def add(at):
            both = self.mine[lax.rem(i, 2), at, :] + self.from_pair[i, at, :].astype(jnp.float32)
            self.to_chip[i, at, :] = both.astype(jnp.bfloat16)

        row_loop(self.rows, add)
        self.chips(i).start()

    def last(self, hooks):
        for hook in hooks:
            hook()
        nchip = self.place.nchip
        self.pair(nchip - 1).wait_recv()
        for i in range(nchip - 1):
            self.chips(i).wait_recv()

    def run(self, hooks=()):
        place, rows, tile = self.place, self.rows, self.TILE
        nchip = place.nchip
        width = self.mine.shape[-1]

        def step(i, carry):
            first = pl.multiple_of(self.chip_of(i) * 2 * rows, 2 * rows)
            slot = lax.rem(i, 2)
            pl.when(i >= 2)(lambda: self.pair(i - 2).wait_send())

            def columns(j, inner):
                cols = pl.ds(pl.multiple_of(j * tile, tile), tile)
                part = self.product(pl.ds(first, 2 * rows), cols)

                @pl.when(place.k == 0)
                def _():
                    self.mine[slot, :, cols] = part[:rows]
                    self.to_pair[slot, :, cols] = part[rows:].astype(jnp.bfloat16)

                @pl.when(place.k == 1)
                def _():
                    self.mine[slot, :, cols] = part[rows:]
                    self.to_pair[slot, :, cols] = part[:rows].astype(jnp.bfloat16)

                return inner

            lax.fori_loop(0, width // tile, columns, 0)
            self.pair(i).start()
            pl.when(i > 0)(lambda: self.hand_on(i - 1))
            return carry

        lax.fori_loop(0, nchip, step, 0)
        self.last(list(hooks))

    def total(self, at):
        last = self.place.nchip - 1
        value = self.mine[last % 2, at, :] + self.from_pair[last, at, :].astype(jnp.float32)
        for i in range(last):
            value = value + self.from_chip[i, at, :].astype(jnp.float32)
        return value

    def finish(self):
        for i in range(max(self.place.nchip - 2, 0), self.place.nchip):
            self.pair(i).wait_send()
        for i in range(self.place.nchip - 1):
            self.chips(i).wait_send()


class BoxScatter(SumScatter):
    def near(self, axis):
        p = self.place.p
        x, y = lax.rem(p, 2), lax.div(p, 2)
        return self.place.same_core(2 * y + 1 - x if axis == 0 else 2 * (1 - y) + x)

    def half(self, src, dst, rows, sem, axis):
        size = self.rows // 2
        at = pl.ds(rows * size, size)
        return push(
            self.to_chip.at[src, at], self.from_chip.at[dst, at], self.chip_send.at[sem], self.chip_recv.at[sem], self.near(axis)
        )

    def moves(self):
        return [
            self.half(0, 2, 0, 0, 0),
            self.half(0, 2, 1, 1, 1),
            self.half(1, 0, 0, 2, 0),
            self.half(2, 1, 1, 3, 1),
            self.half(1, 0, 1, 4, 0),
            self.half(2, 1, 0, 5, 1),
        ]

    def chip_of(self, i):
        p = self.place.p
        x, y = lax.rem(p, 2), lax.div(p, 2)
        other_x = jnp.logical_or(i == 0, i == 1)
        other_y = jnp.logical_or(i == 0, i == 2)
        return 2 * jnp.where(other_y, 1 - y, y) + jnp.where(other_x, 1 - x, x)

    def hand_on(self, i):
        self.pair(i).wait_recv()
        slot = lax.rem(i, 2)

        def add(at):
            both = self.mine[slot, at, :] + self.from_pair[i, at, :].astype(jnp.float32)
            self.to_chip[i, at, :] = both.astype(jnp.bfloat16)

        row_loop(self.rows, add)
        moves = self.moves()

        @pl.when(i == 0)
        def _():
            moves[0].start()
            moves[1].start()

        pl.when(i == 1)(moves[2].start)
        pl.when(i == 2)(moves[3].start)

    def last(self, hooks):
        moves = self.moves()
        size = self.rows // 2
        for arrived, src, first, onward in ((1, 1, size, 4), (0, 2, 0, 5)):
            if hooks:
                hooks.pop(0)()
            moves[arrived].wait_recv()

            def add(at, src=src, first=first):
                at = pl.ds(pl.multiple_of(first + at.start, STEP), STEP)
                both = self.to_chip[src, at, :].astype(jnp.float32) + self.from_chip[2, at, :].astype(jnp.float32)
                self.to_chip[src, at, :] = both.astype(jnp.bfloat16)

            row_loop(size, add)
            moves[onward].start()
        self.pair(3).wait_recv()
        for n in (2, 3, 4, 5):
            moves[n].wait_recv()

    def total(self, at):
        value = self.mine[1, at, :] + self.from_pair[3, at, :].astype(jnp.float32)
        return value + self.from_chip[0, at, :].astype(jnp.float32) + self.from_chip[1, at, :].astype(jnp.float32)

    def finish(self):
        for i in (2, 3):
            self.pair(i).wait_send()
        for copy in self.moves():
            copy.wait_send()


def sum_scatter(place, *args):
    return (BoxScatter if place.nchip == 4 else SumScatter)(place, *args)


def scatter_scratch(nctx, rows, d):
    n = nctx // 2
    bf16 = jnp.bfloat16
    return [
        pltpu.VMEM((2, rows, d), jnp.float32),
        pltpu.VMEM((2, rows, d), bf16),
        pltpu.VMEM((n, rows, d), bf16),
        pltpu.VMEM((n - 1, rows, d), bf16),
        pltpu.VMEM((n - 1, rows, d), bf16),
        DMA((n,)),
        DMA((n,)),
        DMA((6 if n == 4 else n - 1,)),
        DMA((6 if n == 4 else n - 1,)),
    ]


def dot_nn(a, b):
    return jnp.dot(a, b, preferred_element_type=jnp.float32)


def dot_nt(a, b):
    return lax.dot_general(a, b, (((1,), (1,)), ((), ())), preferred_element_type=jnp.float32)


HALF = ROT // 2
PAIR = 256


def tiles(count, body):
    def step(i, carry):
        body(i)
        return carry

    lax.fori_loop(0, count, step, 0)


def span(i, size):
    return pl.ds(pl.multiple_of(i * size, size), size)


def turn(columns, cosine, sine, heads):
    out = []
    for h in range(heads):
        at = h * HEAD_DIM
        a, b = columns[at : at + HALF], columns[at + HALF : at + ROT]
        out += [a * cosine - b * sine, b * cosine + a * sine, columns[at + ROT : at + HEAD_DIM]]
    return jnp.concatenate(out, axis=0)


def attend(rows_ref, w_ref, shift_ref, cos_ref, sin_ref, pos_col, pos_row, q_t, k_t, v_t, attn_t, lse, k_n, bias, attn):
    seq = rows_ref.shape[0]
    width = w_ref.shape[2]
    heads = width // HEAD_DIM
    bf16 = jnp.bfloat16

    def project(t):
        at = span(t, PAIR)
        cosine, sine = cos_ref[:, at], sin_ref[:, at]
        for i, ref in enumerate((q_t, k_t, v_t)):
            raw = (dot_nn(rows_ref[at, :], w_ref[i]) + shift_ref[i : i + 1, :]).T
            if i < 2:
                raw = turn(raw, cosine, sine, heads)
            raw = raw.astype(bf16)
            if i == 0:
                raw = raw * jnp.asarray(1.0 / math.sqrt(HEAD_DIM), bf16)
            ref[:, at] = raw

    tiles(seq // PAIR, project)
    for h in range(heads):
        k_n[h] = k_t[h * HEAD_DIM : (h + 1) * HEAD_DIM, :].T

    def queries(t):
        at = span(t, PAIR)
        bias[...] = jnp.where(pos_col[...] <= pos_row[:, at], 0.0, neg_big)

        for h in range(heads):
            feats = slice(h * HEAD_DIM, (h + 1) * HEAD_DIM)
            scores = dot_nn(k_n[h], q_t[feats, at]) + bias[...]
            peak = jnp.max(scores, axis=0, keepdims=True)
            probs = jnp.exp(scores - peak)
            total = jnp.sum(probs, axis=0, keepdims=True)
            out = dot_nn(v_t[feats, :], probs.astype(bf16)) / total
            attn_t[feats, at] = out.astype(bf16)
            lse[h : h + 1, at] = peak + jnp.log(total)
        attn[at, :] = attn_t[:, at].T

    tiles(seq // PAIR, queries)


class DepthScatter:
    def __init__(self, place, source, part, got, both, width, send, recv):
        self.place, self.source, self.part = place, source, part
        self.got, self.both, self.width = got, both, width
        self.send, self.recv = send, recv
        self.line = place.ndp == 4
        z = place.z
        self.end = jnp.logical_or(z == 0, z == 3)
        self.middle = jnp.logical_not(self.end)
        self.next = jnp.where(z == 3, 2, 1)
        self.other = jnp.clip(3 - z, 1, 2)
        self.near = jnp.clip(3 * (z - 1), 0, 3)

    def block(self, z):
        return self.source.at[:, pl.ds(pl.multiple_of(z * self.width, self.width), self.width)]

    def copy(self, src, slot, sem, z):
        return push(src, self.got.at[slot], self.send.at[sem], self.recv.at[slot], {"dp": z, "ctx": self.place.c})

    def from_end(self):
        far = 3 - self.place.z
        return [
            self.copy(self.block(far), 2, 0, self.next),
            self.copy(self.block(3 - self.next), 3, 1, self.next),
            self.copy(self.block(self.next), 0, 2, self.next),
        ]

    def from_middle(self):
        return [
            self.copy(self.both.at[0], 4, 0, self.other),
            self.copy(self.both.at[1], 1, 1, self.other),
            self.copy(self.both.at[2], 0, 2, self.near),
        ]

    def across(self):
        z, n = self.place.z, self.place.ndp
        return [self.copy(self.block(lax.rem(z + i, n)), i - 1, i - 1, lax.rem(z + i, n)) for i in range(1, n)]

    def start(self):
        if not self.line:
            for copy in self.across():
                copy.start()
            return

        @pl.when(self.end)
        def _():
            for copy in self.from_end():
                copy.start()

    def hand_on(self, n):
        if not self.line:
            return

        @pl.when(self.middle)
        def _():
            owner, slot = ((3 - self.near, 2), (self.other, 3), (self.near, 4))[n]
            self.copy(self.both.at[0], slot, 0, self.near).wait_recv()
            cols = pl.ds(pl.multiple_of(owner * self.width, self.width), self.width)

            def add(at):
                total = self.part[at, cols].astype(jnp.float32) + self.got[slot, at, :].astype(jnp.float32)
                self.both[n, at, :] = total.astype(jnp.bfloat16)

            row_loop(self.part.shape[0], add)
            self.from_middle()[n].start()

    def collect(self, count, out_ref):
        for slot in range(count):
            self.copy(self.got.at[slot], slot, 0, self.next).wait_recv()
        cols = pl.ds(pl.multiple_of(self.place.z * self.width, self.width), self.width)

        def add(at):
            value = self.part[at, cols].astype(jnp.float32)
            for slot in range(count):
                value = value + self.got[slot, at, :].astype(jnp.float32)
            out_ref[at, :] = value

        row_loop(self.part.shape[0], add)

    def finish(self, out_ref):
        if not self.line:
            self.collect(self.place.ndp - 1, out_ref)
            for copy in self.across():
                copy.wait_send()
            return

        @pl.when(self.end)
        def _():
            self.collect(1, out_ref)
            for copy in self.from_end():
                copy.wait_send()

        @pl.when(self.middle)
        def _():
            self.collect(2, out_ref)
            for copy in self.from_middle():
                copy.wait_send()


def depth_scatter_scratch(ndp, rows, width):
    slots = 5 if ndp == 4 else ndp - 1
    return [
        pltpu.VMEM((slots, rows, width), jnp.bfloat16),
        pltpu.VMEM((3, rows, width), jnp.bfloat16),
        DMA((max(slots, 3),)),
        DMA((slots,)),
    ]


def tables(perm_ref, cos_ref, sin_ref, pos_col, pos_row, size):
    seq = pos_row.shape[1]
    lane = lax.broadcasted_iota(jnp.int32, (8, seq), 1)
    group = lane // size
    start = jnp.zeros((8, seq), jnp.int32)
    for g in range(seq // size):
        start = jnp.where(group == g, perm_ref[0, g], start)
    pos = (start * size + lane - group * size).astype(jnp.float32)
    pos_row[...] = pos[0:1]
    pos_col[...] = pos.T[:, 0:1]
    step = lax.broadcasted_iota(jnp.int32, (8, seq), 0).astype(jnp.float32)
    angle = pos * jnp.exp(step * (-2.0 / ROT * math.log(rope_base)))
    cos_ref[...] = jnp.cos(angle)
    sin_ref[...] = jnp.sin(angle)


def forward_kernel(
    perm_ref, x_ref, cot_ref, gain1_ref, bias1_ref, gain2_ref, bias2_ref, shift_ref,
    qkv_ref, out_ref, gateup_ref, down_ref,
    resid_ref, q_t, k_t, v_t, attn_t, lse, hidden_ref, gate_side, up_side, first_sums, cos_ref, sin_ref, pos_col, pos_row,
    rows_out, qkv_out, out_out, gateup_out, down_out, grads_out,
    row_block, cot_block, rows_all, cot_all, qkv_all, out_all, gateup_all, down_all,
    k_n, bias, attn, gate_f, hidden_t, gate_t, up_t, part, shifts, *sems
):
    f32, bf16 = jnp.float32, jnp.bfloat16
    place = Place()
    greet(place, along_dp=True)
    sems = list(sems)

    def take(n):
        head = sems[:n]
        del sems[:n]
        return head

    def along_rows(size):
        return lambda ref, z: ref.at[:, pl.ds(pl.multiple_of(z * size, size), size), :]

    def along_lanes(size):
        return lambda ref, z: ref.at[:, pl.ds(pl.multiple_of(z * size, size), size)]

    depth, width = qkv_ref.shape[1], out_ref.shape[1]

    ff = gateup_ref.shape[1]
    half = ff // 2

    def slab(first):
        return lambda ref, z: ref.at[pl.ds(first, half), pl.ds(pl.multiple_of(z * depth, depth), depth)]

    qkv = DepthGather(place, qkv_ref, qkv_all, along_rows(depth), *take(3))
    out = DepthGather(place, out_ref, out_all, along_lanes(width), *take(3), passing=False)
    gate, up, down = [], [], []
    for h in range(2):
        at = pl.ds(h * half, half)
        gate.append(DepthGather(place, gateup_ref.at[0, at], gateup_all, slab(h * half), *take(3)))
        up.append(DepthGather(place, gateup_ref.at[1, at], gateup_all, slab(ff + h * half), *take(3)))
        down.append(DepthGather(place, down_ref.at[at], down_all, slab(h * half), *take(3)))
    rows = row_gather(place, row_block, rows_all, *take(3))
    cots = row_gather(place, cot_block, cot_all, *take(3))
    normeds = row_gather(place, row_block, rows_all, *take(3))
    scatter_refs = take(9)
    got, both, dsend, drecv = take(4)
    (save_sem,) = take(1)
    seq, d = rows_all.shape

    def save(i, src, dst):
        return pltpu.make_async_copy(src, dst, save_sem.at[i])

    saves = [
        save(0, rows_all, rows_out),
        save(1, qkv_all, qkv_out),
        save(2, out_all, out_out),
        save(3, gateup_all, gateup_out),
        save(4, down_all, down_out),
        save(5, gateup_all.at[pl.ds(0, 3 * half)], grads_out),
    ]

    qkv.start()
    gain, shift = gain1_ref[...].astype(f32)[None, :], bias1_ref[...].astype(f32)[None, :]

    def norm1(at):
        normed, _ = normal(x_ref[at, :].astype(f32))
        row_block[at, :] = (normed * gain + shift).astype(bf16)
        cot_block[at, :] = cot_ref[at, :].astype(bf16)

    row_loop(x_ref.shape[0], norm1)
    rows.start()
    cots.start()
    head = qkv_ref.shape[2]
    shifts[...] = shift_ref[:, pl.ds(pl.multiple_of(place.c * head, head), head)].astype(f32)
    tables(perm_ref, cos_ref, sin_ref, pos_col, pos_row, x_ref.shape[0] // 2)
    rows.forward()
    qkv.forward_next()
    cots.forward()
    qkv.forward_far()
    out.start()
    gate[0].start()
    up[0].start()
    rows.finish()
    saves[0].start()
    cots.finish()
    qkv.finish()
    saves[1].start()
    attend(rows_all, qkv_all, shifts, cos_ref, sin_ref, pos_col, pos_row, q_t, k_t, v_t, attn_t, lse, k_n, bias, attn)
    gate[0].forward_next()
    up[0].forward_next()
    down[0].start()
    gate[1].start()
    out.finish()
    saves[2].start()
    saves[0].wait()
    scatter = sum_scatter(
        place,
        x_ref.shape[0],
        lambda at, cols: dot_nn(attn[at, :], out_all[:, cols]),
        *scatter_refs[:5],
        scatter_refs[5:9],
    )
    scatter.run()
    gate[0].forward_far()
    up[0].forward_far()
    down[0].forward_next()
    gain2, shift2 = gain2_ref[...].astype(f32)[None, :], bias2_ref[...].astype(f32)[None, :]

    def norm2(at):
        resid = x_ref[at, :].astype(f32) + scatter.total(at)
        resid_ref[at, :] = resid
        normed, _ = normal(resid)
        row_block[at, :] = (normed * gain2 + shift2).astype(bf16)

    row_loop(x_ref.shape[0], norm2)
    normeds.start()
    normeds.forward()
    down[0].forward_far()
    gate[1].forward_next()
    up[1].start()
    normeds.finish()
    scatter.finish()

    def gates(h):
        def body(t):
            at = span(t, PAIR)
            gate_f[at, :] = dot_nt(rows_all[at, :], gateup_all[h * half : (h + 1) * half, :])

        tiles(seq // PAIR, body)

    def ups(h):
        def body(t):
            at = span(t, PAIR)
            value = dot_nt(rows_all[at, :], gateup_all[ff + h * half : ff + (h + 1) * half, :])
            g = gate_f[at, :]
            sigma = jax.nn.sigmoid(g)
            swish = g * sigma
            hidden = (swish * value).astype(bf16)
            hidden_ref[h, at, :] = hidden
            hidden_t[:, at] = hidden.T
            gate_side[h, at, :] = (value * sigma * (1.0 + g * (1.0 - sigma))).astype(bf16)
            up_side[h, at, :] = swish.astype(bf16)

        tiles(seq // PAIR, body)

    def sides(h):
        def body(t):
            at = span(t, PAIR)
            grad = dot_nt(cot_all[at, :], down_all[h * half : (h + 1) * half, :])
            gate_grad = (grad * gate_side[h, at, :].astype(f32)).astype(bf16)
            up_grad = (grad * up_side[h, at, :].astype(f32)).astype(bf16)
            gate_side[h, at, :] = gate_grad
            up_side[h, at, :] = up_grad
            gate_t[:, at] = gate_grad.T
            up_t[:, at] = up_grad.T

        tiles(seq // PAIR, body)

    def weights(target):
        def body(j):
            cols = span(j, 2 * PAIR)
            normed = rows_all[:, cols]
            target[:half, cols] = dot_nn(gate_t[...], normed).astype(bf16)
            target[half : 2 * half, cols] = dot_nn(up_t[...], normed).astype(bf16)
            target[2 * half : 3 * half, cols] = dot_nn(hidden_t[...], cot_all[:, cols]).astype(bf16)

        tiles(d // (2 * PAIR), body)

    gate[0].finish()
    gates(0)
    up[0].finish()
    ups(0)
    gate[1].forward_far()
    up[1].forward_next()
    down[1].start()
    down[0].finish()
    sides(0)
    weights(part)
    summed = DepthScatter(place, part, part, got, both, width, dsend, drecv)
    summed.start()
    up[1].forward_far()
    down[1].forward_next()
    down[1].forward_far()
    gate[1].finish()
    gates(1)
    summed.hand_on(0)
    up[1].finish()
    saves[3].start()
    ups(1)
    summed.hand_on(1)
    summed.hand_on(2)
    down[1].finish()
    saves[4].start()
    saves[3].wait()
    sides(1)
    weights(gateup_all)
    saves[5].start()
    summed.finish(first_sums)
    for i in (1, 2, 4, 5):
        saves[i].wait()


def forward(perm, x, cot, gain1, bias1, gain2, bias2, shift, qkv, out, gateup, down):
    ndp, nctx = lax.axis_size("dp"), lax.axis_size("ctx")
    rows, d = x.shape
    seq, width, ff = rows * nctx, qkv.shape[2], gateup.shape[1]
    heads = width // HEAD_DIM
    bf16, f32 = jnp.bfloat16, jnp.float32
    row = [gain1, bias1, gain2, bias2]

    def shaped(shape, dtype=bf16):
        return jax.ShapeDtypeStruct(shape, dtype)

    return pl.pallas_call(
        forward_kernel,
        out_shape=(
            shaped((rows, d), f32),
            shaped((width, seq)),
            shaped((width, seq)),
            shaped((width, seq)),
            shaped((width, seq)),
            shaped((8, seq), f32),
            shaped((2, seq, ff // 2)),
            shaped((2, seq, ff // 2)),
            shaped((2, seq, ff // 2)),
            shaped((3 * ff // 2, d // ndp), f32),
            shaped((8, seq), f32),
            shaped((8, seq), f32),
            shaped((seq, 1), f32),
            shaped((1, seq), f32),
            shaped((seq, d)),
            shaped((3, d, width)),
            shaped((width, d)),
            shaped((2 * ff, d)),
            shaped((ff, d)),
            shaped((3 * ff // 2, d)),
        ),
        in_specs=[pl.BlockSpec(memory_space=pltpu.SMEM)] + [VMEM] * 7 + [ANY] * 4,
        out_specs=(VMEM,) * 14 + (ANY,) * 6,
        scratch_shapes=[
            pltpu.VMEM((rows, d), bf16),
            pltpu.VMEM((rows, d), bf16),
            pltpu.VMEM((seq, d), bf16),
            pltpu.VMEM((seq, d), bf16),
            pltpu.VMEM((3, d, width), bf16),
            pltpu.VMEM((width, d), bf16),
            pltpu.VMEM((2 * ff, d), bf16),
            pltpu.VMEM((ff, d), bf16),
            pltpu.VMEM((heads, seq, HEAD_DIM), bf16),
            pltpu.VMEM((seq, PAIR), f32),
            pltpu.VMEM((seq, width), bf16),
            pltpu.VMEM((seq, ff // 2), f32),
            pltpu.VMEM((ff // 2, seq), bf16),
            pltpu.VMEM((ff // 2, seq), bf16),
            pltpu.VMEM((ff // 2, seq), bf16),
            pltpu.VMEM((3 * ff // 2, d), bf16),
            pltpu.VMEM((3, width), f32),
        ]
        + depth_sems(ndp) * 8
        + gather_sems(nctx) * 3
        + scatter_scratch(nctx, rows, d)
        + depth_scatter_scratch(ndp, 3 * ff // 2, d // ndp)
        + [DMA((6,))],
        compiler_params=pltpu.CompilerParams(
            collective_id=0, has_side_effects=True, vmem_limit_bytes=67_000_000
        ),
        cost_estimate=pl.CostEstimate(flops=0, bytes_accessed=700_000_000, transcendentals=0),
        name="forward",
    )(perm, x, cot, *row, shift, qkv, out, gateup, down)


def attend_back(
    grad_ref, w_ref, rows_ref, cos_ref, sin_ref, pos_col, pos_row, q_t, k_t, v_t, attn_t, lse,
    parts_ref, sums_ref, w_grads, g_t, delta, q_grad, kv_grad, bias, flat, rows_buf, rows_sem, between
):
    seq, d = grad_ref.shape
    width = w_ref.shape[0]
    heads = width // HEAD_DIM
    bf16, f32 = jnp.bfloat16, jnp.float32
    count = d // (2 * PAIR)

    def load(j):
        slot = lax.rem(j, 2)
        return pltpu.make_async_copy(rows_ref.at[:, span(j, 2 * PAIR)], rows_buf.at[slot], rows_sem.at[slot])

    def first(t):
        at = span(t, PAIR)
        grad = dot_nt(w_ref[...], grad_ref[at, :])
        both = grad * attn_t[:, at].astype(f32)
        for h in range(heads):
            delta[h : h + 1, at] = jnp.sum(both[h * HEAD_DIM : (h + 1) * HEAD_DIM], axis=0, keepdims=True)
        g_t[:, at] = grad.astype(bf16)

    tiles(seq // PAIR, first)
    between()
    q_grad[...] = jnp.zeros_like(q_grad)

    def keys(t):
        at = span(t, PAIR)
        bias[...] = jnp.where(pos_col[at, :] <= pos_row[...], 0.0, neg_big)
        for h in range(heads):
            feats = slice(h * HEAD_DIM, (h + 1) * HEAD_DIM)
            keys_t = k_t[feats, at]
            probs = jnp.exp(dot_nn(keys_t.T, q_t[feats, :]) + bias[...] - lse[h : h + 1, :])
            kv_grad[1, feats, at] = dot_nt(g_t[feats, :], probs.astype(bf16))
            back = dot_nn(v_t[feats, at].T, g_t[feats, :])
            scores = (probs * (back - delta[h : h + 1, :])).astype(bf16)
            kv_grad[0, feats, at] = dot_nt(q_t[feats, :], scores)
            q_grad[feats, :] += dot_nn(keys_t, scores)

    tiles(seq // PAIR, keys)
    load(0).start()
    sums_ref[...] = jnp.zeros_like(sums_ref)

    def part(t):
        at = span(t, PAIR)
        cosine, sine = cos_ref[:, at], sin_ref[:, at]
        for i in range(3):
            if i == 0:
                grad = turn(q_grad[:, at] * (1.0 / math.sqrt(HEAD_DIM)), cosine, -sine, heads)
            elif i == 1:
                grad = turn(kv_grad[0, :, at], cosine, -sine, heads)
            else:
                grad = kv_grad[1, :, at]
            natural = grad.T
            sums_ref[i : i + 1, :] += jnp.sum(natural, axis=0, keepdims=True)
            parts_ref[i, at, :] = natural.astype(bf16)
            flat[i, :, at] = grad.astype(bf16)

    tiles(seq // PAIR, part)

    def weights(j):
        pl.when(j + 1 < count)(lambda: load(j + 1).start())
        load(j).wait()
        cols = span(j, 2 * PAIR)
        rows = rows_buf[lax.rem(j, 2)]
        for i in range(3):
            w_grads[i * width : (i + 1) * width, cols] = dot_nn(flat[i], rows).astype(bf16)
        w_grads[3 * width : 4 * width, cols] = dot_nn(attn_t[...], grad_ref[:, cols]).astype(bf16)

    tiles(count, weights)


def middle_kernel(
    gate_ref, up_ref, w_hbm, part_ref, resid_ref, cot_ref, gain_ref, out_ref, rows_ref,
    cos_ref, sin_ref, pos_col, pos_row, q_t, k_t, v_t, attn_t, lse,
    grad_ref, vec_ref, parts_ref, sums_ref, second_sums, w_out,
    arena, part_all, block, grad_all, g_t, delta, q_grad, kv_grad, bias, flat, rows_buf, rows_sem, save_sem, *scratch
):
    place = Place()
    greet(place, along_dp=True)
    scratch = list(scratch)

    def take(n):
        head = scratch[:n]
        del scratch[:n]
        return head

    rows = resid_ref.shape[0]
    half, d = gate_ref.shape[2], part_ref.shape[1]
    ff = 2 * half
    piece = d // place.ndp
    refs = take(9)
    sum_refs = take(4)
    summed = DepthScatter(place, part_ref, part_all, *sum_refs[:2], piece, *sum_refs[2:])
    summed.start()
    load = pltpu.make_async_copy(w_hbm, arena, save_sem.at[0])
    fetch = pltpu.make_async_copy(part_ref, part_all, save_sem.at[1])
    load.start()
    fetch.start()
    load.wait()
    fetch.wait()

    def product(at, cols):
        total = dot_nn(gate_ref[0, at, :], arena[:half, cols])
        total = total + dot_nn(gate_ref[1, at, :], arena[half:ff, cols])
        total = total + dot_nn(up_ref[0, at, :], arena[ff : ff + half, cols])
        return total + dot_nn(up_ref[1, at, :], arena[ff + half :, cols])

    scatter = sum_scatter(place, rows, product, *refs[:5], refs[5:9])
    scatter.run()
    gain = gain_ref[...].astype(jnp.float32)[None, :]
    vec_ref[...] = jnp.zeros_like(vec_ref)

    def back(at):
        grad = scatter.total(at)
        normed, rscale = normal(resid_ref[at, :])
        vec_ref[0:1, :] += jnp.sum(grad * normed, axis=0, keepdims=True)
        vec_ref[1:2, :] += jnp.sum(grad, axis=0, keepdims=True)
        out = cot_ref[at, :] + normal_back(grad, normed, rscale, gain)
        grad_ref[at, :] = out
        block[at, :] = out.astype(jnp.bfloat16)

    row_loop(rows, back)
    gathered = row_gather(place, block, grad_all, *take(3))
    gathered.start()
    summed.hand_on(0)
    gathered.forward()
    gathered.finish()
    scatter.finish()

    def between():
        summed.hand_on(1)
        summed.hand_on(2)

    w_grads = arena.at[: w_out.shape[0]]
    attend_back(
        grad_all, out_ref, rows_ref, cos_ref, sin_ref, pos_col, pos_row, q_t, k_t, v_t, attn_t, lse,
        parts_ref, sums_ref, w_grads, g_t, delta, q_grad, kv_grad, bias, flat, rows_buf, rows_sem, between,
    )
    keep = pltpu.make_async_copy(w_grads, w_out, save_sem.at[2])
    keep.start()
    summed.finish(second_sums)
    keep.wait()


def middle(gate_grad, up_grad, w, part, resid, cot, gain, out, rows_all, cosine, sine, pos_col, pos_row, q_t, k_t, v_t, attn_t, lse):
    ndp, nctx = lax.axis_size("dp"), lax.axis_size("ctx")
    rows, d = resid.shape
    seq, width, ff = rows * nctx, out.shape[0], w.shape[0] // 2
    bf16, f32 = jnp.bfloat16, jnp.float32
    return pl.pallas_call(
        middle_kernel,
        out_shape=(
            jax.ShapeDtypeStruct((rows, d), f32),
            jax.ShapeDtypeStruct((2, d), f32),
            jax.ShapeDtypeStruct((3, seq, width), bf16),
            jax.ShapeDtypeStruct((3, width), f32),
            jax.ShapeDtypeStruct((3 * ff // 2, d // ndp), f32),
            jax.ShapeDtypeStruct((4 * width, d), bf16),
        ),
        in_specs=[VMEM] * 2 + [ANY] * 2 + [VMEM] * 4 + [ANY] + [VMEM] * 9,
        out_specs=(VMEM,) * 5 + (ANY,),
        scratch_shapes=[
            pltpu.VMEM((2 * ff, d), bf16),
            pltpu.VMEM((3 * ff // 2, d), bf16),
            pltpu.VMEM((rows, d), bf16),
            pltpu.VMEM((seq, d), bf16),
            pltpu.VMEM((width, seq), bf16),
            pltpu.VMEM((8, seq), f32),
            pltpu.VMEM((width, seq), f32),
            pltpu.VMEM((2, width, seq), f32),
            pltpu.VMEM((PAIR, seq), f32),
            pltpu.VMEM((3, width, seq), bf16),
            pltpu.VMEM((2, seq, 2 * PAIR), bf16),
            DMA((2,)),
            DMA((4,)),
        ]
        + scatter_scratch(nctx, rows, d)
        + depth_scatter_scratch(ndp, 3 * ff // 2, d // ndp)
        + gather_sems(nctx),
        compiler_params=pltpu.CompilerParams(
            collective_id=2, has_side_effects=True, vmem_limit_bytes=67_000_000
        ),
        cost_estimate=pl.CostEstimate(flops=0, bytes_accessed=300_000_000, transcendentals=0),
        name="middle",
    )(gate_grad, up_grad, w, part, resid, cot, gain, out, rows_all, cosine, sine, pos_col, pos_row, q_t, k_t, v_t, attn_t, lse)


class VectorSum:
    def __init__(self, place, value, from_ctx, from_dp, plane, ctx_send, ctx_recv, dp_send, dp_recv):
        self.place, self.value, self.from_ctx, self.from_dp, self.plane = place, value, from_ctx, from_dp, plane
        self.ctx_send, self.ctx_recv, self.dp_send, self.dp_recv = ctx_send, ctx_recv, dp_send, dp_recv

    def across(self, i):
        place = self.place
        return push(
            self.value, self.from_ctx.at[place.c], self.ctx_send.at[i - 1], self.ctx_recv.at[place.c],
            place.at(lax.rem(place.c + i, place.nctx)),
        )

    def along(self, i):
        place = self.place
        return push(
            self.plane, self.from_dp.at[place.z], self.dp_send.at[i - 1], self.dp_recv.at[place.z],
            {"dp": lax.rem(place.z + i, place.ndp), "ctx": place.c},
        )

    def start(self):
        for i in range(1, self.place.nctx):
            self.across(i).start()
        self.from_ctx[self.place.c] = self.value[...]

    def turn(self):
        place = self.place
        for i in range(1, place.nctx):
            c = lax.rem(place.c + i, place.nctx)
            push(self.value, self.from_ctx.at[c], self.ctx_send.at[0], self.ctx_recv.at[c], place.at(c)).wait_recv()
        total = self.from_ctx[0]
        for i in range(1, place.nctx):
            total = total + self.from_ctx[i]
        self.plane[...] = total
        self.from_dp[place.z] = total
        for i in range(1, place.ndp):
            self.along(i).start()

    def finish(self, out_ref):
        place = self.place
        for i in range(1, place.ndp):
            z = lax.rem(place.z + i, place.ndp)
            device = {"dp": z, "ctx": place.c}
            push(self.plane, self.from_dp.at[z], self.dp_send.at[0], self.dp_recv.at[z], device).wait_recv()
        total = self.from_dp[0]
        for i in range(1, place.ndp):
            total = total + self.from_dp[i]
        out_ref[...] = total
        for i in range(1, place.nctx):
            self.across(i).wait_send()
        for i in range(1, place.ndp):
            self.along(i).wait_send()


def vector_scratch(ndp, nctx, shape):
    f32 = jnp.float32
    return [
        pltpu.VMEM(shape, f32),
        pltpu.VMEM((nctx,) + shape, f32),
        pltpu.VMEM((ndp,) + shape, f32),
        pltpu.VMEM(shape, f32),
        DMA((nctx - 1,)),
        DMA((nctx,)),
        DMA((ndp - 1,)),
        DMA((ndp,)),
    ]


def tail_kernel(
    w_grads, parts_ref, qkv_ref, x_ref, grad_ref, gain_ref, hidden_ref, down_ref, resid_ref, vec_ref, sums_ref,
    block_out, input_grad, small, qkv_grads, out_grads,
    total, *scratch
):
    place = Place()
    greet(place, all_ctx=True, along_dp=True)
    scratch = list(scratch)

    def take(n):
        head = scratch[:n]
        del scratch[:n]
        return head

    rows, d = x_ref.shape
    width = qkv_ref.shape[2]
    first_refs, second_refs = take(9), take(9)
    long_refs, short_refs = take(4), take(4)
    vectors = VectorSum(place, *take(8))
    w_all, down_all, load_sem = take(3)
    piece, cut = d // place.ndp, 3 * width
    upper, lower = pl.ds(0, cut), pl.ds(cut, width)
    long_sum = DepthScatter(place, w_grads.at[upper], w_all.at[upper], *long_refs[:2], piece, *long_refs[2:])
    short_sum = DepthScatter(place, w_grads.at[lower], w_all.at[lower], *short_refs[:2], piece, *short_refs[2:])
    long_sum.start()
    short_sum.start()
    loads = [
        pltpu.make_async_copy(w_grads, w_all, load_sem.at[0]),
        pltpu.make_async_copy(down_ref, down_all, load_sem.at[1]),
    ]
    for copy in loads:
        copy.start()

    def product(at, cols):
        part = dot_nt(parts_ref[0, at, :], qkv_ref[0, cols, :])
        part = part + dot_nt(parts_ref[1, at, :], qkv_ref[1, cols, :])
        return part + dot_nt(parts_ref[2, at, :], qkv_ref[2, cols, :])

    first = sum_scatter(place, rows, product, *first_refs[:5], first_refs[5:9])
    half = hidden_ref.shape[2]

    def down_product(at, cols):
        return dot_nn(hidden_ref[0, at, :], down_all[:half, cols]) + dot_nn(hidden_ref[1, at, :], down_all[half:, cols])

    second = sum_scatter(place, rows, down_product, *second_refs[:5], second_refs[5:9])
    first.run()
    gain = gain_ref[...].astype(jnp.float32)[None, :]
    value = vectors.value
    value[...] = jnp.zeros_like(value)
    value[2:4, :] = vec_ref[...]
    value[4:7, pl.ds(pl.multiple_of(place.c * width, width), width)] = sums_ref[...]

    def back(at):
        grad = first.total(at)
        normed, rscale = normal(x_ref[at, :].astype(jnp.float32))
        value[0:1, :] += jnp.sum(grad * normed, axis=0, keepdims=True)
        value[1:2, :] += jnp.sum(grad, axis=0, keepdims=True)
        input_grad[at, :] = grad_ref[at, :] + normal_back(grad, normed, rscale, gain)

    row_loop(rows, back)
    vectors.start()
    for copy in loads:
        copy.wait()
    long_sum.hand_on(0)
    second.run((lambda: long_sum.hand_on(1), lambda: long_sum.hand_on(2)))

    def add(at):
        block_out[at, :] = (resid_ref[at, :] + second.total(at)).astype(jnp.bfloat16)

    row_loop(rows, add)
    vectors.turn()
    short_sum.hand_on(0)
    short_sum.hand_on(1)
    short_sum.hand_on(2)
    first.finish()
    second.finish()
    vectors.finish(small)
    long_sum.finish(total.at[upper])
    short_sum.finish(out_grads)
    for i in range(3):
        qkv_grads[i] = total[i * width : (i + 1) * width, :].T


def tail(w_grads, parts, qkv, x, grad, gain, hidden, down, resid, vec, sums):
    ndp, nctx = lax.axis_size("dp"), lax.axis_size("ctx")
    rows, d = x.shape
    width = qkv.shape[2]
    bf16, f32 = jnp.bfloat16, jnp.float32
    return pl.pallas_call(
        tail_kernel,
        out_shape=(
            jax.ShapeDtypeStruct((rows, d), bf16),
            jax.ShapeDtypeStruct((rows, d), f32),
            jax.ShapeDtypeStruct((8, d), f32),
            jax.ShapeDtypeStruct((3, d // ndp, width), f32),
            jax.ShapeDtypeStruct((width, d // ndp), f32),
        ),
        in_specs=[ANY] + [VMEM] * 6 + [ANY] + [VMEM] * 3,
        out_specs=(VMEM,) * 5,
        scratch_shapes=[pltpu.VMEM((3 * width, d // ndp), f32)]
        + scatter_scratch(nctx, rows, d) * 2
        + depth_scatter_scratch(ndp, 3 * width, d // ndp)
        + depth_scatter_scratch(ndp, width, d // ndp)
        + vector_scratch(ndp, nctx, (8, d))
        + [pltpu.VMEM((4 * width, d), bf16), pltpu.VMEM(down.shape, bf16), DMA((2,))],
        compiler_params=pltpu.CompilerParams(
            collective_id=3, has_side_effects=True, vmem_limit_bytes=67_000_000
        ),
        cost_estimate=pl.CostEstimate(flops=0, bytes_accessed=300_000_000, transcendentals=0),
        name="tail",
    )(w_grads, parts, qkv, x, grad, gain, hidden, down, resid, vec, sums)


def per_device(
    block_input,
    out_cotangent,
    group_perm,
    attn_norm_gain,
    attn_norm_bias,
    qkv_weight,
    qkv_bias,
    out_weight,
    mlp_norm_gain,
    mlp_norm_bias,
    gateup_weight,
    down_weight,
):
    width_local = qkv_weight.shape[2]
    (
        residual_stream, q_t, k_t, v_t, attn_t, lse, hidden_b, gate_grad, up_grad, first_sums, cos_all, sin_all, pos_col, pos_row,
        rows_all, qkv_local, out_local, gateup_local, down_local, mlp_grads,
    ) = forward(
        group_perm, block_input, out_cotangent, attn_norm_gain, attn_norm_bias, mlp_norm_gain, mlp_norm_bias, qkv_bias,
        qkv_weight, out_weight, gateup_weight.transpose(0, 2, 1), down_weight,
    )
    resid_grad, second_vectors, grad_parts_b, shift_part, second_sums, attn_grads = middle(
        gate_grad, up_grad, gateup_local, mlp_grads, residual_stream, out_cotangent, mlp_norm_gain, out_local,
        rows_all, cos_all, sin_all, pos_col, pos_row, q_t, k_t, v_t, attn_t, lse,
    )
    block_output, input_grad, small, qkv_grads, out_grads = tail(
        attn_grads, grad_parts_b, qkv_local, block_input, resid_grad, attn_norm_gain,
        hidden_b, down_local, residual_stream, second_vectors, shift_part,
    )
    half = first_sums.shape[0] // 3
    both = [
        jnp.concatenate([first_sums[i * half : (i + 1) * half], second_sums[i * half : (i + 1) * half]])
        for i in range(3)
    ]
    gateup_grads, down_grads = jnp.stack(both[:2]), both[2]
    return (
        block_output,
        input_grad,
        small[0],
        small[1],
        qkv_grads,
        small[4:7],
        out_grads,
        small[2],
        small[3],
        gateup_grads.transpose(0, 2, 1),
        down_grads,
    )


def solution(mesh):
    return jax.shard_map(
        per_device,
        mesh=mesh,
        in_specs=(
            P(("dp", "ctx"), None),
            P(("dp", "ctx"), None),
            P("dp", None),
            P(),
            P(),
            P(None, "dp", "ctx"),
            P(),
            P("ctx", "dp"),
            P(),
            P(),
            P(None, "dp", "ctx"),
            P("ctx", "dp"),
        ),
        out_specs=(
            P(("dp", "ctx"), None),
            P(("dp", "ctx"), None),
            P(),
            P(),
            P(None, "dp", "ctx"),
            P(),
            P("ctx", "dp"),
            P(),
            P(),
            P(None, "dp", "ctx"),
            P("ctx", "dp"),
        ),
        check_vma=False,
    )
```

```python
import functools
import math

import jax
import jax.numpy as jnp
from jax import lax
from jax.experimental import pallas as pl
from jax.experimental.pallas import tpu as pltpu
from jax.sharding import PartitionSpec as P

MESH = pl.DeviceIdType.MESH
VMEM = pl.BlockSpec(memory_space=pltpu.VMEM)
ANY = pl.BlockSpec(memory_space=pl.ANY)
DMA = pltpu.SemaphoreType.DMA

D = 2048
HEADS = 32
HEAD_DIM = 64
ROT = 16


eps_norm = 1e-05
rope_base = 10000.0
neg_big = -1e30


class Place:
    def __init__(self):
        self.ndp = lax.axis_size("dp")
        self.nctx = lax.axis_size("ctx")
        self.nchip = self.nctx // 2
        self.z = lax.axis_index("dp")
        self.c = lax.axis_index("ctx")
        self.p = lax.div(self.c, 2)
        self.k = lax.rem(self.c, 2)

    def chip(self, offset):
        return lax.rem(self.p + offset, self.nchip)

    def at(self, c):
        return {"dp": self.z, "ctx": c}

    def partner(self):
        return self.at(2 * self.p + 1 - self.k)

    def same_core(self, q):
        return self.at(2 * q + self.k)


def greet(place, along_ctx=True, along_dp=False, all_ctx=False):
    barrier = pltpu.get_barrier_semaphore()
    peers = []
    if all_ctx:
        peers += [place.at(lax.rem(place.c + i, place.nctx)) for i in range(1, place.nctx)]
    elif along_ctx:
        peers += [place.partner()] + [place.same_core(place.chip(i)) for i in range(1, place.nchip)]
    if along_dp:
        peers += [{"dp": lax.rem(place.z + i, place.ndp), "ctx": place.c} for i in range(1, place.ndp)]
    for peer in peers:
        pl.semaphore_signal(barrier, inc=1, device_id=peer, device_id_type=MESH)
    pl.semaphore_wait(barrier, len(peers))


def push(src, dst, send, recv, device):
    return pltpu.make_async_remote_copy(
        src_ref=src, dst_ref=dst, send_sem=send, recv_sem=recv, device_id=device, device_id_type=MESH
    )


class RowGather:
    def __init__(self, place, block, whole, send, recv, local):
        self.place, self.block, self.whole = place, block, whole
        self.send, self.recv, self.local = send, recv, local
        self.rows = block.shape[0]

    def slot(self, c):
        return self.whole.at[pl.ds(pl.multiple_of(c * self.rows, self.rows), self.rows)]

    def direct(self, i):
        place = self.place
        q = place.chip(i)
        return push(self.block, self.slot(place.c), self.send.at[i], self.recv.at[place.c], place.same_core(q))

    def own(self):
        place = self.place
        return push(self.block, self.slot(place.c), self.send.at[0], self.recv.at[place.c], place.partner())

    def passed(self, i):
        place = self.place
        c = 2 * place.chip(i) + place.k
        return push(
            self.slot(c), self.slot(c), self.send.at[place.nchip + i - 1], self.recv.at[c], place.partner()
        )

    def arrival(self, c):
        return push(self.block, self.slot(c), self.send.at[0], self.recv.at[c], self.place.partner())

    def keep(self):
        return pltpu.make_async_copy(self.block, self.slot(self.place.c), self.local)

    def start(self):
        for i in range(1, self.place.nchip):
            self.direct(i).start()
        self.own().start()
        self.keep().start()

    def forward(self):
        place = self.place
        for i in range(1, place.nchip):
            self.arrival(2 * place.chip(i) + place.k).wait_recv()
            self.passed(i).start()

    def finish(self):
        place = self.place
        for i in range(place.nchip):
            self.arrival(2 * place.chip(i) + 1 - place.k).wait_recv()
        self.own().wait_send()
        for i in range(1, place.nchip):
            self.direct(i).wait_send()
            self.passed(i).wait_send()
        self.keep().wait()


class BoxGather(RowGather):
    def part(self, c, half):
        size = self.rows // 2
        return self.whole.at[pl.ds(pl.multiple_of(c * self.rows + half * size, size), size)]

    def near(self, axis):
        place = self.place
        other = 1 - lax.rem(place.p, 2) if axis == 0 else 1 - lax.div(place.p, 2)
        q = 2 * lax.div(place.p, 2) + other if axis == 0 else 2 * other + lax.rem(place.p, 2)
        return 2 * q + place.k

    def across(self):
        return 2 * (3 - self.place.p) + self.place.k

    def piece(self, c, half, sem, to, own=False):
        size = self.rows // 2
        src = self.block.at[pl.ds(half * size, size)] if own else self.part(c, half)
        return push(src, self.part(c, half), self.send.at[sem], self.recv.at[2 * c + half], self.place.at(to))

    def own(self):
        place = self.place
        return push(self.block, self.slot(place.c), self.send.at[0], self.recv.at[2 * place.c], place.partner())

    def first(self):
        c = self.place.c
        return [self.piece(c, h, 1 + n, self.near(a), True) for n, (a, h) in enumerate(((0, 0), (1, 1), (0, 1), (1, 0)))]

    def second(self):
        return [self.piece(self.near(a), a, 5 + a, self.near(1 - a)) for a in (0, 1)]

    def to_partner(self):
        place = self.place
        pair = 2 * place.p + 1 - place.k
        return [
            self.piece(c, h, 7 + n, pair)
            for n, (c, h) in enumerate(
                ((self.near(0), 0), (self.near(1), 1), (self.near(0), 1), (self.near(1), 0), (self.across(), 0), (self.across(), 1))
            )
        ]

    def start(self):
        for copy in self.first():
            copy.start()
        self.own().start()
        self.keep().start()

    def forward(self):
        second, pair = self.second(), self.to_partner()
        for n, copy in enumerate(pair):
            copy.wait_recv()
            if n < 2:
                second[n].start()
            copy.start()

    def finish(self):
        place = self.place
        pair = 2 * place.p + 1 - place.k
        self.arrival_pair().wait_recv()
        for n in range(6):
            c = (self.near(0), self.near(1), self.near(0), self.near(1), self.across(), self.across())[n]
            half = (0, 1, 1, 0, 0, 1)[n]
            twin = c + 1 - 2 * place.k
            self.piece(twin, half, 7 + n, pair).wait_recv()
        self.own().wait_send()
        for copy in self.first() + self.second() + self.to_partner():
            copy.wait_send()
        self.keep().wait()

    def arrival_pair(self):
        c = self.place.c + 1 - 2 * self.place.k
        return push(self.block, self.slot(c), self.send.at[0], self.recv.at[2 * c], self.place.partner())


def row_gather(place, *args):
    return (BoxGather if place.nchip == 4 else RowGather)(place, *args)


def gather_sems(nctx):
    return [DMA((13,)), DMA((2 * nctx,)), DMA] if nctx == 8 else [DMA((nctx,)), DMA((nctx,)), DMA]


class DepthGather:
    def __init__(self, place, piece, whole, where, send, recv, local, passing=True):
        self.place, self.piece, self.whole, self.where = place, piece, whole, where
        self.send, self.recv, self.local = send, recv, local
        self.line = place.ndp == 4 and passing
        z = place.z
        self.end = jnp.logical_or(z == 0, z == 3)
        self.middle = jnp.logical_not(self.end)
        self.near = jnp.clip(3 * (z - 1), 0, 3)
        self.far = 3 - self.near
        self.other = jnp.clip(3 - z, 1, 2)

    def copy(self, src, z_src, z_dst, sem):
        return push(
            src, self.where(self.whole, z_src), self.send.at[sem], self.recv.at[z_src], {"dp": z_dst, "ctx": self.place.c}
        )

    def directs(self):
        z, n = self.place.z, self.place.ndp
        if not self.line:
            return [(None, self.copy(self.piece, z, lax.rem(z + i, n), i - 1)) for i in range(1, n)]
        out = []
        for sem, step in enumerate((1, -1, 2, -2)):
            d = z + step
            ok = jnp.logical_and(d >= 0, d < 4)
            if abs(step) == 2:
                ok = jnp.logical_and(ok, self.end)
            out.append((ok, self.copy(self.piece, z, jnp.clip(d, 0, 3), sem)))
        return out

    def keep(self):
        return pltpu.make_async_copy(self.piece, self.where(self.whole, self.place.z), self.local)

    def start(self):
        for ok, copy in self.directs():
            if ok is None:
                copy.start()
            else:
                pl.when(ok)(copy.start)
        self.keep().start()

    def passed(self, src, sem):
        return self.copy(self.where(self.whole, src), src, self.near, sem)

    def forward_next(self):
        self.forward(self.other, 4)

    def forward_far(self):
        self.forward(self.far, 5)

    def forward(self, src, sem):
        if self.line:

            @pl.when(self.middle)
            def _():
                self.copy(self.piece, src, src, sem).wait_recv()
                self.passed(src, sem).start()

    def finish(self):
        z, n = self.place.z, self.place.ndp
        for i in range(1, n):
            src = lax.rem(z + i, n)
            wait = self.copy(self.piece, src, src, 0).wait_recv
            if self.line:
                pl.when(jnp.logical_or(self.end, src == self.near))(wait)
            else:
                wait()
        for ok, copy in self.directs():
            if ok is None:
                copy.wait_send()
            else:
                pl.when(ok)(copy.wait_send)
        if self.line:

            @pl.when(self.middle)
            def _():
                self.passed(self.other, 4).wait_send()
                self.passed(self.far, 5).wait_send()

        self.keep().wait()


def depth_sems(ndp):
    return [DMA((max(ndp, 6),)), DMA((ndp,)), DMA]


STEP = 16


def row_loop(rows, body):
    def step(i, carry):
        body(pl.ds(pl.multiple_of(i * STEP, STEP), STEP))
        return carry

    lax.fori_loop(0, rows // STEP, step, 0)


def normal(values):
    centred = values - jnp.mean(values, axis=-1, keepdims=True)
    rscale = lax.rsqrt(jnp.mean(centred * centred, axis=-1, keepdims=True) + eps_norm)
    return centred * rscale, rscale


def normal_back(grad_out, normed, rscale, gain):
    scaled = grad_out * gain
    return rscale * (
        scaled
        - jnp.mean(scaled, axis=-1, keepdims=True)
        - normed * jnp.mean(scaled * normed, axis=-1, keepdims=True)
    )


class SumScatter:
    TILE = 512

    def __init__(self, place, rows, product, mine, to_pair, from_pair, to_chip, from_chip, sems):
        self.place, self.rows, self.product = place, rows, product
        self.mine, self.to_pair, self.from_pair = mine, to_pair, from_pair
        self.to_chip, self.from_chip = to_chip, from_chip
        self.pair_send, self.pair_recv, self.chip_send, self.chip_recv = sems

    def pair(self, i):
        return push(
            self.to_pair.at[lax.rem(i, 2)], self.from_pair.at[i], self.pair_send.at[i], self.pair_recv.at[i], self.place.partner()
        )

    def chips(self, i):
        return push(
            self.to_chip.at[i],
            self.from_chip.at[i],
            self.chip_send.at[i],
            self.chip_recv.at[i],
            self.place.same_core(self.place.chip(i + 1)),
        )

    def chip_of(self, i):
        return lax.rem(self.place.p + 1 + i, self.place.nchip)

    def hand_on(self, i):
        self.pair(i).wait_recv()

        def add(at):
            both = self.mine[lax.rem(i, 2), at, :] + self.from_pair[i, at, :].astype(jnp.float32)
            self.to_chip[i, at, :] = both.astype(jnp.bfloat16)

        row_loop(self.rows, add)
        self.chips(i).start()

    def last(self, hooks):
        for hook in hooks:
            hook()
        nchip = self.place.nchip
        self.pair(nchip - 1).wait_recv()
        for i in range(nchip - 1):
            self.chips(i).wait_recv()

    def run(self, hooks=()):
        place, rows, tile = self.place, self.rows, self.TILE
        nchip = place.nchip
        width = self.mine.shape[-1]

        def step(i, carry):
            first = pl.multiple_of(self.chip_of(i) * 2 * rows, 2 * rows)
            slot = lax.rem(i, 2)
            pl.when(i >= 2)(lambda: self.pair(i - 2).wait_send())

            def columns(j, inner):
                cols = pl.ds(pl.multiple_of(j * tile, tile), tile)
                part = self.product(pl.ds(first, 2 * rows), cols)

                @pl.when(place.k == 0)
                def _():
                    self.mine[slot, :, cols] = part[:rows]
                    self.to_pair[slot, :, cols] = part[rows:].astype(jnp.bfloat16)

                @pl.when(place.k == 1)
                def _():
                    self.mine[slot, :, cols] = part[rows:]
                    self.to_pair[slot, :, cols] = part[:rows].astype(jnp.bfloat16)

                return inner

            lax.fori_loop(0, width // tile, columns, 0)
            self.pair(i).start()
            pl.when(i > 0)(lambda: self.hand_on(i - 1))
            return carry

        lax.fori_loop(0, nchip, step, 0)
        self.last(list(hooks))

    def total(self, at):
        last = self.place.nchip - 1
        value = self.mine[last % 2, at, :] + self.from_pair[last, at, :].astype(jnp.float32)
        for i in range(last):
            value = value + self.from_chip[i, at, :].astype(jnp.float32)
        return value

    def finish(self):
        for i in range(max(self.place.nchip - 2, 0), self.place.nchip):
            self.pair(i).wait_send()
        for i in range(self.place.nchip - 1):
            self.chips(i).wait_send()


class BoxScatter(SumScatter):
    def near(self, axis):
        p = self.place.p
        x, y = lax.rem(p, 2), lax.div(p, 2)
        return self.place.same_core(2 * y + 1 - x if axis == 0 else 2 * (1 - y) + x)

    def half(self, src, dst, rows, sem, axis):
        size = self.rows // 2
        at = pl.ds(rows * size, size)
        return push(
            self.to_chip.at[src, at], self.from_chip.at[dst, at], self.chip_send.at[sem], self.chip_recv.at[sem], self.near(axis)
        )

    def moves(self):
        return [
            self.half(0, 2, 0, 0, 0),
            self.half(0, 2, 1, 1, 1),
            self.half(1, 0, 0, 2, 0),
            self.half(2, 1, 1, 3, 1),
            self.half(1, 0, 1, 4, 0),
            self.half(2, 1, 0, 5, 1),
        ]

    def chip_of(self, i):
        p = self.place.p
        x, y = lax.rem(p, 2), lax.div(p, 2)
        other_x = jnp.logical_or(i == 0, i == 1)
        other_y = jnp.logical_or(i == 0, i == 2)
        return 2 * jnp.where(other_y, 1 - y, y) + jnp.where(other_x, 1 - x, x)

    def hand_on(self, i):
        self.pair(i).wait_recv()
        slot = lax.rem(i, 2)

        def add(at):
            both = self.mine[slot, at, :] + self.from_pair[i, at, :].astype(jnp.float32)
            self.to_chip[i, at, :] = both.astype(jnp.bfloat16)

        row_loop(self.rows, add)
        moves = self.moves()

        @pl.when(i == 0)
        def _():
            moves[0].start()
            moves[1].start()

        pl.when(i == 1)(moves[2].start)
        pl.when(i == 2)(moves[3].start)

    def last(self, hooks):
        moves = self.moves()
        size = self.rows // 2
        for arrived, src, first, onward in ((1, 1, size, 4), (0, 2, 0, 5)):
            if hooks:
                hooks.pop(0)()
            moves[arrived].wait_recv()

            def add(at, src=src, first=first):
                at = pl.ds(pl.multiple_of(first + at.start, STEP), STEP)
                both = self.to_chip[src, at, :].astype(jnp.float32) + self.from_chip[2, at, :].astype(jnp.float32)
                self.to_chip[src, at, :] = both.astype(jnp.bfloat16)

            row_loop(size, add)
            moves[onward].start()
        self.pair(3).wait_recv()
        for n in (2, 3, 4, 5):
            moves[n].wait_recv()

    def total(self, at):
        value = self.mine[1, at, :] + self.from_pair[3, at, :].astype(jnp.float32)
        return value + self.from_chip[0, at, :].astype(jnp.float32) + self.from_chip[1, at, :].astype(jnp.float32)

    def finish(self):
        for i in (2, 3):
            self.pair(i).wait_send()
        for copy in self.moves():
            copy.wait_send()


def sum_scatter(place, *args):
    return (BoxScatter if place.nchip == 4 else SumScatter)(place, *args)


def scatter_scratch(nctx, rows, d):
    n = nctx // 2
    bf16 = jnp.bfloat16
    return [
        pltpu.VMEM((2, rows, d), jnp.float32),
        pltpu.VMEM((2, rows, d), bf16),
        pltpu.VMEM((n, rows, d), bf16),
        pltpu.VMEM((n - 1, rows, d), bf16),
        pltpu.VMEM((n - 1, rows, d), bf16),
        DMA((n,)),
        DMA((n,)),
        DMA((6 if n == 4 else n - 1,)),
        DMA((6 if n == 4 else n - 1,)),
    ]


def dot_nn(a, b):
    return jnp.dot(a, b, preferred_element_type=jnp.float32)


def dot_nt(a, b):
    return lax.dot_general(a, b, (((1,), (1,)), ((), ())), preferred_element_type=jnp.float32)


HALF = ROT // 2
PAIR = 256


def tiles(count, body):
    def step(i, carry):
        body(i)
        return carry

    lax.fori_loop(0, count, step, 0)


def span(i, size):
    return pl.ds(pl.multiple_of(i * size, size), size)


def turn(columns, cosine, sine, heads):
    out = []
    for h in range(heads):
        at = h * HEAD_DIM
        a, b = columns[at : at + HALF], columns[at + HALF : at + ROT]
        out += [a * cosine - b * sine, b * cosine + a * sine, columns[at + ROT : at + HEAD_DIM]]
    return jnp.concatenate(out, axis=0)


def attend(rows_ref, w_ref, shift_ref, cos_ref, sin_ref, pos_col, pos_row, q_t, k_t, v_t, attn_t, lse, k_n, bias, attn):
    seq = rows_ref.shape[0]
    width = w_ref.shape[2]
    heads = width // HEAD_DIM
    bf16 = jnp.bfloat16

    def project(t):
        at = span(t, PAIR)
        cosine, sine = cos_ref[:, at], sin_ref[:, at]
        for i, ref in enumerate((q_t, k_t, v_t)):
            raw = (dot_nn(rows_ref[at, :], w_ref[i]) + shift_ref[i : i + 1, :]).T
            if i < 2:
                raw = turn(raw, cosine, sine, heads)
            raw = raw.astype(bf16)
            if i == 0:
                raw = raw * jnp.asarray(1.0 / math.sqrt(HEAD_DIM), bf16)
            ref[:, at] = raw

    tiles(seq // PAIR, project)
    for h in range(heads):
        k_n[h] = k_t[h * HEAD_DIM : (h + 1) * HEAD_DIM, :].T

    def queries(t):
        at = span(t, PAIR)
        bias[...] = jnp.where(pos_col[...] <= pos_row[:, at], 0.0, neg_big)

        for h in range(heads):
            feats = slice(h * HEAD_DIM, (h + 1) * HEAD_DIM)
            scores = dot_nn(k_n[h], q_t[feats, at]) + bias[...]
            peak = jnp.max(scores, axis=0, keepdims=True)
            probs = jnp.exp(scores - peak)
            total = jnp.sum(probs, axis=0, keepdims=True)
            out = dot_nn(v_t[feats, :], probs.astype(bf16)) / total
            attn_t[feats, at] = out.astype(bf16)
            lse[h : h + 1, at] = peak + jnp.log(total)
        attn[at, :] = attn_t[:, at].T

    tiles(seq // PAIR, queries)


class DepthScatter:
    def __init__(self, place, source, part, got, both, width, send, recv):
        self.place, self.source, self.part = place, source, part
        self.got, self.both, self.width = got, both, width
        self.send, self.recv = send, recv
        self.line = place.ndp == 4
        z = place.z
        self.end = jnp.logical_or(z == 0, z == 3)
        self.middle = jnp.logical_not(self.end)
        self.next = jnp.where(z == 3, 2, 1)
        self.other = jnp.clip(3 - z, 1, 2)
        self.near = jnp.clip(3 * (z - 1), 0, 3)

    def block(self, z):
        return self.source.at[:, pl.ds(pl.multiple_of(z * self.width, self.width), self.width)]

    def copy(self, src, slot, sem, z):
        return push(src, self.got.at[slot], self.send.at[sem], self.recv.at[slot], {"dp": z, "ctx": self.place.c})

    def from_end(self):
        far = 3 - self.place.z
        return [
            self.copy(self.block(far), 2, 0, self.next),
            self.copy(self.block(3 - self.next), 3, 1, self.next),
            self.copy(self.block(self.next), 0, 2, self.next),
        ]

    def from_middle(self):
        return [
            self.copy(self.both.at[0], 4, 0, self.other),
            self.copy(self.both.at[1], 1, 1, self.other),
            self.copy(self.both.at[2], 0, 2, self.near),
        ]

    def across(self):
        z, n = self.place.z, self.place.ndp
        return [self.copy(self.block(lax.rem(z + i, n)), i - 1, i - 1, lax.rem(z + i, n)) for i in range(1, n)]

    def start(self):
        self.start_first()
        self.start_last()

    def start_first(self):
        if not self.line:
            for copy in self.across():
                copy.start()
            return

        @pl.when(self.end)
        def _():
            for copy in self.from_end()[:2]:
                copy.start()

    def start_last(self):
        if self.line:
            pl.when(self.end)(self.from_end()[2].start)

    def hand_on(self, n):
        if not self.line:
            return

        @pl.when(self.middle)
        def _():
            owner, slot = ((3 - self.near, 2), (self.other, 3), (self.near, 4))[n]
            self.copy(self.both.at[0], slot, 0, self.near).wait_recv()
            cols = pl.ds(pl.multiple_of(owner * self.width, self.width), self.width)

            def add(at):
                total = self.part[at, cols].astype(jnp.float32) + self.got[slot, at, :].astype(jnp.float32)
                self.both[n, at, :] = total.astype(jnp.bfloat16)

            row_loop(self.part.shape[0], add)
            self.from_middle()[n].start()

    def collect(self, count, out_ref):
        for slot in range(count):
            self.copy(self.got.at[slot], slot, 0, self.next).wait_recv()
        cols = pl.ds(pl.multiple_of(self.place.z * self.width, self.width), self.width)

        def add(at):
            value = self.part[at, cols].astype(jnp.float32)
            for slot in range(count):
                value = value + self.got[slot, at, :].astype(jnp.float32)
            out_ref[at, :] = value

        row_loop(self.part.shape[0], add)

    def finish(self, out_ref):
        if not self.line:
            self.collect(self.place.ndp - 1, out_ref)
            for copy in self.across():
                copy.wait_send()
            return

        @pl.when(self.end)
        def _():
            self.collect(1, out_ref)
            for copy in self.from_end():
                copy.wait_send()

        @pl.when(self.middle)
        def _():
            self.collect(2, out_ref)
            for copy in self.from_middle():
                copy.wait_send()


def depth_scatter_scratch(ndp, rows, width):
    slots = 5 if ndp == 4 else ndp - 1
    return [
        pltpu.VMEM((slots, rows, width), jnp.bfloat16),
        pltpu.VMEM((3, rows, width), jnp.bfloat16),
        DMA((max(slots, 3),)),
        DMA((slots,)),
    ]


def tables(perm_ref, cos_ref, sin_ref, pos_col, pos_row, size):
    seq = pos_row.shape[1]
    lane = lax.broadcasted_iota(jnp.int32, (8, seq), 1)
    group = lane // size
    start = jnp.zeros((8, seq), jnp.int32)
    for g in range(seq // size):
        start = jnp.where(group == g, perm_ref[0, g], start)
    pos = (start * size + lane - group * size).astype(jnp.float32)
    pos_row[...] = pos[0:1]
    pos_col[...] = pos.T[:, 0:1]
    step = lax.broadcasted_iota(jnp.int32, (8, seq), 0).astype(jnp.float32)
    angle = pos * jnp.exp(step * (-2.0 / ROT * math.log(rope_base)))
    cos_ref[...] = jnp.cos(angle)
    sin_ref[...] = jnp.sin(angle)


def forward_kernel(
    perm_ref, x_ref, cot_ref, gain1_ref, bias1_ref, gain2_ref, bias2_ref, shift_ref,
    qkv_ref, out_ref, gateup_ref, down_ref,
    lse, first_sums, cos_ref, sin_ref, pos_col, pos_row,
    resid_out, q_out, k_out, v_out, attn_out, hidden_out, gate_side_out, up_side_out,
    rows_out, qkv_out, out_out, gateup_out, down_out, grads_out,
    row_block, cot_block, rows_all, cot_all, qkv_all, out_all, gateup_all, down_all,
    k_n, bias, attn, gate_f, hidden_t, gate_t, up_t, part, shifts,
    resid_ref, q_t, k_t, v_t, attn_t, hidden_ref, gate_side, up_side, *sems
):
    f32, bf16 = jnp.float32, jnp.bfloat16
    place = Place()
    greet(place, along_dp=True)
    sems = list(sems)

    def take(n):
        head = sems[:n]
        del sems[:n]
        return head

    def along_rows(size):
        return lambda ref, z: ref.at[:, pl.ds(pl.multiple_of(z * size, size), size), :]

    def along_lanes(size):
        return lambda ref, z: ref.at[:, pl.ds(pl.multiple_of(z * size, size), size)]

    depth, width = qkv_ref.shape[1], out_ref.shape[1]

    ff = gateup_ref.shape[1]
    half = ff // 2

    def slab(first):
        return lambda ref, z: ref.at[pl.ds(first, half), pl.ds(pl.multiple_of(z * depth, depth), depth)]

    qkv = DepthGather(place, qkv_ref, qkv_all, along_rows(depth), *take(3))
    out = DepthGather(place, out_ref, out_all, along_lanes(width), *take(3), passing=False)
    gate, up, down = [], [], []
    for h in range(2):
        at = pl.ds(h * half, half)
        gate.append(DepthGather(place, gateup_ref.at[0, at], gateup_all, slab(h * half), *take(3)))
        up.append(DepthGather(place, gateup_ref.at[1, at], gateup_all, slab(ff + h * half), *take(3)))
        down.append(DepthGather(place, down_ref.at[at], down_all, slab(h * half), *take(3)))
    rows = row_gather(place, row_block, rows_all, *take(3))
    cots = row_gather(place, cot_block, cot_all, *take(3))
    normeds = row_gather(place, row_block, rows_all, *take(3))
    scatter_refs = take(9)
    got, both, dsend, drecv = take(4)
    (save_sem,) = take(1)
    seq, d = rows_all.shape

    def save(i, src, dst):
        return pltpu.make_async_copy(src, dst, save_sem.at[i])

    saves = [
        save(0, rows_all, rows_out),
        save(1, qkv_all, qkv_out),
        save(2, out_all, out_out),
        save(3, gateup_all, gateup_out),
        save(4, down_all, down_out),
        save(5, gateup_all.at[pl.ds(0, 3 * half)], grads_out),
        save(6, q_t, q_out),
        save(7, k_t, k_out),
        save(8, v_t, v_out),
        save(9, attn_t, attn_out),
        save(10, resid_ref, resid_out),
    ]
    for h in range(2):
        saves.append(save(11 + 3 * h, hidden_ref.at[h], hidden_out.at[h]))
        saves.append(save(12 + 3 * h, gate_side.at[h], gate_side_out.at[h]))
        saves.append(save(13 + 3 * h, up_side.at[h], up_side_out.at[h]))

    qkv.start()
    gain, shift = gain1_ref[...].astype(f32)[None, :], bias1_ref[...].astype(f32)[None, :]

    def norm1(at):
        normed, _ = normal(x_ref[at, :].astype(f32))
        row_block[at, :] = (normed * gain + shift).astype(bf16)
        cot_block[at, :] = cot_ref[at, :].astype(bf16)

    row_loop(x_ref.shape[0], norm1)
    rows.start()
    cots.start()
    head = qkv_ref.shape[2]
    shifts[...] = shift_ref[:, pl.ds(pl.multiple_of(place.c * head, head), head)].astype(f32)
    tables(perm_ref, cos_ref, sin_ref, pos_col, pos_row, x_ref.shape[0] // 2)
    rows.forward()
    qkv.forward_next()
    cots.forward()
    qkv.forward_far()
    out.start()
    gate[0].start()
    up[0].start()
    rows.finish()
    saves[0].start()
    cots.finish()
    qkv.finish()
    saves[1].start()
    attend(rows_all, qkv_all, shifts, cos_ref, sin_ref, pos_col, pos_row, q_t, k_t, v_t, attn_t, lse, k_n, bias, attn)
    for i in range(6, 10):
        saves[i].start()
    gate[0].forward_next()
    up[0].forward_next()
    down[0].start()
    gate[1].start()
    out.finish()
    saves[2].start()
    saves[0].wait()
    scatter = sum_scatter(
        place,
        x_ref.shape[0],
        lambda at, cols: dot_nn(attn[at, :], out_all[:, cols]),
        *scatter_refs[:5],
        scatter_refs[5:9],
    )
    scatter.run()
    gate[0].forward_far()
    up[0].forward_far()
    down[0].forward_next()
    gain2, shift2 = gain2_ref[...].astype(f32)[None, :], bias2_ref[...].astype(f32)[None, :]

    def norm2(at):
        resid = x_ref[at, :].astype(f32) + scatter.total(at)
        resid_ref[at, :] = resid
        normed, _ = normal(resid)
        row_block[at, :] = (normed * gain2 + shift2).astype(bf16)

    row_loop(x_ref.shape[0], norm2)
    normeds.start()
    saves[10].start()
    normeds.forward()
    down[0].forward_far()
    gate[1].forward_next()
    up[1].start()
    normeds.finish()
    scatter.finish()

    def gates(h):
        def body(t):
            at = span(t, PAIR)
            gate_f[at, :] = dot_nt(rows_all[at, :], gateup_all[h * half : (h + 1) * half, :])

        tiles(seq // PAIR, body)

    def ups(h):
        def body(t):
            at = span(t, PAIR)
            value = dot_nt(rows_all[at, :], gateup_all[ff + h * half : ff + (h + 1) * half, :])
            g = gate_f[at, :]
            sigma = jax.nn.sigmoid(g)
            swish = g * sigma
            hidden = (swish * value).astype(bf16)
            hidden_ref[h, at, :] = hidden
            hidden_t[:, at] = hidden.T
            gate_side[h, at, :] = (value * sigma * (1.0 + g * (1.0 - sigma))).astype(bf16)
            up_side[h, at, :] = swish.astype(bf16)

        tiles(seq // PAIR, body)

    def sides(h):
        def body(t):
            at = span(t, PAIR)
            grad = dot_nt(cot_all[at, :], down_all[h * half : (h + 1) * half, :])
            gate_grad = (grad * gate_side[h, at, :].astype(f32)).astype(bf16)
            up_grad = (grad * up_side[h, at, :].astype(f32)).astype(bf16)
            gate_side[h, at, :] = gate_grad
            up_side[h, at, :] = up_grad
            gate_t[:, at] = gate_grad.T
            up_t[:, at] = up_grad.T

        tiles(seq // PAIR, body)

    def weights(target):
        def body(j):
            cols = span(j, 2 * PAIR)
            normed = rows_all[:, cols]
            target[:half, cols] = dot_nn(gate_t[...], normed).astype(bf16)
            target[half : 2 * half, cols] = dot_nn(up_t[...], normed).astype(bf16)
            target[2 * half : 3 * half, cols] = dot_nn(hidden_t[...], cot_all[:, cols]).astype(bf16)

        tiles(d // (2 * PAIR), body)

    gate[0].finish()
    gates(0)
    up[0].finish()
    ups(0)
    gate[1].forward_far()
    up[1].forward_next()
    down[1].start()
    down[0].finish()
    sides(0)
    for i in range(11, 14):
        saves[i].start()
    weights(part)
    summed = DepthScatter(place, part, part, got, both, width, dsend, drecv)
    summed.start()
    up[1].forward_far()
    down[1].forward_next()
    down[1].forward_far()
    gate[1].finish()
    gates(1)
    summed.hand_on(0)
    up[1].finish()
    saves[3].start()
    ups(1)
    summed.hand_on(1)
    summed.hand_on(2)
    down[1].finish()
    saves[4].start()
    saves[3].wait()
    sides(1)
    for i in range(14, 17):
        saves[i].start()
    weights(gateup_all)
    saves[5].start()
    summed.finish(first_sums)
    for i in (1, 2, *range(4, 17)):
        saves[i].wait()


def forward(perm, x, cot, gain1, bias1, gain2, bias2, shift, qkv, out, gateup, down):
    ndp, nctx = lax.axis_size("dp"), lax.axis_size("ctx")
    rows, d = x.shape
    seq, width, ff = rows * nctx, qkv.shape[2], gateup.shape[1]
    heads = width // HEAD_DIM
    bf16, f32 = jnp.bfloat16, jnp.float32
    row = [gain1, bias1, gain2, bias2]

    def shaped(shape, dtype=bf16):
        return jax.ShapeDtypeStruct(shape, dtype)

    return pl.pallas_call(
        forward_kernel,
        out_shape=(
            shaped((8, seq), f32),
            shaped((3 * ff // 2, d // ndp), f32),
            shaped((8, seq), f32),
            shaped((8, seq), f32),
            shaped((seq, 1), f32),
            shaped((1, seq), f32),
            shaped((rows, d), f32),
            shaped((width, seq)),
            shaped((width, seq)),
            shaped((width, seq)),
            shaped((width, seq)),
            shaped((2, seq, ff // 2)),
            shaped((2, seq, ff // 2)),
            shaped((2, seq, ff // 2)),
            shaped((seq, d)),
            shaped((3, d, width)),
            shaped((width, d)),
            shaped((2 * ff, d)),
            shaped((ff, d)),
            shaped((3 * ff // 2, d)),
        ),
        in_specs=[pl.BlockSpec(memory_space=pltpu.SMEM)] + [VMEM] * 7 + [ANY] * 4,
        out_specs=(VMEM,) * 6 + (ANY,) * 14,
        scratch_shapes=[
            pltpu.VMEM((rows, d), bf16),
            pltpu.VMEM((rows, d), bf16),
            pltpu.VMEM((seq, d), bf16),
            pltpu.VMEM((seq, d), bf16),
            pltpu.VMEM((3, d, width), bf16),
            pltpu.VMEM((width, d), bf16),
            pltpu.VMEM((2 * ff, d), bf16),
            pltpu.VMEM((ff, d), bf16),
            pltpu.VMEM((heads, seq, HEAD_DIM), bf16),
            pltpu.VMEM((seq, PAIR), f32),
            pltpu.VMEM((seq, width), bf16),
            pltpu.VMEM((seq, ff // 2), f32),
            pltpu.VMEM((ff // 2, seq), bf16),
            pltpu.VMEM((ff // 2, seq), bf16),
            pltpu.VMEM((ff // 2, seq), bf16),
            pltpu.VMEM((3 * ff // 2, d), bf16),
            pltpu.VMEM((3, width), f32),
            pltpu.VMEM((rows, d), f32),
            pltpu.VMEM((width, seq), bf16),
            pltpu.VMEM((width, seq), bf16),
            pltpu.VMEM((width, seq), bf16),
            pltpu.VMEM((width, seq), bf16),
            pltpu.VMEM((2, seq, ff // 2), bf16),
            pltpu.VMEM((2, seq, ff // 2), bf16),
            pltpu.VMEM((2, seq, ff // 2), bf16),
        ]
        + depth_sems(ndp) * 8
        + gather_sems(nctx) * 3
        + scatter_scratch(nctx, rows, d)
        + depth_scatter_scratch(ndp, 3 * ff // 2, d // ndp)
        + [DMA((17,))],
        compiler_params=pltpu.CompilerParams(
            collective_id=0, has_side_effects=True, vmem_limit_bytes=67_000_000
        ),
        cost_estimate=pl.CostEstimate(flops=0, bytes_accessed=700_000_000, transcendentals=0),
        name="forward",
    )(perm, x, cot, *row, shift, qkv, out, gateup, down)


def attend_back(
    grad_ref, w_ref, rows_ref, cos_ref, sin_ref, pos_col, pos_row, q_t, k_t, v_t, attn_t, lse,
    parts_ref, sums_ref, w_grads, g_t, delta, q_grad, kv_grad, bias, flat, rows_buf, rows_sem, between
):
    seq, d = grad_ref.shape
    width = w_ref.shape[0]
    heads = width // HEAD_DIM
    bf16, f32 = jnp.bfloat16, jnp.float32
    count = d // (2 * PAIR)

    def load(j):
        slot = lax.rem(j, 2)
        return pltpu.make_async_copy(rows_ref.at[:, span(j, 2 * PAIR)], rows_buf.at[slot], rows_sem.at[slot])

    def first(t):
        at = span(t, PAIR)
        grad = dot_nt(w_ref[...], grad_ref[at, :])
        both = grad * attn_t[:, at].astype(f32)
        for h in range(heads):
            delta[h : h + 1, at] = jnp.sum(both[h * HEAD_DIM : (h + 1) * HEAD_DIM], axis=0, keepdims=True)
        g_t[:, at] = grad.astype(bf16)

    tiles(seq // PAIR, first)
    between()
    q_grad[...] = jnp.zeros_like(q_grad)

    def keys(t):
        at = span(t, PAIR)
        bias[...] = jnp.where(pos_col[at, :] <= pos_row[...], 0.0, neg_big)
        for h in range(heads):
            feats = slice(h * HEAD_DIM, (h + 1) * HEAD_DIM)
            keys_t = k_t[feats, at]
            probs = jnp.exp(dot_nn(keys_t.T, q_t[feats, :]) + bias[...] - lse[h : h + 1, :])
            kv_grad[1, feats, at] = dot_nt(g_t[feats, :], probs.astype(bf16))
            back = dot_nn(v_t[feats, at].T, g_t[feats, :])
            scores = (probs * (back - delta[h : h + 1, :])).astype(bf16)
            kv_grad[0, feats, at] = dot_nt(q_t[feats, :], scores)
            q_grad[feats, :] += dot_nn(keys_t, scores)

    tiles(seq // PAIR, keys)
    load(0).start()
    sums_ref[...] = jnp.zeros_like(sums_ref)

    def part(t):
        at = span(t, PAIR)
        cosine, sine = cos_ref[:, at], sin_ref[:, at]
        for i in range(3):
            if i == 0:
                grad = turn(q_grad[:, at] * (1.0 / math.sqrt(HEAD_DIM)), cosine, -sine, heads)
            elif i == 1:
                grad = turn(kv_grad[0, :, at], cosine, -sine, heads)
            else:
                grad = kv_grad[1, :, at]
            natural = grad.T
            sums_ref[i : i + 1, :] += jnp.sum(natural, axis=0, keepdims=True)
            parts_ref[i, at, :] = natural.astype(bf16)
            flat[i, :, at] = grad.astype(bf16)

    tiles(seq // PAIR, part)

    def weights(j):
        pl.when(j + 1 < count)(lambda: load(j + 1).start())
        load(j).wait()
        cols = span(j, 2 * PAIR)
        rows = rows_buf[lax.rem(j, 2)]
        for i in range(3):
            w_grads[i * width : (i + 1) * width, cols] = dot_nn(flat[i], rows).astype(bf16)
        w_grads[3 * width : 4 * width, cols] = dot_nn(attn_t[...], grad_ref[:, cols]).astype(bf16)

    tiles(count, weights)


def middle_kernel(
    gate_ref, up_ref, w_hbm, part_ref, resid_ref, cot_ref, gain_ref, out_hbm, rows_ref,
    cos_ref, sin_ref, pos_col, pos_row, q_hbm, k_hbm, v_hbm, attn_hbm, lse,
    grad_ref, vec_ref, parts_ref, sums_ref, second_sums, w_out,
    arena, part_all, block, out_ref, q_t, k_t, v_t, attn_t, grad_all, g_t, delta, q_grad, kv_grad, bias, flat, rows_buf, rows_sem, save_sem, *scratch
):
    place = Place()
    greet(place, along_dp=True)
    scratch = list(scratch)

    def take(n):
        head = scratch[:n]
        del scratch[:n]
        return head

    rows = resid_ref.shape[0]
    half, d = gate_ref.shape[2], part_ref.shape[1]
    ff = 2 * half
    piece = d // place.ndp
    refs = take(9)
    sum_refs = take(4)
    summed = DepthScatter(place, part_ref, part_all, *sum_refs[:2], piece, *sum_refs[2:])
    summed.start()
    load = pltpu.make_async_copy(w_hbm, arena, save_sem.at[0])
    fetch = pltpu.make_async_copy(part_ref, part_all, save_sem.at[1])
    later = [
        pltpu.make_async_copy(src, dst, save_sem.at[4 + i])
        for i, (src, dst) in enumerate(
            ((out_hbm, out_ref), (q_hbm, q_t), (k_hbm, k_t), (v_hbm, v_t), (attn_hbm, attn_t))
        )
    ]
    load.start()
    fetch.start()
    for copy in later:
        copy.start()
    load.wait()

    def product(at, cols):
        total = dot_nn(gate_ref[0, at, :], arena[:half, cols])
        total = total + dot_nn(gate_ref[1, at, :], arena[half:ff, cols])
        total = total + dot_nn(up_ref[0, at, :], arena[ff : ff + half, cols])
        return total + dot_nn(up_ref[1, at, :], arena[ff + half :, cols])

    scatter = sum_scatter(place, rows, product, *refs[:5], refs[5:9])
    scatter.run()
    gain = gain_ref[...].astype(jnp.float32)[None, :]
    vec_ref[...] = jnp.zeros_like(vec_ref)

    def back(at):
        grad = scatter.total(at)
        normed, rscale = normal(resid_ref[at, :])
        vec_ref[0:1, :] += jnp.sum(grad * normed, axis=0, keepdims=True)
        vec_ref[1:2, :] += jnp.sum(grad, axis=0, keepdims=True)
        out = cot_ref[at, :] + normal_back(grad, normed, rscale, gain)
        grad_ref[at, :] = out
        block[at, :] = out.astype(jnp.bfloat16)

    row_loop(rows, back)
    gathered = row_gather(place, block, grad_all, *take(3))
    gathered.start()
    fetch.wait()
    summed.hand_on(0)
    gathered.forward()
    gathered.finish()
    for copy in later:
        copy.wait()
    scatter.finish()

    def between():
        summed.hand_on(1)
        summed.hand_on(2)

    w_grads = arena.at[: w_out.shape[0]]
    attend_back(
        grad_all, out_ref, rows_ref, cos_ref, sin_ref, pos_col, pos_row, q_t, k_t, v_t, attn_t, lse,
        parts_ref, sums_ref, w_grads, g_t, delta, q_grad, kv_grad, bias, flat, rows_buf, rows_sem, between,
    )
    keep = pltpu.make_async_copy(w_grads, w_out, save_sem.at[2])
    keep.start()
    summed.finish(second_sums)
    keep.wait()


def middle(gate_grad, up_grad, w, part, resid, cot, gain, out, rows_all, cosine, sine, pos_col, pos_row, q_t, k_t, v_t, attn_t, lse):
    ndp, nctx = lax.axis_size("dp"), lax.axis_size("ctx")
    rows, d = resid.shape
    seq, width, ff = rows * nctx, out.shape[0], w.shape[0] // 2
    bf16, f32 = jnp.bfloat16, jnp.float32
    return pl.pallas_call(
        middle_kernel,
        out_shape=(
            jax.ShapeDtypeStruct((rows, d), f32),
            jax.ShapeDtypeStruct((2, d), f32),
            jax.ShapeDtypeStruct((3, seq, width), bf16),
            jax.ShapeDtypeStruct((3, width), f32),
            jax.ShapeDtypeStruct((3 * ff // 2, d // ndp), f32),
            jax.ShapeDtypeStruct((4 * width, d), bf16),
        ),
        in_specs=[VMEM] * 2 + [ANY] * 2 + [VMEM] * 3 + [ANY] * 2 + [VMEM] * 4 + [ANY] * 4 + [VMEM],
        out_specs=(VMEM,) * 5 + (ANY,),
        scratch_shapes=[
            pltpu.VMEM((2 * ff, d), bf16),
            pltpu.VMEM((3 * ff // 2, d), bf16),
            pltpu.VMEM((rows, d), bf16),
            pltpu.VMEM((width, d), bf16),
            pltpu.VMEM((width, seq), bf16),
            pltpu.VMEM((width, seq), bf16),
            pltpu.VMEM((width, seq), bf16),
            pltpu.VMEM((width, seq), bf16),
            pltpu.VMEM((seq, d), bf16),
            pltpu.VMEM((width, seq), bf16),
            pltpu.VMEM((8, seq), f32),
            pltpu.VMEM((width, seq), f32),
            pltpu.VMEM((2, width, seq), f32),
            pltpu.VMEM((PAIR, seq), f32),
            pltpu.VMEM((3, width, seq), bf16),
            pltpu.VMEM((2, seq, 2 * PAIR), bf16),
            DMA((2,)),
            DMA((9,)),
        ]
        + scatter_scratch(nctx, rows, d)
        + depth_scatter_scratch(ndp, 3 * ff // 2, d // ndp)
        + gather_sems(nctx),
        compiler_params=pltpu.CompilerParams(
            collective_id=2, has_side_effects=True, vmem_limit_bytes=67_000_000
        ),
        cost_estimate=pl.CostEstimate(flops=0, bytes_accessed=300_000_000, transcendentals=0),
        name="middle",
    )(gate_grad, up_grad, w, part, resid, cot, gain, out, rows_all, cosine, sine, pos_col, pos_row, q_t, k_t, v_t, attn_t, lse)


class VectorSum:
    def __init__(self, place, value, from_ctx, from_dp, plane, ctx_send, ctx_recv, dp_send, dp_recv):
        self.place, self.value, self.from_ctx, self.from_dp, self.plane = place, value, from_ctx, from_dp, plane
        self.ctx_send, self.ctx_recv, self.dp_send, self.dp_recv = ctx_send, ctx_recv, dp_send, dp_recv

    def across(self, i):
        place = self.place
        return push(
            self.value, self.from_ctx.at[place.c], self.ctx_send.at[i - 1], self.ctx_recv.at[place.c],
            place.at(lax.rem(place.c + i, place.nctx)),
        )

    def along(self, i):
        place = self.place
        return push(
            self.plane, self.from_dp.at[place.z], self.dp_send.at[i - 1], self.dp_recv.at[place.z],
            {"dp": lax.rem(place.z + i, place.ndp), "ctx": place.c},
        )

    def start(self):
        for i in range(1, self.place.nctx):
            self.across(i).start()
        self.from_ctx[self.place.c] = self.value[...]

    def turn(self):
        place = self.place
        for i in range(1, place.nctx):
            c = lax.rem(place.c + i, place.nctx)
            push(self.value, self.from_ctx.at[c], self.ctx_send.at[0], self.ctx_recv.at[c], place.at(c)).wait_recv()
        total = self.from_ctx[0]
        for i in range(1, place.nctx):
            total = total + self.from_ctx[i]
        self.plane[...] = total
        self.from_dp[place.z] = total
        for i in range(1, place.ndp):
            self.along(i).start()

    def finish(self, out_ref):
        place = self.place
        for i in range(1, place.ndp):
            z = lax.rem(place.z + i, place.ndp)
            device = {"dp": z, "ctx": place.c}
            push(self.plane, self.from_dp.at[z], self.dp_send.at[0], self.dp_recv.at[z], device).wait_recv()
        total = self.from_dp[0]
        for i in range(1, place.ndp):
            total = total + self.from_dp[i]
        out_ref[...] = total
        for i in range(1, place.nctx):
            self.across(i).wait_send()
        for i in range(1, place.ndp):
            self.along(i).wait_send()


def vector_scratch(ndp, nctx, shape):
    f32 = jnp.float32
    return [
        pltpu.VMEM(shape, f32),
        pltpu.VMEM((nctx,) + shape, f32),
        pltpu.VMEM((ndp,) + shape, f32),
        pltpu.VMEM(shape, f32),
        DMA((nctx - 1,)),
        DMA((nctx,)),
        DMA((ndp - 1,)),
        DMA((ndp,)),
    ]


def tail_kernel(
    w_grads, parts_hbm, qkv_hbm, x_ref, grad_ref, gain_ref, hidden_hbm, down_ref, resid_ref, vec_ref, sums_ref,
    block_out, input_grad, small, qkv_grads, out_grads,
    total, *scratch
):
    place = Place()
    greet(place, all_ctx=True, along_dp=True)
    scratch = list(scratch)

    def take(n):
        head = scratch[:n]
        del scratch[:n]
        return head

    rows, d = x_ref.shape
    width = qkv_hbm.shape[2]
    first_refs, second_refs = take(9), take(9)
    long_refs, short_refs = take(4), take(4)
    vectors = VectorSum(place, *take(8))
    w_all, down_all, parts_ref, qkv_ref, hidden_ref, load_sem = take(6)
    piece, cut = d // place.ndp, 3 * width
    upper, lower = pl.ds(0, cut), pl.ds(cut, width)
    long_sum = DepthScatter(place, w_grads.at[upper], w_all.at[upper], *long_refs[:2], piece, *long_refs[2:])
    short_sum = DepthScatter(place, w_grads.at[lower], w_all.at[lower], *short_refs[:2], piece, *short_refs[2:])
    long_sum.start_first()
    short_sum.start_first()
    long_sum.start_last()
    short_sum.start_last()
    loads = [
        pltpu.make_async_copy(src, dst, load_sem.at[i])
        for i, (src, dst) in enumerate(
            ((parts_hbm, parts_ref), (qkv_hbm, qkv_ref), (w_grads, w_all), (hidden_hbm, hidden_ref), (down_ref, down_all))
        )
    ]
    for copy in loads:
        copy.start()

    def product(at, cols):
        part = dot_nt(parts_ref[0, at, :], qkv_ref[0, cols, :])
        part = part + dot_nt(parts_ref[1, at, :], qkv_ref[1, cols, :])
        return part + dot_nt(parts_ref[2, at, :], qkv_ref[2, cols, :])

    first = sum_scatter(place, rows, product, *first_refs[:5], first_refs[5:9])
    half = hidden_ref.shape[2]

    def down_product(at, cols):
        return dot_nn(hidden_ref[0, at, :], down_all[:half, cols]) + dot_nn(hidden_ref[1, at, :], down_all[half:, cols])

    second = sum_scatter(place, rows, down_product, *second_refs[:5], second_refs[5:9])
    for copy in loads[:2]:
        copy.wait()
    first.run()
    gain = gain_ref[...].astype(jnp.float32)[None, :]
    value = vectors.value
    value[...] = jnp.zeros_like(value)
    value[2:4, :] = vec_ref[...]
    value[4:7, pl.ds(pl.multiple_of(place.c * width, width), width)] = sums_ref[...]

    def back(at):
        grad = first.total(at)
        normed, rscale = normal(x_ref[at, :].astype(jnp.float32))
        value[0:1, :] += jnp.sum(grad * normed, axis=0, keepdims=True)
        value[1:2, :] += jnp.sum(grad, axis=0, keepdims=True)
        input_grad[at, :] = grad_ref[at, :] + normal_back(grad, normed, rscale, gain)

    row_loop(rows, back)
    vectors.start()
    for copy in loads[2:]:
        copy.wait()
    long_sum.hand_on(0)

    def between_first():
        long_sum.hand_on(1)
        short_sum.hand_on(0)

    def between_second():
        long_sum.hand_on(2)
        short_sum.hand_on(1)

    second.run((between_first, between_second))
    short_sum.hand_on(2)

    def add(at):
        block_out[at, :] = (resid_ref[at, :] + second.total(at)).astype(jnp.bfloat16)

    row_loop(rows, add)
    vectors.turn()
    first.finish()
    second.finish()
    vectors.finish(small)
    long_sum.finish(total.at[upper])
    short_sum.finish(out_grads)
    for i in range(3):
        qkv_grads[i] = total[i * width : (i + 1) * width, :].T


def tail(w_grads, parts, qkv, x, grad, gain, hidden, down, resid, vec, sums):
    ndp, nctx = lax.axis_size("dp"), lax.axis_size("ctx")
    rows, d = x.shape
    width = qkv.shape[2]
    bf16, f32 = jnp.bfloat16, jnp.float32
    return pl.pallas_call(
        tail_kernel,
        out_shape=(
            jax.ShapeDtypeStruct((rows, d), bf16),
            jax.ShapeDtypeStruct((rows, d), f32),
            jax.ShapeDtypeStruct((8, d), f32),
            jax.ShapeDtypeStruct((3, d // ndp, width), f32),
            jax.ShapeDtypeStruct((width, d // ndp), f32),
        ),
        in_specs=[ANY] * 3 + [VMEM] * 3 + [ANY] * 2 + [VMEM] * 3,
        out_specs=(VMEM,) * 5,
        scratch_shapes=[pltpu.VMEM((3 * width, d // ndp), f32)]
        + scatter_scratch(nctx, rows, d) * 2
        + depth_scatter_scratch(ndp, 3 * width, d // ndp)
        + depth_scatter_scratch(ndp, width, d // ndp)
        + vector_scratch(ndp, nctx, (8, d))
        + [pltpu.VMEM(v.shape, bf16) for v in (w_grads, down, parts, qkv, hidden)]
        + [DMA((5,))],
        compiler_params=pltpu.CompilerParams(
            collective_id=3, has_side_effects=True, vmem_limit_bytes=67_000_000
        ),
        cost_estimate=pl.CostEstimate(flops=0, bytes_accessed=300_000_000, transcendentals=0),
        name="tail",
    )(w_grads, parts, qkv, x, grad, gain, hidden, down, resid, vec, sums)


def per_device(
    block_input,
    out_cotangent,
    group_perm,
    attn_norm_gain,
    attn_norm_bias,
    qkv_weight,
    qkv_bias,
    out_weight,
    mlp_norm_gain,
    mlp_norm_bias,
    gateup_weight,
    down_weight,
):
    width_local = qkv_weight.shape[2]
    (
        lse, first_sums, cos_all, sin_all, pos_col, pos_row,
        residual_stream, q_t, k_t, v_t, attn_t, hidden_b, gate_grad, up_grad,
        rows_all, qkv_local, out_local, gateup_local, down_local, mlp_grads,
    ) = forward(
        group_perm, block_input, out_cotangent, attn_norm_gain, attn_norm_bias, mlp_norm_gain, mlp_norm_bias, qkv_bias,
        qkv_weight, out_weight, gateup_weight.transpose(0, 2, 1), down_weight,
    )
    resid_grad, second_vectors, grad_parts_b, shift_part, second_sums, attn_grads = middle(
        gate_grad, up_grad, gateup_local, mlp_grads, residual_stream, out_cotangent, mlp_norm_gain, out_local,
        rows_all, cos_all, sin_all, pos_col, pos_row, q_t, k_t, v_t, attn_t, lse,
    )
    block_output, input_grad, small, qkv_grads, out_grads = tail(
        attn_grads, grad_parts_b, qkv_local, block_input, resid_grad, attn_norm_gain,
        hidden_b, down_local, residual_stream, second_vectors, shift_part,
    )
    half = first_sums.shape[0] // 3
    both = [
        jnp.concatenate([first_sums[i * half : (i + 1) * half], second_sums[i * half : (i + 1) * half]])
        for i in range(3)
    ]
    gateup_grads, down_grads = jnp.stack(both[:2]), both[2]
    return (
        block_output,
        input_grad,
        small[0],
        small[1],
        qkv_grads,
        small[4:7],
        out_grads,
        small[2],
        small[3],
        gateup_grads.transpose(0, 2, 1),
        down_grads,
    )


def solution(mesh):
    return jax.shard_map(
        per_device,
        mesh=mesh,
        in_specs=(
            P(("dp", "ctx"), None),
            P(("dp", "ctx"), None),
            P("dp", None),
            P(),
            P(),
            P(None, "dp", "ctx"),
            P(),
            P("ctx", "dp"),
            P(),
            P(),
            P(None, "dp", "ctx"),
            P("ctx", "dp"),
        ),
        out_specs=(
            P(("dp", "ctx"), None),
            P(("dp", "ctx"), None),
            P(),
            P(),
            P(None, "dp", "ctx"),
            P(),
            P("ctx", "dp"),
            P(),
            P(),
            P(None, "dp", "ctx"),
            P("ctx", "dp"),
        ),
        check_vma=False,
    )
```

```python
import functools
import math

import jax
import jax.numpy as jnp
from jax import lax
from jax.experimental import pallas as pl
from jax.experimental.pallas import tpu as pltpu
from jax.sharding import PartitionSpec as P

MESH = pl.DeviceIdType.MESH
VMEM = pl.BlockSpec(memory_space=pltpu.VMEM)
ANY = pl.BlockSpec(memory_space=pl.ANY)
DMA = pltpu.SemaphoreType.DMA

D = 2048
HEADS = 32
HEAD_DIM = 64
ROT = 16


eps_norm = 1e-05
rope_base = 10000.0
neg_big = -1e30


class Place:
    def __init__(self):
        self.ndp = lax.axis_size("dp")
        self.nctx = lax.axis_size("ctx")
        self.nchip = self.nctx // 2
        self.z = lax.axis_index("dp")
        self.c = lax.axis_index("ctx")
        self.p = lax.div(self.c, 2)
        self.k = lax.rem(self.c, 2)

    def chip(self, offset):
        return lax.rem(self.p + offset, self.nchip)

    def at(self, c):
        return {"dp": self.z, "ctx": c}

    def partner(self):
        return self.at(2 * self.p + 1 - self.k)

    def same_core(self, q):
        return self.at(2 * q + self.k)


def greet(place, along_ctx=True, along_dp=False, all_ctx=False):
    barrier = pltpu.get_barrier_semaphore()
    peers = []
    if all_ctx:
        peers += [place.at(lax.rem(place.c + i, place.nctx)) for i in range(1, place.nctx)]
    elif along_ctx:
        peers += [place.partner()] + [place.same_core(place.chip(i)) for i in range(1, place.nchip)]
    if along_dp:
        peers += [{"dp": lax.rem(place.z + i, place.ndp), "ctx": place.c} for i in range(1, place.ndp)]
    for peer in peers:
        pl.semaphore_signal(barrier, inc=1, device_id=peer, device_id_type=MESH)
    pl.semaphore_wait(barrier, len(peers))


def push(src, dst, send, recv, device):
    return pltpu.make_async_remote_copy(
        src_ref=src, dst_ref=dst, send_sem=send, recv_sem=recv, device_id=device, device_id_type=MESH
    )


class RowGather:
    def __init__(self, place, block, whole, send, recv, local):
        self.place, self.block, self.whole = place, block, whole
        self.send, self.recv, self.local = send, recv, local
        self.rows = block.shape[0]

    def slot(self, c):
        return self.whole.at[pl.ds(pl.multiple_of(c * self.rows, self.rows), self.rows)]

    def direct(self, i):
        place = self.place
        q = place.chip(i)
        return push(self.block, self.slot(place.c), self.send.at[i], self.recv.at[place.c], place.same_core(q))

    def own(self):
        place = self.place
        return push(self.block, self.slot(place.c), self.send.at[0], self.recv.at[place.c], place.partner())

    def passed(self, i):
        place = self.place
        c = 2 * place.chip(i) + place.k
        return push(
            self.slot(c), self.slot(c), self.send.at[place.nchip + i - 1], self.recv.at[c], place.partner()
        )

    def arrival(self, c):
        return push(self.block, self.slot(c), self.send.at[0], self.recv.at[c], self.place.partner())

    def keep(self):
        return pltpu.make_async_copy(self.block, self.slot(self.place.c), self.local)

    def start(self):
        for i in range(1, self.place.nchip):
            self.direct(i).start()
        self.own().start()
        self.keep().start()

    def forward(self):
        place = self.place
        for i in range(1, place.nchip):
            self.arrival(2 * place.chip(i) + place.k).wait_recv()
            self.passed(i).start()

    def finish(self):
        place = self.place
        for i in range(place.nchip):
            self.arrival(2 * place.chip(i) + 1 - place.k).wait_recv()
        self.own().wait_send()
        for i in range(1, place.nchip):
            self.direct(i).wait_send()
            self.passed(i).wait_send()
        self.keep().wait()


class BoxGather(RowGather):
    def part(self, c, half):
        size = self.rows // 2
        return self.whole.at[pl.ds(pl.multiple_of(c * self.rows + half * size, size), size)]

    def near(self, axis):
        place = self.place
        other = 1 - lax.rem(place.p, 2) if axis == 0 else 1 - lax.div(place.p, 2)
        q = 2 * lax.div(place.p, 2) + other if axis == 0 else 2 * other + lax.rem(place.p, 2)
        return 2 * q + place.k

    def across(self):
        return 2 * (3 - self.place.p) + self.place.k

    def piece(self, c, half, sem, to, own=False):
        size = self.rows // 2
        src = self.block.at[pl.ds(half * size, size)] if own else self.part(c, half)
        return push(src, self.part(c, half), self.send.at[sem], self.recv.at[2 * c + half], self.place.at(to))

    def own(self):
        place = self.place
        return push(self.block, self.slot(place.c), self.send.at[0], self.recv.at[2 * place.c], place.partner())

    def first(self):
        c = self.place.c
        return [self.piece(c, h, 1 + n, self.near(a), True) for n, (a, h) in enumerate(((0, 0), (1, 1), (0, 1), (1, 0)))]

    def second(self):
        return [self.piece(self.near(a), a, 5 + a, self.near(1 - a)) for a in (0, 1)]

    def to_partner(self):
        place = self.place
        pair = 2 * place.p + 1 - place.k
        return [
            self.piece(c, h, 7 + n, pair)
            for n, (c, h) in enumerate(
                ((self.near(0), 0), (self.near(1), 1), (self.near(0), 1), (self.near(1), 0), (self.across(), 0), (self.across(), 1))
            )
        ]

    def start(self):
        for copy in self.first():
            copy.start()
        self.own().start()
        self.keep().start()

    def forward(self):
        second, pair = self.second(), self.to_partner()
        for n, copy in enumerate(pair):
            copy.wait_recv()
            if n < 2:
                second[n].start()
            copy.start()

    def finish(self):
        place = self.place
        pair = 2 * place.p + 1 - place.k
        self.arrival_pair().wait_recv()
        for n in range(6):
            c = (self.near(0), self.near(1), self.near(0), self.near(1), self.across(), self.across())[n]
            half = (0, 1, 1, 0, 0, 1)[n]
            twin = c + 1 - 2 * place.k
            self.piece(twin, half, 7 + n, pair).wait_recv()
        self.own().wait_send()
        for copy in self.first() + self.second() + self.to_partner():
            copy.wait_send()
        self.keep().wait()

    def arrival_pair(self):
        c = self.place.c + 1 - 2 * self.place.k
        return push(self.block, self.slot(c), self.send.at[0], self.recv.at[2 * c], self.place.partner())


def row_gather(place, *args):
    return (BoxGather if place.nchip == 4 else RowGather)(place, *args)


def gather_sems(nctx):
    return [DMA((13,)), DMA((2 * nctx,)), DMA] if nctx == 8 else [DMA((nctx,)), DMA((nctx,)), DMA]


class DepthGather:
    def __init__(self, place, piece, whole, where, send, recv, local, passing=True):
        self.place, self.piece, self.whole, self.where = place, piece, whole, where
        self.send, self.recv, self.local = send, recv, local
        self.line = place.ndp == 4 and passing
        z = place.z
        self.end = jnp.logical_or(z == 0, z == 3)
        self.middle = jnp.logical_not(self.end)
        self.near = jnp.clip(3 * (z - 1), 0, 3)
        self.far = 3 - self.near
        self.other = jnp.clip(3 - z, 1, 2)

    def copy(self, src, z_src, z_dst, sem):
        return push(
            src, self.where(self.whole, z_src), self.send.at[sem], self.recv.at[z_src], {"dp": z_dst, "ctx": self.place.c}
        )

    def directs(self):
        z, n = self.place.z, self.place.ndp
        if not self.line:
            return [(None, self.copy(self.piece, z, lax.rem(z + i, n), i - 1)) for i in range(1, n)]
        out = []
        for sem, step in enumerate((1, -1, 2, -2)):
            d = z + step
            ok = jnp.logical_and(d >= 0, d < 4)
            if abs(step) == 2:
                ok = jnp.logical_and(ok, self.end)
            out.append((ok, self.copy(self.piece, z, jnp.clip(d, 0, 3), sem)))
        return out

    def keep(self):
        return pltpu.make_async_copy(self.piece, self.where(self.whole, self.place.z), self.local)

    def start(self):
        for ok, copy in self.directs():
            if ok is None:
                copy.start()
            else:
                pl.when(ok)(copy.start)
        self.keep().start()

    def passed(self, src, sem):
        return self.copy(self.where(self.whole, src), src, self.near, sem)

    def forward_next(self):
        self.forward(self.other, 4)

    def forward_far(self):
        self.forward(self.far, 5)

    def forward(self, src, sem):
        if self.line:

            @pl.when(self.middle)
            def _():
                self.copy(self.piece, src, src, sem).wait_recv()
                self.passed(src, sem).start()

    def finish(self):
        z, n = self.place.z, self.place.ndp
        for i in range(1, n):
            src = lax.rem(z + i, n)
            wait = self.copy(self.piece, src, src, 0).wait_recv
            if self.line:
                pl.when(jnp.logical_or(self.end, src == self.near))(wait)
            else:
                wait()
        for ok, copy in self.directs():
            if ok is None:
                copy.wait_send()
            else:
                pl.when(ok)(copy.wait_send)
        if self.line:

            @pl.when(self.middle)
            def _():
                self.passed(self.other, 4).wait_send()
                self.passed(self.far, 5).wait_send()

        self.keep().wait()


def depth_sems(ndp):
    return [DMA((max(ndp, 6),)), DMA((ndp,)), DMA]


STEP = 16


def row_loop(rows, body):
    def step(i, carry):
        body(pl.ds(pl.multiple_of(i * STEP, STEP), STEP))
        return carry

    lax.fori_loop(0, rows // STEP, step, 0)


def normal(values):
    centred = values - jnp.mean(values, axis=-1, keepdims=True)
    rscale = lax.rsqrt(jnp.mean(centred * centred, axis=-1, keepdims=True) + eps_norm)
    return centred * rscale, rscale


def normal_back(grad_out, normed, rscale, gain):
    scaled = grad_out * gain
    return rscale * (
        scaled
        - jnp.mean(scaled, axis=-1, keepdims=True)
        - normed * jnp.mean(scaled * normed, axis=-1, keepdims=True)
    )


class SumScatter:
    TILE = 512

    def __init__(self, place, rows, product, mine, to_pair, from_pair, to_chip, from_chip, sems):
        self.place, self.rows, self.product = place, rows, product
        self.mine, self.to_pair, self.from_pair = mine, to_pair, from_pair
        self.to_chip, self.from_chip = to_chip, from_chip
        self.pair_send, self.pair_recv, self.chip_send, self.chip_recv = sems

    def pair(self, i):
        return push(
            self.to_pair.at[lax.rem(i, 2)], self.from_pair.at[i], self.pair_send.at[i], self.pair_recv.at[i], self.place.partner()
        )

    def chips(self, i):
        return push(
            self.to_chip.at[i],
            self.from_chip.at[i],
            self.chip_send.at[i],
            self.chip_recv.at[i],
            self.place.same_core(self.place.chip(i + 1)),
        )

    def chip_of(self, i):
        return lax.rem(self.place.p + 1 + i, self.place.nchip)

    def hand_on(self, i):
        self.pair(i).wait_recv()

        def add(at):
            both = self.mine[lax.rem(i, 2), at, :] + self.from_pair[i, at, :].astype(jnp.float32)
            self.to_chip[i, at, :] = both.astype(jnp.bfloat16)

        row_loop(self.rows, add)
        self.chips(i).start()

    def last(self, hooks):
        for hook in hooks:
            hook()
        nchip = self.place.nchip
        self.pair(nchip - 1).wait_recv()
        for i in range(nchip - 1):
            self.chips(i).wait_recv()

    def run(self, hooks=()):
        place, rows, tile = self.place, self.rows, self.TILE
        nchip = place.nchip
        width = self.mine.shape[-1]

        def step(i, carry):
            first = pl.multiple_of(self.chip_of(i) * 2 * rows, 2 * rows)
            slot = lax.rem(i, 2)
            pl.when(i >= 2)(lambda: self.pair(i - 2).wait_send())

            def columns(j, inner):
                cols = pl.ds(pl.multiple_of(j * tile, tile), tile)
                part = self.product(pl.ds(first, 2 * rows), cols)

                @pl.when(place.k == 0)
                def _():
                    self.mine[slot, :, cols] = part[:rows]
                    self.to_pair[slot, :, cols] = part[rows:].astype(jnp.bfloat16)

                @pl.when(place.k == 1)
                def _():
                    self.mine[slot, :, cols] = part[rows:]
                    self.to_pair[slot, :, cols] = part[:rows].astype(jnp.bfloat16)

                return inner

            lax.fori_loop(0, width // tile, columns, 0)
            self.pair(i).start()
            pl.when(i > 0)(lambda: self.hand_on(i - 1))
            return carry

        lax.fori_loop(0, nchip, step, 0)
        self.last(list(hooks))

    def total(self, at):
        last = self.place.nchip - 1
        value = self.mine[last % 2, at, :] + self.from_pair[last, at, :].astype(jnp.float32)
        for i in range(last):
            value = value + self.from_chip[i, at, :].astype(jnp.float32)
        return value

    def finish(self):
        for i in range(max(self.place.nchip - 2, 0), self.place.nchip):
            self.pair(i).wait_send()
        for i in range(self.place.nchip - 1):
            self.chips(i).wait_send()


class BoxScatter(SumScatter):
    def near(self, axis):
        p = self.place.p
        x, y = lax.rem(p, 2), lax.div(p, 2)
        return self.place.same_core(2 * y + 1 - x if axis == 0 else 2 * (1 - y) + x)

    def half(self, src, dst, rows, sem, axis):
        size = self.rows // 2
        at = pl.ds(rows * size, size)
        return push(
            self.to_chip.at[src, at], self.from_chip.at[dst, at], self.chip_send.at[sem], self.chip_recv.at[sem], self.near(axis)
        )

    def moves(self):
        return [
            self.half(0, 2, 0, 0, 0),
            self.half(0, 2, 1, 1, 1),
            self.half(1, 0, 0, 2, 0),
            self.half(2, 1, 1, 3, 1),
            self.half(1, 0, 1, 4, 0),
            self.half(2, 1, 0, 5, 1),
        ]

    def chip_of(self, i):
        p = self.place.p
        x, y = lax.rem(p, 2), lax.div(p, 2)
        other_x = jnp.logical_or(i == 0, i == 1)
        other_y = jnp.logical_or(i == 0, i == 2)
        return 2 * jnp.where(other_y, 1 - y, y) + jnp.where(other_x, 1 - x, x)

    def hand_on(self, i):
        self.pair(i).wait_recv()
        slot = lax.rem(i, 2)

        def add(at):
            both = self.mine[slot, at, :] + self.from_pair[i, at, :].astype(jnp.float32)
            self.to_chip[i, at, :] = both.astype(jnp.bfloat16)

        row_loop(self.rows, add)
        moves = self.moves()

        @pl.when(i == 0)
        def _():
            moves[0].start()
            moves[1].start()

        pl.when(i == 1)(moves[2].start)
        pl.when(i == 2)(moves[3].start)

    def last(self, hooks):
        moves = self.moves()
        size = self.rows // 2
        for arrived, src, first, onward in ((1, 1, size, 4), (0, 2, 0, 5)):
            if hooks:
                hooks.pop(0)()
            moves[arrived].wait_recv()

            def add(at, src=src, first=first):
                at = pl.ds(pl.multiple_of(first + at.start, STEP), STEP)
                both = self.to_chip[src, at, :].astype(jnp.float32) + self.from_chip[2, at, :].astype(jnp.float32)
                self.to_chip[src, at, :] = both.astype(jnp.bfloat16)

            row_loop(size, add)
            moves[onward].start()
        self.pair(3).wait_recv()
        for n in (2, 3, 4, 5):
            moves[n].wait_recv()

    def total(self, at):
        value = self.mine[1, at, :] + self.from_pair[3, at, :].astype(jnp.float32)
        return value + self.from_chip[0, at, :].astype(jnp.float32) + self.from_chip[1, at, :].astype(jnp.float32)

    def finish(self):
        for i in (2, 3):
            self.pair(i).wait_send()
        for copy in self.moves():
            copy.wait_send()


def sum_scatter(place, *args):
    return (BoxScatter if place.nchip == 4 else SumScatter)(place, *args)


def scatter_scratch(nctx, rows, d):
    n = nctx // 2
    bf16 = jnp.bfloat16
    return [
        pltpu.VMEM((2, rows, d), jnp.float32),
        pltpu.VMEM((2, rows, d), bf16),
        pltpu.VMEM((n, rows, d), bf16),
        pltpu.VMEM((n - 1, rows, d), bf16),
        pltpu.VMEM((n - 1, rows, d), bf16),
        DMA((n,)),
        DMA((n,)),
        DMA((6 if n == 4 else n - 1,)),
        DMA((6 if n == 4 else n - 1,)),
    ]


def dot_nn(a, b):
    return jnp.dot(a, b, preferred_element_type=jnp.float32)


def dot_nt(a, b):
    return lax.dot_general(a, b, (((1,), (1,)), ((), ())), preferred_element_type=jnp.float32)


HALF = ROT // 2
PAIR = 256


def tiles(count, body):
    def step(i, carry):
        body(i)
        return carry

    lax.fori_loop(0, count, step, 0)


def span(i, size):
    return pl.ds(pl.multiple_of(i * size, size), size)


def turn(columns, cosine, sine, heads):
    out = []
    for h in range(heads):
        at = h * HEAD_DIM
        a, b = columns[at : at + HALF], columns[at + HALF : at + ROT]
        out += [a * cosine - b * sine, b * cosine + a * sine, columns[at + ROT : at + HEAD_DIM]]
    return jnp.concatenate(out, axis=0)


def attend(rows_ref, w_ref, shift_ref, cos_ref, sin_ref, pos_col, pos_row, q_t, k_t, v_t, attn_t, lse, k_n, bias, attn):
    seq = rows_ref.shape[0]
    width = w_ref.shape[2]
    heads = width // HEAD_DIM
    bf16 = jnp.bfloat16

    def project(t):
        at = span(t, PAIR)
        cosine, sine = cos_ref[:, at], sin_ref[:, at]
        for i, ref in enumerate((q_t, k_t, v_t)):
            raw = (dot_nn(rows_ref[at, :], w_ref[i]) + shift_ref[i : i + 1, :]).T
            if i < 2:
                raw = turn(raw, cosine, sine, heads)
            raw = raw.astype(bf16)
            if i == 0:
                raw = raw * jnp.asarray(1.0 / math.sqrt(HEAD_DIM), bf16)
            ref[:, at] = raw

    tiles(seq // PAIR, project)
    for h in range(heads):
        k_n[h] = k_t[h * HEAD_DIM : (h + 1) * HEAD_DIM, :].T

    def queries(t):
        at = span(t, PAIR)
        bias[...] = jnp.where(pos_col[...] <= pos_row[:, at], 0.0, neg_big)

        for h in range(heads):
            feats = slice(h * HEAD_DIM, (h + 1) * HEAD_DIM)
            scores = dot_nn(k_n[h], q_t[feats, at]) + bias[...]
            peak = jnp.max(scores, axis=0, keepdims=True)
            probs = jnp.exp(scores - peak)
            total = jnp.sum(probs, axis=0, keepdims=True)
            out = dot_nn(v_t[feats, :], probs.astype(bf16)) / total
            attn_t[feats, at] = out.astype(bf16)
            lse[h : h + 1, at] = peak + jnp.log(total)
        attn[at, :] = attn_t[:, at].T

    tiles(seq // PAIR, queries)


class DepthScatter:
    def __init__(self, place, source, part, got, both, width, send, recv):
        self.place, self.source, self.part = place, source, part
        self.got, self.both, self.width = got, both, width
        self.send, self.recv = send, recv
        self.line = place.ndp == 4
        z = place.z
        self.end = jnp.logical_or(z == 0, z == 3)
        self.middle = jnp.logical_not(self.end)
        self.next = jnp.where(z == 3, 2, 1)
        self.other = jnp.clip(3 - z, 1, 2)
        self.near = jnp.clip(3 * (z - 1), 0, 3)

    def block(self, z):
        return self.source.at[:, pl.ds(pl.multiple_of(z * self.width, self.width), self.width)]

    def copy(self, src, slot, sem, z):
        return push(src, self.got.at[slot], self.send.at[sem], self.recv.at[slot], {"dp": z, "ctx": self.place.c})

    def from_end(self):
        far = 3 - self.place.z
        return [
            self.copy(self.block(far), 2, 0, self.next),
            self.copy(self.block(3 - self.next), 3, 1, self.next),
            self.copy(self.block(self.next), 0, 2, self.next),
        ]

    def from_middle(self):
        return [
            self.copy(self.both.at[0], 4, 0, self.other),
            self.copy(self.both.at[1], 1, 1, self.other),
            self.copy(self.both.at[2], 0, 2, self.near),
        ]

    def across(self):
        z, n = self.place.z, self.place.ndp
        return [self.copy(self.block(lax.rem(z + i, n)), i - 1, i - 1, lax.rem(z + i, n)) for i in range(1, n)]

    def start(self):
        self.start_first()
        self.start_last()

    def start_first(self):
        if not self.line:
            for copy in self.across():
                copy.start()
            return

        @pl.when(self.end)
        def _():
            for copy in self.from_end()[:2]:
                copy.start()

    def start_last(self):
        if self.line:
            pl.when(self.end)(self.from_end()[2].start)

    def hand_on(self, n):
        if not self.line:
            return

        @pl.when(self.middle)
        def _():
            owner, slot = ((3 - self.near, 2), (self.other, 3), (self.near, 4))[n]
            self.copy(self.both.at[0], slot, 0, self.near).wait_recv()
            cols = pl.ds(pl.multiple_of(owner * self.width, self.width), self.width)

            def add(at):
                total = self.part[at, cols].astype(jnp.float32) + self.got[slot, at, :].astype(jnp.float32)
                self.both[n, at, :] = total.astype(jnp.bfloat16)

            row_loop(self.part.shape[0], add)
            self.from_middle()[n].start()

    def collect(self, count, out_ref):
        for slot in range(count):
            self.copy(self.got.at[slot], slot, 0, self.next).wait_recv()
        cols = pl.ds(pl.multiple_of(self.place.z * self.width, self.width), self.width)

        def add(at):
            value = self.part[at, cols].astype(jnp.float32)
            for slot in range(count):
                value = value + self.got[slot, at, :].astype(jnp.float32)
            out_ref[at, :] = value

        row_loop(self.part.shape[0], add)

    def finish(self, out_ref):
        if not self.line:
            self.collect(self.place.ndp - 1, out_ref)
            for copy in self.across():
                copy.wait_send()
            return

        @pl.when(self.end)
        def _():
            self.collect(1, out_ref)
            for copy in self.from_end():
                copy.wait_send()

        @pl.when(self.middle)
        def _():
            self.collect(2, out_ref)
            for copy in self.from_middle():
                copy.wait_send()


def depth_scatter_scratch(ndp, rows, width):
    slots = 5 if ndp == 4 else ndp - 1
    return [
        pltpu.VMEM((slots, rows, width), jnp.bfloat16),
        pltpu.VMEM((3, rows, width), jnp.bfloat16),
        DMA((max(slots, 3),)),
        DMA((slots,)),
    ]


def tables(perm_ref, cos_ref, sin_ref, pos_col, pos_row, size):
    seq = pos_row.shape[1]
    lane = lax.broadcasted_iota(jnp.int32, (8, seq), 1)
    group = lane // size
    start = jnp.zeros((8, seq), jnp.int32)
    for g in range(seq // size):
        start = jnp.where(group == g, perm_ref[0, g], start)
    pos = (start * size + lane - group * size).astype(jnp.float32)
    pos_row[...] = pos[0:1]
    pos_col[...] = pos.T[:, 0:1]
    step = lax.broadcasted_iota(jnp.int32, (8, seq), 0).astype(jnp.float32)
    angle = pos * jnp.exp(step * (-2.0 / ROT * math.log(rope_base)))
    cos_ref[...] = jnp.cos(angle)
    sin_ref[...] = jnp.sin(angle)


def forward_kernel(
    perm_ref, x_ref, cot_ref, gain1_ref, bias1_ref, gain2_ref, bias2_ref, shift_ref,
    qkv_ref, out_ref, gateup_ref, down_ref,
    lse, first_sums, cos_ref, sin_ref, pos_col, pos_row,
    resid_out, q_out, k_out, v_out, attn_out, hidden_out, gate_side_out, up_side_out,
    rows_out, qkv_out, out_out, gateup_out, down_out, grads_out,
    row_block, cot_block, rows_all, cot_all, qkv_all, out_all, gateup_all, down_all,
    k_n, bias, attn, gate_f, hidden_t, gate_t, up_t, part, shifts,
    resid_ref, q_t, k_t, v_t, attn_t, hidden_ref, gate_side, up_side, *sems
):
    f32, bf16 = jnp.float32, jnp.bfloat16
    place = Place()
    greet(place, along_dp=True)
    sems = list(sems)

    def take(n):
        head = sems[:n]
        del sems[:n]
        return head

    def along_rows(size):
        return lambda ref, z: ref.at[:, pl.ds(pl.multiple_of(z * size, size), size), :]

    def along_lanes(size):
        return lambda ref, z: ref.at[:, pl.ds(pl.multiple_of(z * size, size), size)]

    depth, width = qkv_ref.shape[1], out_ref.shape[1]

    ff = gateup_ref.shape[1]
    half = ff // 2

    def slab(first):
        return lambda ref, z: ref.at[pl.ds(first, half), pl.ds(pl.multiple_of(z * depth, depth), depth)]

    qkv = DepthGather(place, qkv_ref, qkv_all, along_rows(depth), *take(3))
    out = DepthGather(place, out_ref, out_all, along_lanes(width), *take(3), passing=False)
    gate, up, down = [], [], []
    for h in range(2):
        at = pl.ds(h * half, half)
        gate.append(DepthGather(place, gateup_ref.at[0, at], gateup_all, slab(h * half), *take(3)))
        up.append(DepthGather(place, gateup_ref.at[1, at], gateup_all, slab(ff + h * half), *take(3)))
        down.append(DepthGather(place, down_ref.at[at], down_all, slab(h * half), *take(3)))
    rows = row_gather(place, row_block, rows_all, *take(3))
    cots = row_gather(place, cot_block, cot_all, *take(3))
    normeds = row_gather(place, row_block, rows_all, *take(3))
    scatter_refs = take(9)
    got, both, dsend, drecv = take(4)
    (save_sem,) = take(1)
    seq, d = rows_all.shape

    def save(i, src, dst):
        return pltpu.make_async_copy(src, dst, save_sem.at[i])

    saves = [
        save(0, rows_all, rows_out),
        save(1, qkv_all, qkv_out),
        save(2, out_all, out_out),
        save(3, gateup_all, gateup_out),
        save(4, down_all, down_out),
        save(5, gateup_all.at[pl.ds(0, 3 * half)], grads_out),
        save(6, q_t, q_out),
        save(7, k_t, k_out),
        save(8, v_t, v_out),
        save(9, attn_t, attn_out),
        save(10, resid_ref, resid_out),
    ]
    for h in range(2):
        saves.append(save(11 + 3 * h, hidden_ref.at[h], hidden_out.at[h]))
        saves.append(save(12 + 3 * h, gate_side.at[h], gate_side_out.at[h]))
        saves.append(save(13 + 3 * h, up_side.at[h], up_side_out.at[h]))

    qkv.start()
    gain, shift = gain1_ref[...].astype(f32)[None, :], bias1_ref[...].astype(f32)[None, :]

    def norm1(at):
        normed, _ = normal(x_ref[at, :].astype(f32))
        row_block[at, :] = (normed * gain + shift).astype(bf16)
        cot_block[at, :] = cot_ref[at, :].astype(bf16)

    row_loop(x_ref.shape[0], norm1)
    rows.start()
    cots.start()
    head = qkv_ref.shape[2]
    shifts[...] = shift_ref[:, pl.ds(pl.multiple_of(place.c * head, head), head)].astype(f32)
    tables(perm_ref, cos_ref, sin_ref, pos_col, pos_row, x_ref.shape[0] // 2)
    rows.forward()
    qkv.forward_next()
    cots.forward()
    qkv.forward_far()
    out.start()
    gate[0].start()
    up[0].start()
    rows.finish()
    saves[0].start()
    cots.finish()
    qkv.finish()
    saves[1].start()
    attend(rows_all, qkv_all, shifts, cos_ref, sin_ref, pos_col, pos_row, q_t, k_t, v_t, attn_t, lse, k_n, bias, attn)
    for i in range(6, 10):
        saves[i].start()
    gate[0].forward_next()
    up[0].forward_next()
    down[0].start()
    gate[1].start()
    out.finish()
    saves[2].start()
    saves[0].wait()
    scatter = sum_scatter(
        place,
        x_ref.shape[0],
        lambda at, cols: dot_nn(attn[at, :], out_all[:, cols]),
        *scatter_refs[:5],
        scatter_refs[5:9],
    )
    scatter.run()
    gate[0].forward_far()
    up[0].forward_far()
    down[0].forward_next()
    gain2, shift2 = gain2_ref[...].astype(f32)[None, :], bias2_ref[...].astype(f32)[None, :]

    def norm2(at):
        resid = x_ref[at, :].astype(f32) + scatter.total(at)
        resid_ref[at, :] = resid
        normed, _ = normal(resid)
        row_block[at, :] = (normed * gain2 + shift2).astype(bf16)

    row_loop(x_ref.shape[0], norm2)
    normeds.start()
    saves[10].start()
    normeds.forward()
    down[0].forward_far()
    gate[1].forward_next()
    up[1].start()
    normeds.finish()
    scatter.finish()

    def gates(h):
        def body(t):
            at = span(t, PAIR)
            gate_f[at, :] = dot_nt(rows_all[at, :], gateup_all[h * half : (h + 1) * half, :])

        tiles(seq // PAIR, body)

    def ups(h):
        def body(t):
            at = span(t, PAIR)
            value = dot_nt(rows_all[at, :], gateup_all[ff + h * half : ff + (h + 1) * half, :])
            g = gate_f[at, :]
            sigma = jax.nn.sigmoid(g)
            swish = g * sigma
            hidden = (swish * value).astype(bf16)
            hidden_ref[h, at, :] = hidden
            hidden_t[:, at] = hidden.T
            gate_side[h, at, :] = (value * sigma * (1.0 + g * (1.0 - sigma))).astype(bf16)
            up_side[h, at, :] = swish.astype(bf16)

        tiles(seq // PAIR, body)

    def sides(h):
        def body(t):
            at = span(t, PAIR)
            grad = dot_nt(cot_all[at, :], down_all[h * half : (h + 1) * half, :])
            gate_grad = (grad * gate_side[h, at, :].astype(f32)).astype(bf16)
            up_grad = (grad * up_side[h, at, :].astype(f32)).astype(bf16)
            gate_side[h, at, :] = gate_grad
            up_side[h, at, :] = up_grad
            gate_t[:, at] = gate_grad.T
            up_t[:, at] = up_grad.T

        tiles(seq // PAIR, body)

    def weights(target):
        def body(j):
            cols = span(j, 2 * PAIR)
            normed = rows_all[:, cols]
            target[:half, cols] = dot_nn(gate_t[...], normed).astype(bf16)
            target[half : 2 * half, cols] = dot_nn(up_t[...], normed).astype(bf16)
            target[2 * half : 3 * half, cols] = dot_nn(hidden_t[...], cot_all[:, cols]).astype(bf16)

        tiles(d // (2 * PAIR), body)

    gate[0].finish()
    gates(0)
    up[0].finish()
    ups(0)
    gate[1].forward_far()
    up[1].forward_next()
    down[1].start()
    down[0].finish()
    sides(0)
    for i in range(11, 14):
        saves[i].start()
    weights(part)
    summed = DepthScatter(place, part, part, got, both, width, dsend, drecv)
    summed.start()
    up[1].forward_far()
    down[1].forward_next()
    down[1].forward_far()
    gate[1].finish()
    gates(1)
    summed.hand_on(0)
    up[1].finish()
    saves[3].start()
    ups(1)
    summed.hand_on(1)
    summed.hand_on(2)
    down[1].finish()
    saves[4].start()
    saves[3].wait()
    sides(1)
    for i in range(14, 17):
        saves[i].start()
    weights(gateup_all)
    saves[5].start()
    summed.finish(first_sums)
    for i in (1, 2, *range(4, 17)):
        saves[i].wait()


def forward(perm, x, cot, gain1, bias1, gain2, bias2, shift, qkv, out, gateup, down):
    ndp, nctx = lax.axis_size("dp"), lax.axis_size("ctx")
    rows, d = x.shape
    seq, width, ff = rows * nctx, qkv.shape[2], gateup.shape[1]
    heads = width // HEAD_DIM
    bf16, f32 = jnp.bfloat16, jnp.float32
    row = [gain1, bias1, gain2, bias2]

    def shaped(shape, dtype=bf16):
        return jax.ShapeDtypeStruct(shape, dtype)

    return pl.pallas_call(
        forward_kernel,
        out_shape=(
            shaped((8, seq), f32),
            shaped((3 * ff // 2, d // ndp), f32),
            shaped((8, seq), f32),
            shaped((8, seq), f32),
            shaped((seq, 1), f32),
            shaped((1, seq), f32),
            shaped((rows, d), f32),
            shaped((width, seq)),
            shaped((width, seq)),
            shaped((width, seq)),
            shaped((width, seq)),
            shaped((2, seq, ff // 2)),
            shaped((2, seq, ff // 2)),
            shaped((2, seq, ff // 2)),
            shaped((seq, d)),
            shaped((3, d, width)),
            shaped((width, d)),
            shaped((2 * ff, d)),
            shaped((ff, d)),
            shaped((3 * ff // 2, d)),
        ),
        in_specs=[pl.BlockSpec(memory_space=pltpu.SMEM)] + [VMEM] * 7 + [ANY] * 4,
        out_specs=(VMEM,) * 6 + (ANY,) * 14,
        scratch_shapes=[
            pltpu.VMEM((rows, d), bf16),
            pltpu.VMEM((rows, d), bf16),
            pltpu.VMEM((seq, d), bf16),
            pltpu.VMEM((seq, d), bf16),
            pltpu.VMEM((3, d, width), bf16),
            pltpu.VMEM((width, d), bf16),
            pltpu.VMEM((2 * ff, d), bf16),
            pltpu.VMEM((ff, d), bf16),
            pltpu.VMEM((heads, seq, HEAD_DIM), bf16),
            pltpu.VMEM((seq, PAIR), f32),
            pltpu.VMEM((seq, width), bf16),
            pltpu.VMEM((seq, ff // 2), f32),
            pltpu.VMEM((ff // 2, seq), bf16),
            pltpu.VMEM((ff // 2, seq), bf16),
            pltpu.VMEM((ff // 2, seq), bf16),
            pltpu.VMEM((3 * ff // 2, d), bf16),
            pltpu.VMEM((3, width), f32),
            pltpu.VMEM((rows, d), f32),
            pltpu.VMEM((width, seq), bf16),
            pltpu.VMEM((width, seq), bf16),
            pltpu.VMEM((width, seq), bf16),
            pltpu.VMEM((width, seq), bf16),
            pltpu.VMEM((2, seq, ff // 2), bf16),
            pltpu.VMEM((2, seq, ff // 2), bf16),
            pltpu.VMEM((2, seq, ff // 2), bf16),
        ]
        + depth_sems(ndp) * 8
        + gather_sems(nctx) * 3
        + scatter_scratch(nctx, rows, d)
        + depth_scatter_scratch(ndp, 3 * ff // 2, d // ndp)
        + [DMA((17,))],
        compiler_params=pltpu.CompilerParams(
            collective_id=0, has_side_effects=True, vmem_limit_bytes=67_000_000
        ),
        cost_estimate=pl.CostEstimate(flops=0, bytes_accessed=700_000_000, transcendentals=0),
        name="forward",
    )(perm, x, cot, *row, shift, qkv, out, gateup, down)


def attend_back(
    grad_ref, w_ref, rows_ref, cos_ref, sin_ref, pos_col, pos_row, q_t, k_t, v_t, attn_t, lse,
    parts_ref, sums_ref, w_grads, g_t, delta, q_grad, kv_grad, bias, flat, rows_buf, rows_sem, between, w_out, w_sem
):
    seq, d = grad_ref.shape
    width = w_ref.shape[0]
    heads = width // HEAD_DIM
    bf16, f32 = jnp.bfloat16, jnp.float32
    count = d // (2 * PAIR)

    def load(j):
        slot = lax.rem(j, 2)
        return pltpu.make_async_copy(rows_ref.at[:, span(j, 2 * PAIR)], rows_buf.at[slot], rows_sem.at[slot])

    def first(t):
        at = span(t, PAIR)
        grad = dot_nt(w_ref[...], grad_ref[at, :])
        both = grad * attn_t[:, at].astype(f32)
        for h in range(heads):
            delta[h : h + 1, at] = jnp.sum(both[h * HEAD_DIM : (h + 1) * HEAD_DIM], axis=0, keepdims=True)
        g_t[:, at] = grad.astype(bf16)

    tiles(seq // PAIR, first)
    between()
    q_grad[...] = jnp.zeros_like(q_grad)

    def keys(t):
        at = span(t, PAIR)
        bias[...] = jnp.where(pos_col[at, :] <= pos_row[...], 0.0, neg_big)
        for h in range(heads):
            feats = slice(h * HEAD_DIM, (h + 1) * HEAD_DIM)
            keys_t = k_t[feats, at]
            probs = jnp.exp(dot_nn(keys_t.T, q_t[feats, :]) + bias[...] - lse[h : h + 1, :])
            kv_grad[1, feats, at] = dot_nt(g_t[feats, :], probs.astype(bf16))
            back = dot_nn(v_t[feats, at].T, g_t[feats, :])
            scores = (probs * (back - delta[h : h + 1, :])).astype(bf16)
            kv_grad[0, feats, at] = dot_nt(q_t[feats, :], scores)
            q_grad[feats, :] += dot_nn(keys_t, scores)

    tiles(seq // PAIR, keys)
    load(0).start()
    sums_ref[...] = jnp.zeros_like(sums_ref)

    def part(t):
        at = span(t, PAIR)
        cosine, sine = cos_ref[:, at], sin_ref[:, at]
        for i in range(3):
            if i == 0:
                grad = turn(q_grad[:, at] * (1.0 / math.sqrt(HEAD_DIM)), cosine, -sine, heads)
            elif i == 1:
                grad = turn(kv_grad[0, :, at], cosine, -sine, heads)
            else:
                grad = kv_grad[1, :, at]
            natural = grad.T
            sums_ref[i : i + 1, :] += jnp.sum(natural, axis=0, keepdims=True)
            parts_ref[i, at, :] = natural.astype(bf16)
            flat[i, :, at] = grad.astype(bf16)

    tiles(seq // PAIR, part)

    def weights(j):
        pl.when(j + 1 < count)(lambda: load(j + 1).start())
        load(j).wait()
        cols = span(j, 2 * PAIR)
        rows = rows_buf[lax.rem(j, 2)]
        for i in range(3):
            w_grads[i * width : (i + 1) * width, cols] = dot_nn(flat[i], rows).astype(bf16)
        w_grads[3 * width : 4 * width, cols] = dot_nn(attn_t[...], grad_ref[:, cols]).astype(bf16)
        keep(j).start()

    def keep(j):
        cols = span(j, 2 * PAIR)
        return pltpu.make_async_copy(w_grads.at[:, cols], w_out.at[:, cols], w_sem.at[j])

    tiles(count, weights)
    return lambda: tiles(count, lambda j: keep(j).wait())


def middle_kernel(
    gate_ref, up_ref, w_hbm, part_ref, resid_ref, cot_ref, gain_ref, out_hbm, rows_ref,
    cos_ref, sin_ref, pos_col, pos_row, q_hbm, k_hbm, v_hbm, attn_hbm, lse,
    grad_ref, vec_ref, parts_ref, sums_ref, second_sums, w_out,
    arena, part_all, block, out_ref, q_t, k_t, v_t, attn_t, grad_all, g_t, delta, q_grad, kv_grad, bias, flat, rows_buf, rows_sem, save_sem, w_sem, *scratch
):
    place = Place()
    greet(place, along_dp=True)
    scratch = list(scratch)

    def take(n):
        head = scratch[:n]
        del scratch[:n]
        return head

    rows = resid_ref.shape[0]
    half, d = gate_ref.shape[2], part_ref.shape[1]
    ff = 2 * half
    piece = d // place.ndp
    refs = take(9)
    sum_refs = take(4)
    summed = DepthScatter(place, part_ref, part_all, *sum_refs[:2], piece, *sum_refs[2:])
    summed.start()
    load = pltpu.make_async_copy(w_hbm, arena, save_sem.at[0])
    fetch = pltpu.make_async_copy(part_ref, part_all, save_sem.at[1])
    later = [
        pltpu.make_async_copy(src, dst, save_sem.at[4 + i])
        for i, (src, dst) in enumerate(
            ((out_hbm, out_ref), (q_hbm, q_t), (k_hbm, k_t), (v_hbm, v_t), (attn_hbm, attn_t))
        )
    ]
    load.start()
    fetch.start()
    for copy in later:
        copy.start()
    load.wait()

    def product(at, cols):
        total = dot_nn(gate_ref[0, at, :], arena[:half, cols])
        total = total + dot_nn(gate_ref[1, at, :], arena[half:ff, cols])
        total = total + dot_nn(up_ref[0, at, :], arena[ff : ff + half, cols])
        return total + dot_nn(up_ref[1, at, :], arena[ff + half :, cols])

    scatter = sum_scatter(place, rows, product, *refs[:5], refs[5:9])
    scatter.run()
    gain = gain_ref[...].astype(jnp.float32)[None, :]
    vec_ref[...] = jnp.zeros_like(vec_ref)

    def back(at):
        grad = scatter.total(at)
        normed, rscale = normal(resid_ref[at, :])
        vec_ref[0:1, :] += jnp.sum(grad * normed, axis=0, keepdims=True)
        vec_ref[1:2, :] += jnp.sum(grad, axis=0, keepdims=True)
        out = cot_ref[at, :] + normal_back(grad, normed, rscale, gain)
        grad_ref[at, :] = out
        block[at, :] = out.astype(jnp.bfloat16)

    row_loop(rows, back)
    gathered = row_gather(place, block, grad_all, *take(3))
    gathered.start()
    fetch.wait()
    summed.hand_on(0)
    gathered.forward()
    gathered.finish()
    for copy in later:
        copy.wait()
    scatter.finish()

    def between():
        summed.hand_on(1)
        summed.hand_on(2)

    w_grads = arena.at[: w_out.shape[0]]
    kept = attend_back(
        grad_all, out_ref, rows_ref, cos_ref, sin_ref, pos_col, pos_row, q_t, k_t, v_t, attn_t, lse,
        parts_ref, sums_ref, w_grads, g_t, delta, q_grad, kv_grad, bias, flat, rows_buf, rows_sem, between, w_out, w_sem,
    )
    summed.finish(second_sums)
    kept()


def middle(gate_grad, up_grad, w, part, resid, cot, gain, out, rows_all, cosine, sine, pos_col, pos_row, q_t, k_t, v_t, attn_t, lse):
    ndp, nctx = lax.axis_size("dp"), lax.axis_size("ctx")
    rows, d = resid.shape
    seq, width, ff = rows * nctx, out.shape[0], w.shape[0] // 2
    bf16, f32 = jnp.bfloat16, jnp.float32
    return pl.pallas_call(
        middle_kernel,
        out_shape=(
            jax.ShapeDtypeStruct((rows, d), f32),
            jax.ShapeDtypeStruct((2, d), f32),
            jax.ShapeDtypeStruct((3, seq, width), bf16),
            jax.ShapeDtypeStruct((3, width), f32),
            jax.ShapeDtypeStruct((3 * ff // 2, d // ndp), f32),
            jax.ShapeDtypeStruct((4 * width, d), bf16),
        ),
        in_specs=[VMEM] * 2 + [ANY] * 2 + [VMEM] * 3 + [ANY] * 2 + [VMEM] * 4 + [ANY] * 4 + [VMEM],
        out_specs=(VMEM,) * 5 + (ANY,),
        scratch_shapes=[
            pltpu.VMEM((2 * ff, d), bf16),
            pltpu.VMEM((3 * ff // 2, d), bf16),
            pltpu.VMEM((rows, d), bf16),
            pltpu.VMEM((width, d), bf16),
            pltpu.VMEM((width, seq), bf16),
            pltpu.VMEM((width, seq), bf16),
            pltpu.VMEM((width, seq), bf16),
            pltpu.VMEM((width, seq), bf16),
            pltpu.VMEM((seq, d), bf16),
            pltpu.VMEM((width, seq), bf16),
            pltpu.VMEM((8, seq), f32),
            pltpu.VMEM((width, seq), f32),
            pltpu.VMEM((2, width, seq), f32),
            pltpu.VMEM((PAIR, seq), f32),
            pltpu.VMEM((3, width, seq), bf16),
            pltpu.VMEM((2, seq, 2 * PAIR), bf16),
            DMA((2,)),
            DMA((9,)),
            DMA((d // (2 * PAIR),)),
        ]
        + scatter_scratch(nctx, rows, d)
        + depth_scatter_scratch(ndp, 3 * ff // 2, d // ndp)
        + gather_sems(nctx),
        compiler_params=pltpu.CompilerParams(
            collective_id=2, has_side_effects=True, vmem_limit_bytes=67_000_000
        ),
        cost_estimate=pl.CostEstimate(flops=0, bytes_accessed=300_000_000, transcendentals=0),
        name="middle",
    )(gate_grad, up_grad, w, part, resid, cot, gain, out, rows_all, cosine, sine, pos_col, pos_row, q_t, k_t, v_t, attn_t, lse)


class VectorSum:
    def __init__(self, place, value, from_ctx, from_dp, plane, ctx_send, ctx_recv, dp_send, dp_recv):
        self.place, self.value, self.from_ctx, self.from_dp, self.plane = place, value, from_ctx, from_dp, plane
        self.ctx_send, self.ctx_recv, self.dp_send, self.dp_recv = ctx_send, ctx_recv, dp_send, dp_recv

    def across(self, i):
        place = self.place
        return push(
            self.value, self.from_ctx.at[place.c], self.ctx_send.at[i - 1], self.ctx_recv.at[place.c],
            place.at(lax.rem(place.c + i, place.nctx)),
        )

    def along(self, i):
        place = self.place
        return push(
            self.plane, self.from_dp.at[place.z], self.dp_send.at[i - 1], self.dp_recv.at[place.z],
            {"dp": lax.rem(place.z + i, place.ndp), "ctx": place.c},
        )

    def start(self):
        for i in range(1, self.place.nctx):
            self.across(i).start()
        self.from_ctx[self.place.c] = self.value[...]

    def turn(self):
        place = self.place
        for i in range(1, place.nctx):
            c = lax.rem(place.c + i, place.nctx)
            push(self.value, self.from_ctx.at[c], self.ctx_send.at[0], self.ctx_recv.at[c], place.at(c)).wait_recv()
        total = self.from_ctx[0]
        for i in range(1, place.nctx):
            total = total + self.from_ctx[i]
        self.plane[...] = total
        self.from_dp[place.z] = total
        for i in range(1, place.ndp):
            self.along(i).start()

    def finish(self, out_ref):
        place = self.place
        for i in range(1, place.ndp):
            z = lax.rem(place.z + i, place.ndp)
            device = {"dp": z, "ctx": place.c}
            push(self.plane, self.from_dp.at[z], self.dp_send.at[0], self.dp_recv.at[z], device).wait_recv()
        total = self.from_dp[0]
        for i in range(1, place.ndp):
            total = total + self.from_dp[i]
        out_ref[...] = total
        for i in range(1, place.nctx):
            self.across(i).wait_send()
        for i in range(1, place.ndp):
            self.along(i).wait_send()


def vector_scratch(ndp, nctx, shape):
    f32 = jnp.float32
    return [
        pltpu.VMEM(shape, f32),
        pltpu.VMEM((nctx,) + shape, f32),
        pltpu.VMEM((ndp,) + shape, f32),
        pltpu.VMEM(shape, f32),
        DMA((nctx - 1,)),
        DMA((nctx,)),
        DMA((ndp - 1,)),
        DMA((ndp,)),
    ]


def tail_kernel(
    w_grads, parts_hbm, qkv_hbm, x_ref, grad_ref, gain_ref, hidden_hbm, down_ref, resid_ref, vec_ref, sums_ref,
    block_out, input_grad, small, qkv_grads, out_grads,
    total, *scratch
):
    place = Place()
    greet(place, all_ctx=True, along_dp=True)
    scratch = list(scratch)

    def take(n):
        head = scratch[:n]
        del scratch[:n]
        return head

    rows, d = x_ref.shape
    width = qkv_hbm.shape[2]
    first_refs, second_refs = take(9), take(9)
    long_refs, short_refs = take(4), take(4)
    vectors = VectorSum(place, *take(8))
    w_all, down_all, parts_ref, qkv_ref, hidden_ref, load_sem = take(6)
    piece, cut = d // place.ndp, 3 * width
    upper, lower = pl.ds(0, cut), pl.ds(cut, width)
    long_sum = DepthScatter(place, w_grads.at[upper], w_all.at[upper], *long_refs[:2], piece, *long_refs[2:])
    short_sum = DepthScatter(place, w_grads.at[lower], w_all.at[lower], *short_refs[:2], piece, *short_refs[2:])
    long_sum.start_first()
    short_sum.start_first()
    long_sum.start_last()
    short_sum.start_last()
    loads = [
        pltpu.make_async_copy(src, dst, load_sem.at[i])
        for i, (src, dst) in enumerate(
            ((parts_hbm, parts_ref), (qkv_hbm, qkv_ref), (w_grads, w_all), (hidden_hbm, hidden_ref), (down_ref, down_all))
        )
    ]
    for copy in loads:
        copy.start()

    def product(at, cols):
        part = dot_nt(parts_ref[0, at, :], qkv_ref[0, cols, :])
        part = part + dot_nt(parts_ref[1, at, :], qkv_ref[1, cols, :])
        return part + dot_nt(parts_ref[2, at, :], qkv_ref[2, cols, :])

    first = sum_scatter(place, rows, product, *first_refs[:5], first_refs[5:9])
    half = hidden_ref.shape[2]

    def down_product(at, cols):
        return dot_nn(hidden_ref[0, at, :], down_all[:half, cols]) + dot_nn(hidden_ref[1, at, :], down_all[half:, cols])

    second = sum_scatter(place, rows, down_product, *second_refs[:5], second_refs[5:9])
    for copy in loads[:2]:
        copy.wait()
    first.run()
    gain = gain_ref[...].astype(jnp.float32)[None, :]
    value = vectors.value
    value[...] = jnp.zeros_like(value)
    value[2:4, :] = vec_ref[...]
    value[4:7, pl.ds(pl.multiple_of(place.c * width, width), width)] = sums_ref[...]

    def back(at):
        grad = first.total(at)
        normed, rscale = normal(x_ref[at, :].astype(jnp.float32))
        value[0:1, :] += jnp.sum(grad * normed, axis=0, keepdims=True)
        value[1:2, :] += jnp.sum(grad, axis=0, keepdims=True)
        input_grad[at, :] = grad_ref[at, :] + normal_back(grad, normed, rscale, gain)

    row_loop(rows, back)
    vectors.start()
    for copy in loads[2:]:
        copy.wait()
    long_sum.hand_on(0)

    def between_first():
        long_sum.hand_on(1)
        short_sum.hand_on(0)

    def between_second():
        long_sum.hand_on(2)
        short_sum.hand_on(1)

    second.run((between_first, between_second))
    short_sum.hand_on(2)

    def add(at):
        block_out[at, :] = (resid_ref[at, :] + second.total(at)).astype(jnp.bfloat16)

    row_loop(rows, add)
    vectors.turn()
    first.finish()
    second.finish()
    vectors.finish(small)
    long_sum.finish(total.at[upper])
    short_sum.finish(out_grads)
    for i in range(3):
        qkv_grads[i] = total[i * width : (i + 1) * width, :].T


def tail(w_grads, parts, qkv, x, grad, gain, hidden, down, resid, vec, sums):
    ndp, nctx = lax.axis_size("dp"), lax.axis_size("ctx")
    rows, d = x.shape
    width = qkv.shape[2]
    bf16, f32 = jnp.bfloat16, jnp.float32
    return pl.pallas_call(
        tail_kernel,
        out_shape=(
            jax.ShapeDtypeStruct((rows, d), bf16),
            jax.ShapeDtypeStruct((rows, d), f32),
            jax.ShapeDtypeStruct((8, d), f32),
            jax.ShapeDtypeStruct((3, d // ndp, width), f32),
            jax.ShapeDtypeStruct((width, d // ndp), f32),
        ),
        in_specs=[ANY] * 3 + [VMEM] * 3 + [ANY] * 2 + [VMEM] * 3,
        out_specs=(VMEM,) * 5,
        scratch_shapes=[pltpu.VMEM((3 * width, d // ndp), f32)]
        + scatter_scratch(nctx, rows, d) * 2
        + depth_scatter_scratch(ndp, 3 * width, d // ndp)
        + depth_scatter_scratch(ndp, width, d // ndp)
        + vector_scratch(ndp, nctx, (8, d))
        + [pltpu.VMEM(v.shape, bf16) for v in (w_grads, down, parts, qkv, hidden)]
        + [DMA((5,))],
        compiler_params=pltpu.CompilerParams(
            collective_id=3, has_side_effects=True, vmem_limit_bytes=67_000_000
        ),
        cost_estimate=pl.CostEstimate(flops=0, bytes_accessed=300_000_000, transcendentals=0),
        name="tail",
    )(w_grads, parts, qkv, x, grad, gain, hidden, down, resid, vec, sums)


def per_device(
    block_input,
    out_cotangent,
    group_perm,
    attn_norm_gain,
    attn_norm_bias,
    qkv_weight,
    qkv_bias,
    out_weight,
    mlp_norm_gain,
    mlp_norm_bias,
    gateup_weight,
    down_weight,
):
    width_local = qkv_weight.shape[2]
    (
        lse, first_sums, cos_all, sin_all, pos_col, pos_row,
        residual_stream, q_t, k_t, v_t, attn_t, hidden_b, gate_grad, up_grad,
        rows_all, qkv_local, out_local, gateup_local, down_local, mlp_grads,
    ) = forward(
        group_perm, block_input, out_cotangent, attn_norm_gain, attn_norm_bias, mlp_norm_gain, mlp_norm_bias, qkv_bias,
        qkv_weight, out_weight, gateup_weight.transpose(0, 2, 1), down_weight,
    )
    resid_grad, second_vectors, grad_parts_b, shift_part, second_sums, attn_grads = middle(
        gate_grad, up_grad, gateup_local, mlp_grads, residual_stream, out_cotangent, mlp_norm_gain, out_local,
        rows_all, cos_all, sin_all, pos_col, pos_row, q_t, k_t, v_t, attn_t, lse,
    )
    block_output, input_grad, small, qkv_grads, out_grads = tail(
        attn_grads, grad_parts_b, qkv_local, block_input, resid_grad, attn_norm_gain,
        hidden_b, down_local, residual_stream, second_vectors, shift_part,
    )
    half = first_sums.shape[0] // 3
    both = [
        jnp.concatenate([first_sums[i * half : (i + 1) * half], second_sums[i * half : (i + 1) * half]])
        for i in range(3)
    ]
    gateup_grads, down_grads = jnp.stack(both[:2]), both[2]
    return (
        block_output,
        input_grad,
        small[0],
        small[1],
        qkv_grads,
        small[4:7],
        out_grads,
        small[2],
        small[3],
        gateup_grads.transpose(0, 2, 1),
        down_grads,
    )


def solution(mesh):
    return jax.shard_map(
        per_device,
        mesh=mesh,
        in_specs=(
            P(("dp", "ctx"), None),
            P(("dp", "ctx"), None),
            P("dp", None),
            P(),
            P(),
            P(None, "dp", "ctx"),
            P(),
            P("ctx", "dp"),
            P(),
            P(),
            P(None, "dp", "ctx"),
            P("ctx", "dp"),
        ),
        out_specs=(
            P(("dp", "ctx"), None),
            P(("dp", "ctx"), None),
            P(),
            P(),
            P(None, "dp", "ctx"),
            P(),
            P("ctx", "dp"),
            P(),
            P(),
            P(None, "dp", "ctx"),
            P("ctx", "dp"),
        ),
        check_vma=False,
    )
```
